32 devices in a mesh: dp: 8 (over z, y), fsdp: 4 (over x, core).
Axes of the slice: x: 2, y: 2, z: 4, core: 2. Of those that a mesh axis runs over, the one named last changes fastest.
Arguments:
- block_input: bfloat16 [32768, 768], P(('dp', 'fsdp')), may hold values from -6 to 6
- segment_ids: int32 [32768], P(('dp', 'fsdp')), may hold values from -1 to 63, as said below
- norm1_gain: bfloat16 [768], P('fsdp'), may hold values from 0.5 to 1.5
- norm1_bias: bfloat16 [768], P('fsdp'), may hold values from -3 to 3
- qkv_weight: bfloat16 [768, 2304], P('fsdp'), may hold values from -0.21875 to 0.21875
- qkv_bias: bfloat16 [2304], P('fsdp'), may hold values from -3 to 3
- query_gain: bfloat16 [64], P('fsdp'), may hold values from 0.25 to 1.75
- key_gain: bfloat16 [64], P('fsdp'), may hold values from 0.25 to 1.75
- out_weight: bfloat16 [768, 768], P('fsdp'), may hold values from -2.5 to 2.5
- out_bias: bfloat16 [768], P('fsdp'), may hold values from -3 to 3
- norm2_gain: bfloat16 [768], P('fsdp'), may hold values from 0.5 to 1.5
- norm2_bias: bfloat16 [768], P('fsdp'), may hold values from -3 to 3
- up_weight: bfloat16 [768, 3072], P('fsdp'), may hold values from -0.21875 to 0.21875
- up_bias: bfloat16 [3072], P('fsdp'), may hold values from -3 to 3
- down_weight: bfloat16 [3072, 768], P('fsdp'), may hold values from -0.109375 to 0.109375
- down_bias: bfloat16 [768], P('fsdp'), may hold values from -3 to 3
- output_grad: bfloat16 [32768, 768], P(('dp', 'fsdp')), may hold values from -9 to 9
Outputs:
- output: bfloat16 [32768, 768], P(('dp', 'fsdp'))
- input_grad: bfloat16 [32768, 768], P(('dp', 'fsdp'))
- norm1_gain_grad: float32 [768], P('fsdp')
- norm1_bias_grad: float32 [768], P('fsdp')
- qkv_weight_grad: float32 [768, 2304], P('fsdp')
- qkv_bias_grad: float32 [2304], P('fsdp')
- query_gain_grad: float32 [64], P('fsdp')
- key_gain_grad: float32 [64], P('fsdp')
- out_weight_grad: float32 [768, 768], P('fsdp')
- out_bias_grad: float32 [768], P('fsdp')
- norm2_gain_grad: float32 [768], P('fsdp')
- norm2_bias_grad: float32 [768], P('fsdp')
- up_weight_grad: float32 [768, 3072], P('fsdp')
- up_bias_grad: float32 [3072], P('fsdp')
- down_weight_grad: float32 [3072, 768], P('fsdp')
- down_bias_grad: float32 [768], P('fsdp')
The draws below stay inside these ranges and needn't reach their ends.
Inputs may be any that keep to these rules, and one draw needn't show every extreme that they name: `segment_ids`: within each aligned block of 1024 tokens (one packed sequence) the ids number whole images 0, 1, 2, ... in order, each image 16 to 1024 tokens; tokens after the last image are padding with id -1. The first sequence is a single image of 1024 tokens.
All inputs are finite; a program needn't handle non-finite values.
Results may differ from the reference program's by a relative error of at most 0.014.
Values may be sent and summed in bfloat16 or wider, within the bound.
A program may use at most 256 MiB of HBM per device.

```python
import math
import jax
import jax.numpy as jnp
from jax import lax

D = 768
HEADS = 12
HD = 64
FF = 3072
LEN = 1024
TOKENS = 32768


def draw_segment_ids(key, part):
    sequences = TOKENS // LEN
    slots = LEN // 16
    upper = max(17, LEN * 3 // 8)
    lengths = jax.random.randint(key, (sequences, slots), 16, upper)
    ends = jnp.cumsum(lengths, axis=1)
    position = jnp.arange(LEN, dtype=jnp.int32)
    image = jnp.sum((ends[:, :, None] <= position[None, None, :]).astype(jnp.int32), axis=1)
    last_end = jnp.max(jnp.where(ends <= LEN, ends, 0), axis=1)
    padding = position[None, :] >= last_end[:, None]
    ids = jnp.where(padding, -1, image)
    rows = jnp.arange(sequences, dtype=jnp.int32)[:, None]
    ids = jnp.where(rows == 0, 0, ids)
    padded_row = jnp.where(position < LEN - 16, 0, -1).astype(jnp.int32)
    ids = jnp.where(rows == 1, padded_row[None, :], ids)
    finest_row = (position // 16).astype(jnp.int32)
    ids = jnp.where(rows == sequences - 1, finest_row[None, :], ids)
    return ids.reshape(-1).astype(jnp.int32)


def draw_output_grad(key, part):
    rows = jnp.arange(TOKENS, dtype=jnp.float32)
    scale = 0.6 + 1.2 * rows / TOKENS
    base = jnp.clip(jax.random.normal(key, (TOKENS, D), jnp.float32), -5.0, 5.0)
    return (base * scale[:, None]).astype(jnp.bfloat16)


def block_scale(rng, extent, shards, low, top_value):
    factor_of, own = 1.0, jax.random.fold_in(rng, 6)
    for dim, blocks in shards:
        draws = jnp.exp(jax.random.uniform(jax.random.fold_in(own, dim), (blocks,), jnp.float32, low / len(shards), top_value / len(shards)))
        factor_of = factor_of * jnp.repeat(draws, extent[dim] // blocks).reshape([-1 if axis == dim else 1 for axis in range(len(extent))])
    return factor_of


def scatter_about(rng, shape, scale, bound, shards=(), kind=jnp.bfloat16):
    drawn = scale * jax.random.normal(rng, shape, jnp.float32)
    if shards:
        drawn = drawn * block_scale(rng, shape, shards, -0.22, 0.18)
    return jnp.clip(drawn, -bound, bound).astype(kind)


def setup_inputs(seed: int = 0) -> dict:
    key_list = jax.random.split(jax.random.key(seed), 18)
    block_input = scatter_about(key_list[0], (TOKENS, D), 1.0, 6.0, ((0, 32),))
    segment_ids = draw_segment_ids(jax.random.fold_in(key_list[17], 71), 0)
    norm1_gain = jnp.clip(1.0 + 0.1 * jax.random.normal(key_list[2], (D,), jnp.float32), 0.5, 1.5).astype(jnp.bfloat16)
    norm1_bias = scatter_about(key_list[3], (D,), 0.5, 3.0, ((0, 4),))
    qkv_weight = scatter_about(key_list[4], (D, 3 * D), D ** -0.5, 0.21875, ((0, 4),))
    qkv_bias = scatter_about(key_list[5], (3 * D,), 0.5, 3.0, ((0, 4),))
    query_gain = jnp.clip(1.0 + 0.15 * jax.random.normal(key_list[6], (HD,), jnp.float32), 0.25, 1.75).astype(jnp.bfloat16)
    key_gain = jnp.clip(1.0 + 0.15 * jax.random.normal(key_list[7], (HD,), jnp.float32), 0.25, 1.75).astype(jnp.bfloat16)
    out_weight = scatter_about(key_list[8], (D, D), (max(1, D // 128)) ** -0.5, 2.5, ((0, 4),))
    out_bias = scatter_about(key_list[9], (D,), 0.5, 3.0, ((0, 4),))
    norm2_gain = jnp.clip(1.0 + 0.1 * jax.random.normal(key_list[10], (D,), jnp.float32), 0.5, 1.5).astype(jnp.bfloat16)
    norm2_bias = scatter_about(key_list[11], (D,), 0.5, 3.0, ((0, 4),))
    up_weight = scatter_about(key_list[12], (D, FF), D ** -0.5, 0.21875, ((0, 4),))
    up_bias = scatter_about(key_list[13], (FF,), 0.5, 3.0, ((0, 4),))
    down_weight = scatter_about(key_list[14], (FF, D), FF ** -0.5, 0.109375, ((0, 4),))
    down_bias = scatter_about(key_list[15], (D,), 0.5, 3.0, ((0, 4),))
    output_grad = draw_output_grad(jax.random.fold_in(key_list[17], 71), 0)
    return {"block_input": block_input, "segment_ids": segment_ids, "norm1_gain": norm1_gain, "norm1_bias": norm1_bias, "qkv_weight": qkv_weight, "qkv_bias": qkv_bias, "query_gain": query_gain, "key_gain": key_gain, "out_weight": out_weight, "out_bias": out_bias, "norm2_gain": norm2_gain, "norm2_bias": norm2_bias, "up_weight": up_weight, "up_bias": up_bias, "down_weight": down_weight, "down_bias": down_bias, "output_grad": output_grad}


EPS = 1e-06
HIGHEST_PRECISION = lax.Precision.HIGHEST

@jax.custom_vjp
def low(v):
    return lax.optimization_barrier(v.astype(jnp.bfloat16)).astype(jnp.float32)

@jax.custom_vjp
def low_back(v):
    return v

def low_keep(v):
    return (low(v), None)

def low_pass(kept, grad):
    return (grad,)

def back_keep(v):
    return (v, None)

def back_low(kept, grad):
    return (low(grad),)
low.defvjp(low_keep, low_pass)
low_back.defvjp(back_keep, back_low)

def matmul(left, right):
    return jnp.dot(left, right, precision=HIGHEST_PRECISION)

def layer_norm(values, gain, shift):
    center = values - lax.optimization_barrier(jnp.mean(values, axis=-1, keepdims=True))
    spread = lax.optimization_barrier(jnp.mean(center * center, axis=-1, keepdims=True))
    return center * lax.rsqrt(spread + EPS) * gain + shift

def head_norm(values, gain):
    center = values - lax.optimization_barrier(jnp.mean(values, axis=-1, keepdims=True))
    spread = lax.optimization_barrier(jnp.mean(center * center, axis=-1, keepdims=True))
    return center * lax.rsqrt(spread + EPS) * gain

def attention(query_norm, key_norm, value_low, segments):
    groups = query_norm.shape[0]
    block = min(512, LEN)
    blocks = LEN // block
    scale = 1.0 / math.sqrt(HD)
    query_blocks = query_norm.reshape(groups, blocks, block, HEADS, HD).transpose(1, 0, 2, 3, 4)
    segment_blocks = segments.reshape(groups, blocks, block).transpose(1, 0, 2)

    def one_block(inputs):
        query_block, segment_block = inputs
        scores = jnp.einsum('gqhd,gkhd->ghqk', query_block, key_norm, precision=HIGHEST_PRECISION) * scale
        scores = low_back(scores)
        row_valid = segment_block >= 0
        allowed = jnp.logical_and(segment_block[:, :, None] == segments[:, None, :], row_valid[:, :, None])[:, None]
        row_mask = row_valid[:, None, :, None]
        top = lax.optimization_barrier(jnp.max(jnp.where(allowed, scores, -1e+30), axis=-1, keepdims=True))
        top = jnp.where(row_mask, top, 0.0)
        weights = jnp.exp(jnp.where(allowed, scores - top, -1e+30))
        total = lax.optimization_barrier(jnp.sum(weights, axis=-1, keepdims=True))
        weights = low(weights / jnp.where(row_mask, total, 1.0))
        return jnp.einsum('ghqk,gkhd->gqhd', weights, value_low, precision=HIGHEST_PRECISION)
    outputs = lax.map(jax.checkpoint(one_block), (query_blocks, segment_blocks))
    return outputs.transpose(1, 0, 2, 3, 4).reshape(groups * LEN, HEADS * HD)

def forward(block, segments, params):
    first_gain, first_shift, qkv_matrix, qkv_shift, query_scale, key_scale, out_matrix, out_shift, second_gain, second_shift, up_matrix, up_shift, down_matrix, down_shift = params
    groups = segments.shape[0]
    valid = (segments >= 0).reshape(-1)
    normed = low(layer_norm(block, first_gain, first_shift))
    projected = low_back(matmul(normed, qkv_matrix) + qkv_shift)
    queries = projected[:, :D].reshape(groups, LEN, HEADS, HD)
    keys_raw = projected[:, D:2 * D].reshape(groups, LEN, HEADS, HD)
    values_raw = projected[:, 2 * D:].reshape(groups, LEN, HEADS, HD)
    query_norm = low(head_norm(queries, query_scale))
    key_norm = low(head_norm(keys_raw, key_scale))
    value_low = low(values_raw)
    mixed = attention(query_norm, key_norm, value_low, segments)
    mixed = low(low_back(mixed))
    attn_branch = low_back(matmul(mixed, out_matrix) + out_shift)
    middle = block + attn_branch
    normed_two = low(layer_norm(middle, second_gain, second_shift))
    hidden = low_back(matmul(normed_two, up_matrix) + up_shift)
    active = low(jax.nn.gelu(hidden, approximate=False))
    mlp_branch = low_back(matmul(active, down_matrix) + down_shift)
    return jnp.where(valid[:, None], middle + mlp_branch, 0.0)

def reference(block_input, segment_ids, norm1_gain, norm1_bias, qkv_weight, qkv_bias, query_gain, key_gain, out_weight, out_bias, norm2_gain, norm2_bias, up_weight, up_bias, down_weight, down_bias, output_grad):
    params = tuple((weight.astype(jnp.float32) for weight in (norm1_gain, norm1_bias, qkv_weight, qkv_bias, query_gain, key_gain, out_weight, out_bias, norm2_gain, norm2_bias, up_weight, up_bias, down_weight, down_bias)))
    sequences = TOKENS // LEN
    group = max(1, min(sequences, 4096 // LEN))
    while sequences % group != 0:
        group = group - 1
    rounds = sequences // group
    inputs = block_input.astype(jnp.float32).reshape(rounds, group * LEN, D)
    segment_groups = segment_ids.reshape(rounds, group, LEN)
    cotangents = output_grad.astype(jnp.float32).reshape(rounds, group * LEN, D)

    def one_group(totals, batch):
        block, segments, cotangent = batch

        def apply(block_arg, *weights):
            return forward(block_arg, segments, weights)
        result, pull = jax.vjp(apply, block, *params)
        pulled = pull(cotangent)
        totals = tuple((total + grad for total, grad in zip(totals, pulled[1:])))
        return (totals, (result.astype(jnp.bfloat16), pulled[0].astype(jnp.bfloat16)))
    zeros = tuple((jnp.zeros(weight.shape, jnp.float32) for weight in params))
    totals, (outputs, input_grads) = lax.scan(one_group, zeros, (inputs, segment_groups, cotangents))
    grad_one, grad_two, grad_three, grad_four, grad_five, grad_six, grad_seven, grad_eight, grad_nine, grad_ten, grad_eleven, grad_twelve, grad_thirteen, grad_fourteen = totals
    return (outputs.reshape(TOKENS, D), input_grads.reshape(TOKENS, D), grad_one, grad_two, grad_three, grad_four, grad_five, grad_six, grad_seven, grad_eight, grad_nine, grad_ten, grad_eleven, grad_twelve, grad_thirteen, grad_fourteen)
```

```python
import functools
import math

import jax
import jax.numpy as jnp
from jax import lax
from jax.experimental import pallas as pl
from jax.experimental.pallas import tpu as pltpu
from jax.sharding import PartitionSpec as P

D = 768
HEADS = 12
HD = 64
PAIR = 128
PAIRS = HEADS // 2
EPS = 1e-06
BF = jnp.bfloat16
F32 = jnp.float32
LOG2E = 1.4426950408889634
ROWS = 256
FBLOCK = 512
QMARK = 16.0
KMARK = 12.0

NN = (((1,), (0,)), ((), ()))
NT = (((1,), (1,)), ((), ()))
TN = (((0,), (0,)), ((), ()))


def dot(left, right, dims):
    return lax.dot_general(left, right, dims, preferred_element_type=F32)


def params(*semantics):
    return pltpu.CompilerParams(
        dimension_semantics=semantics or ("arbitrary",), vmem_limit_bytes=60 * 1024 * 1024
    )


def cost(flops, nbytes, trans=0):
    return pl.CostEstimate(flops=int(flops), bytes_accessed=int(nbytes), transcendentals=int(trans))


def whole(shape):
    return pl.BlockSpec(shape, lambda *_: (0,) * len(shape))


ANY = pl.BlockSpec(memory_space=pl.ANY)


def fetch(pieces, full, sems):
    rank = lax.axis_index("fsdp")
    rows = full.shape[0] // len(pieces)
    copies = []
    for distance, piece in enumerate(pieces):
        start = pl.multiple_of((rank ^ distance) * rows, rows)
        copies.append(
            pltpu.make_async_copy(piece, full.at[pl.ds(start, rows)], sems.at[distance])
        )
    for item in copies:
        item.start()
    return copies


def stats(values):
    center = values - jnp.mean(values, axis=-1, keepdims=True)
    rstd = lax.rsqrt(jnp.mean(center * center, axis=-1, keepdims=True) + EPS)
    return center, rstd


def low_half(rows):
    return lax.broadcasted_iota(jnp.int32, (rows, PAIR), 1) < HD


def pair_mean(values, low):
    first = jnp.sum(jnp.where(low, values, 0.0), axis=-1, keepdims=True)
    second = jnp.sum(jnp.where(low, 0.0, values), axis=-1, keepdims=True)
    return jnp.where(low, first, second) * (1.0 / HD)


def front_body(count, *refs):
    x_ref, gain_ref, shift_ref = refs[:3]
    pieces = refs[3 : 3 + count]
    bias_ref, qgain_ref, kgain_ref, h_ref, qkv_ref, rstd_ref, full, sems = refs[3 + count :]

    @pl.when(pl.program_id(0) == 0)
    def _():
        for item in fetch(pieces, full, sems):
            item.wait()

    center, rstd = stats(x_ref[...].astype(F32))
    h = (center * rstd * gain_ref[...] + shift_ref[...]).astype(BF)
    h_ref[...] = h
    low = low_half(h.shape[0])
    for part in range(3):
        for block in range(D // 256):
            at = part * D + block * 256
            y = dot(h, full[:, at : at + 256], NN) + bias_ref[:, at : at + 256]
            if part == 2:
                qkv_ref[2, :, block * 256 : block * 256 + 256] = y.astype(BF)
                continue
            gain = (qgain_ref, kgain_ref)[part][...]
            for half in range(2):
                tile = y[:, half * PAIR : half * PAIR + PAIR]
                cols = slice(block * 256 + half * PAIR, block * 256 + half * PAIR + PAIR)
                c = tile - pair_mean(tile, low)
                r = lax.rsqrt(pair_mean(c * c, low) + EPS)
                normed = (c * r * gain).astype(BF)
                qkv_ref[part, :, cols] = normed * BF(0.125) if part == 0 else normed
                rstd_ref[part, :, cols] = r


def front(x, gain, shift, pieces, bias, qgain, kgain):
    tokens = x.shape[0]
    row = pl.BlockSpec((ROWS, D), lambda i: (i, 0))
    return pl.pallas_call(
        functools.partial(front_body, len(pieces)),
        grid=(tokens // ROWS,),
        in_specs=[row, whole((1, D)), whole((1, D))]
        + [ANY] * len(pieces)
        + [whole((1, 3 * D)), whole((1, PAIR)), whole((1, PAIR))],
        out_specs=[
            row,
            pl.BlockSpec((3, ROWS, D), lambda i: (0, i, 0)),
            pl.BlockSpec((2, ROWS, D), lambda i: (0, i, 0)),
        ],
        out_shape=[
            jax.ShapeDtypeStruct((tokens, D), BF),
            jax.ShapeDtypeStruct((3, tokens, D), BF),
            jax.ShapeDtypeStruct((2, tokens, D), F32),
        ],
        scratch_shapes=[pltpu.VMEM((D, 3 * D), BF), pltpu.SemaphoreType.DMA((len(pieces),))],
        compiler_params=params(),
        cost_estimate=cost(2 * tokens * D * 3 * D, 18 * tokens * D, tokens),
        name="front",
    )(x, gain, shift, *pieces, bias, qgain, kgain)


def attend_body(q_ref, k_ref, v_ref, segq_ref, segk_ref, o_ref, lse_ref):
    tokens = o_ref.shape[0]
    low = low_half(tokens)
    keys = jnp.concatenate([k_ref[0], segk_ref[...]], axis=1)
    values = v_ref[0]
    one = jnp.ones_like(values)
    values_a = jnp.where(low, values, one)
    values_b = jnp.where(low, one, values)
    low_rows = low_half(ROWS)
    for block in range(tokens // ROWS):
        rows = slice(block * ROWS, block * ROWS + ROWS)
        q = q_ref[0, rows, :]
        seg = segq_ref[rows, :]
        zero = jnp.zeros_like(q)
        sa = dot(jnp.concatenate([jnp.where(low_rows, q, zero), seg], axis=1), keys, NT)
        acc_a = dot(jnp.exp2(sa * LOG2E).astype(BF), values_a, NN)
        sb = dot(jnp.concatenate([jnp.where(low_rows, zero, q), seg], axis=1), keys, NT)
        acc_b = dot(jnp.exp2(sb * LOG2E).astype(BF), values_b, NN)
        top = jnp.where(low_rows, acc_a, acc_b)
        total = pltpu.roll(jnp.where(low_rows, acc_b, acc_a), HD, 1)
        total = jnp.where(total > 0, total, 1.0)
        o_ref[rows, :] = (top / total).astype(BF)
        lse_ref[rows, :] = jnp.log(total)


def attend(qkv, segq, segk):
    tokens = qkv.shape[1]

    def part(which):
        return pl.BlockSpec((1, tokens, PAIR), lambda i: (which, 0, i))

    col = pl.BlockSpec((tokens, PAIR), lambda i: (0, i))
    return pl.pallas_call(
        attend_body,
        grid=(PAIRS,),
        in_specs=[part(0), part(1), part(2), whole((tokens, PAIR)), whole((tokens, PAIR))],
        out_specs=[col, col],
        out_shape=[
            jax.ShapeDtypeStruct((tokens, D), BF),
            jax.ShapeDtypeStruct((tokens, D), F32),
        ],
        compiler_params=params(),
        cost_estimate=cost(
            HEADS * tokens * tokens * 256 * 6, 10 * tokens * D, HEADS * tokens * tokens
        ),
        name="attend",
    )(qkv, qkv, qkv, segq, segk)


def middle_body(count, *refs):
    o_ref, x_ref = refs[:2]
    pieces = refs[2 : 2 + count]
    bias_ref, gain_ref, shift_ref, x1_ref, h_ref, full, sems = refs[2 + count :]

    @pl.when(pl.program_id(0) == 0)
    def _():
        for item in fetch(pieces, full, sems):
            item.wait()

    x1 = x_ref[...].astype(F32) + dot(o_ref[...], full[...], NN) + bias_ref[...]
    x1_ref[...] = x1
    center, rstd = stats(x1)
    h_ref[...] = (center * rstd * gain_ref[...] + shift_ref[...]).astype(BF)


def middle(o, x, pieces, bias, gain, shift):
    tokens = x.shape[0]
    row = pl.BlockSpec((ROWS, D), lambda i: (i, 0))
    return pl.pallas_call(
        functools.partial(middle_body, len(pieces)),
        grid=(tokens // ROWS,),
        in_specs=[row, row] + [ANY] * len(pieces) + [whole((1, D))] * 3,
        out_specs=[row, row],
        out_shape=[
            jax.ShapeDtypeStruct((tokens, D), F32),
            jax.ShapeDtypeStruct((tokens, D), BF),
        ],
        scratch_shapes=[pltpu.VMEM((D, D), BF), pltpu.SemaphoreType.DMA((len(pieces),))],
        compiler_params=params(),
        cost_estimate=cost(2 * tokens * D * D, 10 * tokens * D, tokens),
        name="middle",
    )(o, x, *pieces, bias, gain, shift)


def mlp_body(count, *refs):
    h_ref, x1_ref, valid_ref, gout_ref = refs[:4]
    ups = refs[4 : 4 + count]
    downs = refs[4 + count : 4 + 2 * count]
    (
        ubias_ref,
        dbias_ref,
        gain_ref,
        out_ref,
        gx1_ref,
        ga_ref,
        dup_ref,
        ddown_ref,
        dubias_ref,
        dvec_ref,
        up,
        down,
        acc,
        gh,
        gm,
        ht,
        act,
        gu,
        sems,
    ) = refs[4 + 2 * count :]
    tokens = h_ref.shape[0]
    blocks = tokens // ROWS
    step = pl.program_id(0)

    @pl.when(step == 0)
    def _():
        copies = fetch(ups, up, sems.at[0]) + fetch(downs, down, sems.at[1])
        ht[...] = h_ref[...].T
        gm[...] = jnp.where(valid_ref[...] >= 0, gout_ref[...].astype(F32), 0.0).astype(BF)
        acc[...] = jnp.zeros_like(acc)
        gh[...] = jnp.zeros_like(gh)
        for item in copies:
            item.wait()

    start = pl.multiple_of(step * FBLOCK, FBLOCK)
    cols = pl.ds(start, FBLOCK)
    ubias = ubias_ref[...]

    def rows_step(block, total):
        rows = pl.ds(pl.multiple_of(block * ROWS, ROWS), ROWS)
        u = dot(h_ref[rows, :], up[:, cols], NN) + ubias
        phi = 0.5 * (1.0 + lax.erf(u * math.sqrt(0.5)))
        a = (u * phi).astype(BF)
        act[rows, :] = a
        acc[rows, :] += dot(a, down[cols, :], NN)
        slope = phi + u * (jnp.exp2(u * u * (-0.5 * LOG2E)) * (1.0 / math.sqrt(2.0 * math.pi)))
        g = (slope * dot(gm[rows, :], down[cols, :], NT)).astype(BF)
        gu[rows, :] = g
        gh[rows, :] += dot(g, up[:, cols], NT)
        return total + jnp.sum(g.astype(F32), axis=0, keepdims=True)

    dubias_ref[...] = lax.fori_loop(0, blocks, rows_step, jnp.zeros((1, FBLOCK), F32))
    ddown_ref[...] = dot(act[...], gm[...], TN).astype(BF)
    dup_ref[...] = dot(ht[...], gu[...], NN).astype(BF)

    @pl.when(step == pl.num_programs(0) - 1)
    def _():
        gain = gain_ref[...]
        dbias = dbias_ref[...]

        def finish(block, totals):
            dgain, dshift, dob, ddb = totals
            rows = pl.ds(pl.multiple_of(block * ROWS, ROWS), ROWS)
            x1 = x1_ref[rows, :]
            valid = valid_ref[rows, :] >= 0
            out_ref[rows, :] = jnp.where(valid, x1 + acc[rows, :] + dbias, 0.0).astype(BF)
            center, rstd = stats(x1)
            hat = center * rstd
            g = gh[rows, :]
            t = g * gain
            gy = gm[rows, :].astype(F32)
            gx1 = gy + rstd * (
                t
                - jnp.mean(t, axis=-1, keepdims=True)
                - hat * jnp.mean(t * hat, axis=-1, keepdims=True)
            )
            gx1_ref[rows, :] = gx1
            low = gx1.astype(BF)
            ga_ref[rows, :] = low
            return (
                dgain + jnp.sum(g * hat, axis=0, keepdims=True),
                dshift + jnp.sum(g, axis=0, keepdims=True),
                dob + jnp.sum(low.astype(F32), axis=0, keepdims=True),
                ddb + jnp.sum(gy, axis=0, keepdims=True),
            )

        zero = jnp.zeros((1, D), F32)
        totals = lax.fori_loop(0, blocks, finish, (zero,) * 4)
        for place, total in enumerate(totals):
            dvec_ref[place : place + 1, :] = total


def mlp(h, x1, segments, gout, ups, downs, ubias, dbias, gain):
    tokens = h.shape[0]
    count = len(ups)
    hidden = ubias.shape[1]
    act = whole((tokens, D))
    return pl.pallas_call(
        functools.partial(mlp_body, count),
        grid=(hidden // FBLOCK,),
        in_specs=[act, act, whole((tokens, 1)), act]
        + [ANY] * (2 * count)
        + [pl.BlockSpec((1, FBLOCK), lambda i: (0, i)), whole((1, D)), whole((1, D))],
        out_specs=[
            act,
            act,
            act,
            pl.BlockSpec((D, FBLOCK), lambda i: (0, i)),
            pl.BlockSpec((FBLOCK, D), lambda i: (i, 0)),
            pl.BlockSpec((1, FBLOCK), lambda i: (0, i)),
            whole((4, D)),
        ],
        out_shape=[
            jax.ShapeDtypeStruct((tokens, D), BF),
            jax.ShapeDtypeStruct((tokens, D), F32),
            jax.ShapeDtypeStruct((tokens, D), BF),
            jax.ShapeDtypeStruct((D, hidden), BF),
            jax.ShapeDtypeStruct((hidden, D), BF),
            jax.ShapeDtypeStruct((1, hidden), F32),
            jax.ShapeDtypeStruct((4, D), F32),
        ],
        scratch_shapes=[
            pltpu.VMEM((D, hidden), BF),
            pltpu.VMEM((hidden, D), BF),
            pltpu.VMEM((tokens, D), F32),
            pltpu.VMEM((tokens, D), F32),
            pltpu.VMEM((tokens, D), BF),
            pltpu.VMEM((D, tokens), BF),
            pltpu.VMEM((tokens, FBLOCK), BF),
            pltpu.VMEM((tokens, FBLOCK), BF),
            pltpu.SemaphoreType.DMA((2, count)),
        ],
        compiler_params=params(),
        cost_estimate=cost(12 * tokens * D * hidden, 30 * tokens * D, 2 * tokens * hidden),
        name="mlp",
    )(h, x1, segments, gout, *ups, *downs, ubias, dbias, gain)


def outback_body(count, *refs):
    o_ref, ga_ref = refs[:2]
    pieces = refs[2 : 2 + count]
    go_ref, dout_ref, full, sems = refs[2 + count :]
    step = pl.program_id(0)

    @pl.when(step == 0)
    def _():
        for item in fetch(pieces, full, sems):
            item.wait()

    start = pl.multiple_of(step * 256, 256)
    go_ref[...] = dot(ga_ref[...], full[pl.ds(start, 256), :], NT).astype(BF)
    dout_ref[...] = dot(o_ref[...], ga_ref[...], TN).astype(BF)


def outback(o, ga, pieces):
    tokens = o.shape[0]
    col = pl.BlockSpec((tokens, 256), lambda i: (0, i))
    return pl.pallas_call(
        functools.partial(outback_body, len(pieces)),
        grid=(D // 256,),
        in_specs=[col, whole((tokens, D))] + [ANY] * len(pieces),
        out_specs=[col, pl.BlockSpec((256, D), lambda i: (i, 0))],
        out_shape=[jax.ShapeDtypeStruct((tokens, D), BF), jax.ShapeDtypeStruct((D, D), BF)],
        scratch_shapes=[pltpu.VMEM((D, D), BF), pltpu.SemaphoreType.DMA((len(pieces),))],
        compiler_params=params(),
        cost_estimate=cost(4 * tokens * D * D, 6 * tokens * D),
        name="outback",
    )(o, ga, *pieces)


def split3(values):
    first = values.astype(BF)
    rest = values - first.astype(F32)
    second = rest.astype(BF)
    third = (rest - second.astype(F32)).astype(BF)
    return first, second, third


def attback_body(
    q_ref,
    k_ref,
    v_ref,
    segq_ref,
    segk_ref,
    o_ref,
    lse_ref,
    go_ref,
    rq_ref,
    rk_ref,
    qgain_ref,
    kgain_ref,
    g_ref,
    dgain_ref,
    gqt,
    gk,
    gv,
):
    tokens = o_ref.shape[0]
    low = low_half(tokens)
    lane = lax.broadcasted_iota(jnp.int32, (tokens, PAIR), 1)
    q, k, v, go = q_ref[0], k_ref[0], v_ref[0], go_ref[...]
    zero = jnp.zeros_like(q)
    product = o_ref[...].astype(F32) * go.astype(F32)
    minus = jnp.where(lane < 3, BF(-1.0), zero)
    for head in range(2):
        mine = low if head == 0 else jnp.logical_not(low)
        at = head * HD
        hi, mid, lo = split3(lse_ref[:, at : at + 1])
        segq = segq_ref[...]
        for place, piece in ((65, hi), (66, mid), (67, lo)):
            segq = jnp.where(lane == place, piece, segq)
        q_mine = jnp.where(mine, q, zero)
        go_mine = jnp.where(mine, go, zero)
        k_mine = jnp.where(mine, k, zero)
        q_wide = jnp.concatenate([q_mine, segq], axis=1)
        inner = jnp.sum(jnp.where(mine, product, 0.0), axis=-1, keepdims=True)
        extra = zero
        for place, piece in enumerate(split3(inner)):
            extra = jnp.where(lane == place, piece, extra)
        go_wide = jnp.concatenate([go_mine, extra], axis=1)
        for block in range(tokens // ROWS):
            rows = slice(block * ROWS, block * ROWS + ROWS)
            k_wide = jnp.concatenate([k[rows], segk_ref[rows, :]], axis=1)
            v_wide = jnp.concatenate([v[rows], minus[rows]], axis=1)
            p = jnp.exp2(dot(k_wide, q_wide, NT) * LOG2E)
            gs = (p * dot(v_wide, go_wide, NT)).astype(BF)
            value_part = dot(p.astype(BF), go_mine, NN)
            key_part = dot(gs, q_mine, NN)
            query_part = dot(k_mine[rows], gs, TN)
            if head == 0:
                gv[rows, :] = value_part
                gk[rows, :] = key_part
            else:
                gv[rows, :] += value_part
                gk[rows, :] += key_part
            if head == 0 and block == 0:
                gqt[...] = query_part
            else:
                gqt[...] += query_part
    g_ref[2] = gv[...].astype(BF)
    gq = gqt[...].T * 0.125
    pieces = (
        (0, gq, q.astype(F32) * 8.0, qgain_ref[...], rq_ref[0]),
        (1, gk[...], k.astype(F32), kgain_ref[...], rk_ref[0]),
    )
    for part, grad, normed, gain, rstd in pieces:
        hat = normed / gain
        t = grad * gain
        dgain_ref[part] = jnp.broadcast_to(jnp.sum(grad * hat, axis=0, keepdims=True), (8, PAIR))
        g_ref[part] = (rstd * (t - pair_mean(t, low) - hat * pair_mean(t * hat, low))).astype(BF)


def attback(qkv, segq, segk, o, lse, go, rstd, qgain, kgain):
    tokens = o.shape[0]

    def part(which):
        return pl.BlockSpec((1, tokens, PAIR), lambda i: (which, 0, i))

    col = pl.BlockSpec((tokens, PAIR), lambda i: (0, i))
    seg = whole((tokens, PAIR))
    return pl.pallas_call(
        attback_body,
        grid=(PAIRS,),
        in_specs=[part(0), part(1), part(2), seg, seg, col, col, col, part(0), part(1)]
        + [whole((1, PAIR))] * 2,
        out_specs=[
            pl.BlockSpec((3, tokens, PAIR), lambda i: (0, 0, i)),
            pl.BlockSpec((2, 8, PAIR), lambda i: (0, 0, i)),
        ],
        out_shape=[
            jax.ShapeDtypeStruct((3, tokens, D), BF),
            jax.ShapeDtypeStruct((2, 8, D), F32),
        ],
        scratch_shapes=[
            pltpu.VMEM((PAIR, tokens), F32),
            pltpu.VMEM((tokens, PAIR), F32),
            pltpu.VMEM((tokens, PAIR), F32),
        ],
        compiler_params=params(),
        cost_estimate=cost(
            HEADS * tokens * tokens * 256 * 10, 30 * tokens * D, HEADS * tokens * tokens
        ),
        name="attback",
    )(qkv, qkv, qkv, segq, segk, o, lse, go, rstd, rstd, qgain, kgain)


def qkvgrad_body(h_ref, g_ref, dw_ref, db_ref, ht):
    @pl.when(pl.program_id(0) == 0)
    def _():
        ht[...] = h_ref[...].T

    g = g_ref[0]
    dw_ref[...] = dot(ht[...], g, NN).astype(BF)
    db_ref[...] = jnp.sum(g.astype(F32), axis=0, keepdims=True)


def qkvgrad(h, g):
    tokens = h.shape[0]
    return pl.pallas_call(
        qkvgrad_body,
        grid=(3, 3),
        in_specs=[
            whole((tokens, D)),
            pl.BlockSpec((1, tokens, 256), lambda i, j: (i, 0, j)),
        ],
        out_specs=[
            pl.BlockSpec((D, 256), lambda i, j: (0, 3 * i + j)),
            pl.BlockSpec((1, 256), lambda i, j: (0, 3 * i + j)),
        ],
        out_shape=[
            jax.ShapeDtypeStruct((D, 3 * D), BF),
            jax.ShapeDtypeStruct((1, 3 * D), F32),
        ],
        scratch_shapes=[pltpu.VMEM((D, tokens), BF)],
        compiler_params=params("arbitrary", "arbitrary"),
        cost_estimate=cost(6 * tokens * D * D, 14 * tokens * D),
        name="qkvgrad",
    )(h, g)


def back_body(count, *refs):
    g_ref, x_ref, gx1_ref = refs[:3]
    pieces = refs[3 : 3 + count]
    gain_ref, gx_ref, dvec_ref, full, sems = refs[3 + count :]
    step = pl.program_id(0)

    @pl.when(step == 0)
    def _():
        for item in fetch(pieces, full, sems):
            item.wait()
        dvec_ref[...] = jnp.zeros_like(dvec_ref)

    g = dot(g_ref[0], full[:, :D], NT)
    g += dot(g_ref[1], full[:, D : 2 * D], NT)
    g += dot(g_ref[2], full[:, 2 * D :], NT)
    center, rstd = stats(x_ref[...].astype(F32))
    hat = center * rstd
    t = g * gain_ref[...]
    gx = gx1_ref[...] + rstd * (
        t - jnp.mean(t, axis=-1, keepdims=True) - hat * jnp.mean(t * hat, axis=-1, keepdims=True)
    )
    gx_ref[...] = gx.astype(BF)
    dvec_ref[0:1, :] += jnp.sum(g * hat, axis=0, keepdims=True)
    dvec_ref[1:2, :] += jnp.sum(g, axis=0, keepdims=True)


def back(g, x, gx1, pieces, gain):
    tokens = x.shape[0]
    row = pl.BlockSpec((ROWS, D), lambda i: (i, 0))
    return pl.pallas_call(
        functools.partial(back_body, len(pieces)),
        grid=(tokens // ROWS,),
        in_specs=[pl.BlockSpec((3, ROWS, D), lambda i: (0, i, 0)), row, row]
        + [ANY] * len(pieces)
        + [whole((1, D))],
        out_specs=[row, whole((2, D))],
        out_shape=[jax.ShapeDtypeStruct((tokens, D), BF), jax.ShapeDtypeStruct((2, D), F32)],
        scratch_shapes=[pltpu.VMEM((D, 3 * D), BF), pltpu.SemaphoreType.DMA((len(pieces),))],
        compiler_params=params(),
        cost_estimate=cost(6 * tokens * D * D, 16 * tokens * D, tokens),
        name="back",
    )(g, x, gx1, *pieces, gain)


def swap(values, axis, mask, size):
    return lax.ppermute(values, axis, [(i, i ^ mask) for i in range(size)])


def bits_of(size):
    return [1 << b for b in range(size.bit_length() - 1)]


def gather_shards(shard, size):
    held = [shard]
    for mask in reversed(bits_of(size)):
        held = held + [swap(item, "fsdp", mask, size) for item in held]
    order = [0]
    for mask in reversed(bits_of(size)):
        order = order + [place ^ mask for place in order]
    placed = [None] * size
    for place, item in zip(order, held):
        placed[place] = item
    return placed


def reduce_grad(grad, order, sizes):
    fsdp, dp = sizes["fsdp"], sizes["dp"]
    rows, columns = grad.shape
    names = [("fsdp", m) for m in reversed(bits_of(fsdp))] + [
        ("dp", m) for m in reversed(bits_of(dp))
    ]
    held = grad.reshape((2,) * len(names) + (rows // fsdp // dp, columns))
    undo = []
    for step in order:
        axis, mask = step
        place = names.index(step)
        mine = (lax.axis_index(axis) // mask) % 2
        send = lax.dynamic_index_in_dim(held, 1 - mine, place, keepdims=False)
        keep = lax.dynamic_index_in_dim(held, mine, place, keepdims=False)
        held = (
            keep.astype(F32) + swap(send, axis, mask, sizes[axis]).astype(F32)
        ).astype(BF)
        names.pop(place)
        if axis == "dp":
            place -= sum(name == "fsdp" for name, _ in names[:place])
            undo.append((axis, mask, place, mine))
    for axis, mask, place, mine in reversed(undo):
        other = swap(held, axis, mask, sizes[axis])
        first = jnp.where(mine == 0, held, other)
        second = jnp.where(mine == 0, other, held)
        held = jnp.stack([first, second], axis=place)
    return held.reshape(rows // fsdp, columns).astype(F32)


def reduce_small(grad, sizes):
    held = grad.reshape((2,) * len(bits_of(sizes["fsdp"])) + (grad.shape[1],))
    for mask in reversed(bits_of(sizes["fsdp"])):
        mine = (lax.axis_index("fsdp") // mask) % 2
        send = lax.dynamic_index_in_dim(held, 1 - mine, 0, keepdims=False)
        keep = lax.dynamic_index_in_dim(held, mine, 0, keepdims=False)
        held = keep + swap(send, "fsdp", mask, sizes["fsdp"])
    for mask in bits_of(sizes["dp"]):
        held = held + swap(held, "dp", mask, sizes["dp"])
    return held


def local(sizes, *arguments):
    (
        block_input,
        segment_ids,
        norm1_gain,
        norm1_bias,
        qkv_weight,
        qkv_bias,
        query_gain,
        key_gain,
        out_weight,
        out_bias,
        norm2_gain,
        norm2_bias,
        up_weight,
        up_bias,
        down_weight,
        down_bias,
        output_grad,
    ) = arguments
    fsdp = sizes["fsdp"]
    rank = lax.axis_index("fsdp")
    small_args = (
        norm1_gain,
        norm1_bias,
        qkv_bias,
        query_gain,
        key_gain,
        out_bias,
        norm2_gain,
        norm2_bias,
        up_bias,
        down_bias,
    )
    widths = [item.shape[0] for item in small_args]
    packed = jnp.stack(gather_shards(jnp.concatenate(small_args), fsdp))
    packed = packed[jnp.arange(fsdp) ^ rank].astype(F32)
    smalls = []
    at = 0
    for width in widths:
        smalls.append(packed[:, at : at + width].reshape(1, fsdp * width))
        at += width
    gain1, shift1, qkvb, qgain, kgain, outb, gain2, shift2, upb, downb = smalls
    qgain = jnp.concatenate([qgain, qgain], axis=1)
    kgain = jnp.concatenate([kgain, kgain], axis=1)
    qkv_pieces = gather_shards(qkv_weight, fsdp)
    out_pieces = gather_shards(out_weight, fsdp)
    up_pieces = gather_shards(up_weight, fsdp)
    down_pieces = gather_shards(down_weight, fsdp)

    lane = jnp.arange(PAIR)[None, :]
    seg_col = segment_ids[:, None]
    match = (seg_col == lane) & (lane < HD)
    segq = jnp.where(match, QMARK, jnp.where(lane == HD, 1.0, 0.0)).astype(BF)
    segk = jnp.where(
        match,
        KMARK,
        jnp.where(lane == HD, -QMARK * KMARK, jnp.where((lane > HD) & (lane <= HD + 3), -1.0, 0.0)),
    ).astype(BF)

    h1, qkv, rstd = front(block_input, gain1, shift1, qkv_pieces, qkvb, qgain, kgain)
    mixed, lse = attend(qkv, segq, segk)
    x1, h2 = middle(mixed, block_input, out_pieces, outb, gain2, shift2)
    output, gx1, ga, dup, ddown, dubias, dvec2 = mlp(
        h2, x1, seg_col, output_grad, up_pieces, down_pieces, upb, downb, gain2
    )
    go, dout = outback(mixed, ga, out_pieces)
    gqkv, dheads = attback(qkv, segq, segk, mixed, lse, go, rstd, qgain, kgain)
    dqkv, dqkvb = qkvgrad(h1, gqkv)
    input_grad, dvec1 = back(gqkv, block_input, gx1, qkv_pieces, gain1)

    f_bits = [("fsdp", m) for m in bits_of(fsdp)]
    d_bits = [("dp", m) for m in bits_of(sizes["dp"])]
    near, far = f_bits[:1], f_bits[1:]
    up_total = reduce_grad(dup, near + far + d_bits, sizes)
    down_total = reduce_grad(ddown, near + d_bits[:1] + far + d_bits[1:], sizes)
    out_total = reduce_grad(dout, near + d_bits[1:2] + d_bits[:1] + far + d_bits[2:], sizes)
    qkv_total = reduce_grad(dqkv, near + far + d_bits, sizes)

    dgains = dheads[:, 0, :].reshape(2, HEADS, HD).sum(axis=1)
    parts = (
        dvec1[0],
        dvec1[1],
        dqkvb,
        dgains[0],
        dgains[1],
        dvec2[2],
        dvec2[0],
        dvec2[1],
        dubias,
        dvec2[3],
    )
    small = reduce_small(
        jnp.concatenate([part.reshape(fsdp, -1) for part in parts], axis=1), sizes
    )
    shares = []
    at = 0
    for width in widths:
        shares.append(small[at : at + width])
        at += width
    n1g, n1b, qkvb_total, qg, kg, outb_total, n2g, n2b, upb_total, downb_total = shares
    return (
        output,
        input_grad,
        n1g,
        n1b,
        qkv_total,
        qkvb_total,
        qg,
        kg,
        out_total,
        outb_total,
        n2g,
        n2b,
        up_total,
        upb_total,
        down_total,
        downb_total,
    )


def solution(mesh):
    rows, shard = P(("dp", "fsdp"), None), P("fsdp")
    matrix = P("fsdp", None)
    placed = (
        (rows, P(("dp", "fsdp")), shard, shard, matrix, shard, shard, shard)
        + (matrix, shard, shard, shard, matrix, shard, matrix, shard, rows)
    )
    results = (
        (rows, rows, shard, shard, matrix, shard, shard, shard)
        + (matrix, shard, shard, shard, matrix, shard, matrix, shard)
    )
    return jax.shard_map(
        functools.partial(local, dict(mesh.shape)),
        mesh=mesh,
        in_specs=placed,
        out_specs=results,
        check_vma=False,
    )
```

```python
import functools
import math

import jax
import jax.numpy as jnp
from jax import lax
from jax.experimental import pallas as pl
from jax.experimental.pallas import tpu as pltpu
from jax.sharding import PartitionSpec as P

D = 768
HEADS = 12
HD = 64
PAIR = 128
PAIRS = HEADS // 2
EPS = 1e-06
BF = jnp.bfloat16
F32 = jnp.float32
LOG2E = 1.4426950408889634
ROWS = 256
QMARK = 16.0
KMARK = 12.0

NN = (((1,), (0,)), ((), ()))
NT = (((1,), (1,)), ((), ()))
TN = (((0,), (0,)), ((), ()))


def dot(left, right, dims):
    return lax.dot_general(left, right, dims, preferred_element_type=F32)


def params(*semantics):
    return pltpu.CompilerParams(
        dimension_semantics=semantics or ("arbitrary",), vmem_limit_bytes=60 * 1024 * 1024
    )


def cost(flops, nbytes, trans=0):
    return pl.CostEstimate(flops=int(flops), bytes_accessed=int(nbytes), transcendentals=int(trans))


def whole(shape):
    return pl.BlockSpec(shape, lambda *_: (0,) * len(shape))


def single(shape):
    return pl.BlockSpec(shape, lambda *_: (0,) * len(shape), pipeline_mode=pl.Buffered(1))


ANY = pl.BlockSpec(memory_space=pl.ANY)


def flip(rank, distance):
    bit = 1
    while bit <= distance:
        if distance & bit:
            rank = rank + bit * (1 - 2 * ((rank // bit) % 2))
        bit *= 2
    return rank


def fetch(pieces, full, sems):
    rank = lax.axis_index("fsdp")
    rows = full.shape[0] // len(pieces)
    copies = []
    for distance, piece in enumerate(pieces):
        start = pl.multiple_of(flip(rank, distance) * rows, rows)
        copies.append(
            pltpu.make_async_copy(piece, full.at[pl.ds(start, rows)], sems.at[distance])
        )
    for item in copies:
        item.start()
    return copies


def stats(values):
    center = values - jnp.mean(values, axis=-1, keepdims=True)
    rstd = lax.rsqrt(jnp.mean(center * center, axis=-1, keepdims=True) + EPS)
    return center, rstd


def low_half(rows):
    return lax.broadcasted_iota(jnp.int32, (rows, PAIR), 1) < HD


def pair_mean(values, low):
    first = jnp.sum(jnp.where(low, values, 0.0), axis=-1, keepdims=True)
    second = jnp.sum(jnp.where(low, 0.0, values), axis=-1, keepdims=True)
    return jnp.where(low, first, second) * (1.0 / HD)


def front_body(count, *refs):
    x_ref, gain_ref, shift_ref = refs[:3]
    pieces = refs[3 : 3 + count]
    bias_ref, qgain_ref, kgain_ref, h_ref, qkv_ref, rstd_ref, full, sems = refs[3 + count :]

    @pl.when(pl.program_id(0) == 0)
    def _():
        for item in fetch(pieces, full, sems):
            item.wait()

    center, rstd = stats(x_ref[...].astype(F32))
    h = (center * rstd * gain_ref[...] + shift_ref[...]).astype(BF)
    h_ref[...] = h
    low = low_half(h.shape[0])
    for part in range(3):
        for block in range(D // 256):
            at = part * D + block * 256
            y = dot(h, full[:, at : at + 256], NN) + bias_ref[:, at : at + 256]
            if part == 2:
                qkv_ref[2, :, block * 256 : block * 256 + 256] = y.astype(BF)
                continue
            gain = (qgain_ref, kgain_ref)[part][...]
            for half in range(2):
                tile = y[:, half * PAIR : half * PAIR + PAIR]
                cols = slice(block * 256 + half * PAIR, block * 256 + half * PAIR + PAIR)
                c = tile - pair_mean(tile, low)
                r = lax.rsqrt(pair_mean(c * c, low) + EPS)
                normed = (c * r * gain).astype(BF)
                qkv_ref[part, :, cols] = normed * BF(0.125) if part == 0 else normed
                rstd_ref[part, :, cols] = r


def front(x, gain, shift, pieces, bias, qgain, kgain):
    tokens = x.shape[0]
    row = pl.BlockSpec((ROWS, D), lambda i: (i, 0))
    return pl.pallas_call(
        functools.partial(front_body, len(pieces)),
        grid=(tokens // ROWS,),
        in_specs=[row, whole((1, D)), whole((1, D))]
        + [ANY] * len(pieces)
        + [whole((1, 3 * D)), whole((1, PAIR)), whole((1, PAIR))],
        out_specs=[
            row,
            pl.BlockSpec((3, ROWS, D), lambda i: (0, i, 0)),
            pl.BlockSpec((2, ROWS, D), lambda i: (0, i, 0)),
        ],
        out_shape=[
            jax.ShapeDtypeStruct((tokens, D), BF),
            jax.ShapeDtypeStruct((3, tokens, D), BF),
            jax.ShapeDtypeStruct((2, tokens, D), F32),
        ],
        scratch_shapes=[pltpu.VMEM((D, 3 * D), BF), pltpu.SemaphoreType.DMA((len(pieces),))],
        compiler_params=params(),
        cost_estimate=cost(2 * tokens * D * 3 * D, 18 * tokens * D, tokens),
        name="front",
    )(x, gain, shift, *pieces, bias, qgain, kgain)


def attend_body(q_ref, k_ref, v_ref, segq_ref, segk_ref, o_ref, lse_ref):
    tokens = o_ref.shape[0]
    low = low_half(tokens)
    keys = jnp.concatenate([k_ref[0], segk_ref[...]], axis=1)
    values = v_ref[0]
    one = jnp.ones_like(values)
    values_a = jnp.where(low, values, one)
    values_b = jnp.where(low, one, values)
    low_rows = low_half(ROWS)
    for block in range(tokens // ROWS):
        rows = slice(block * ROWS, block * ROWS + ROWS)
        q = q_ref[0, rows, :]
        seg = segq_ref[rows, :]
        zero = jnp.zeros_like(q)
        sa = dot(jnp.concatenate([jnp.where(low_rows, q, zero), seg], axis=1), keys, NT)
        acc_a = dot(jnp.exp2(sa * LOG2E).astype(BF), values_a, NN)
        sb = dot(jnp.concatenate([jnp.where(low_rows, zero, q), seg], axis=1), keys, NT)
        acc_b = dot(jnp.exp2(sb * LOG2E).astype(BF), values_b, NN)
        top = jnp.where(low_rows, acc_a, acc_b)
        total = pltpu.roll(jnp.where(low_rows, acc_b, acc_a), HD, 1)
        total = jnp.where(total > 0, total, 1.0)
        o_ref[rows, :] = (top / total).astype(BF)
        lse_ref[rows, :] = jnp.log(total)


def attend(qkv, segq, segk):
    tokens = qkv.shape[1]

    def part(which):
        return pl.BlockSpec((1, tokens, PAIR), lambda i: (which, 0, i))

    col = pl.BlockSpec((tokens, PAIR), lambda i: (0, i))
    return pl.pallas_call(
        attend_body,
        grid=(PAIRS,),
        in_specs=[part(0), part(1), part(2), whole((tokens, PAIR)), whole((tokens, PAIR))],
        out_specs=[col, col],
        out_shape=[
            jax.ShapeDtypeStruct((tokens, D), BF),
            jax.ShapeDtypeStruct((tokens, D), F32),
        ],
        compiler_params=params(),
        cost_estimate=cost(
            HEADS * tokens * tokens * 256 * 6, 10 * tokens * D, HEADS * tokens * tokens
        ),
        name="attend",
    )(qkv, qkv, qkv, segq, segk)


def middle_body(count, *refs):
    o_ref, x_ref = refs[:2]
    pieces = refs[2 : 2 + count]
    bias_ref, gain_ref, shift_ref, x1_ref, h_ref, full, sems = refs[2 + count :]

    @pl.when(pl.program_id(0) == 0)
    def _():
        for item in fetch(pieces, full, sems):
            item.wait()

    x1 = x_ref[...].astype(F32) + dot(o_ref[...], full[...], NN) + bias_ref[...]
    x1_ref[...] = x1
    center, rstd = stats(x1)
    h_ref[...] = (center * rstd * gain_ref[...] + shift_ref[...]).astype(BF)


def middle(o, x, pieces, bias, gain, shift):
    tokens = x.shape[0]
    row = pl.BlockSpec((ROWS, D), lambda i: (i, 0))
    return pl.pallas_call(
        functools.partial(middle_body, len(pieces)),
        grid=(tokens // ROWS,),
        in_specs=[row, row] + [ANY] * len(pieces) + [whole((1, D))] * 3,
        out_specs=[row, row],
        out_shape=[
            jax.ShapeDtypeStruct((tokens, D), F32),
            jax.ShapeDtypeStruct((tokens, D), BF),
        ],
        scratch_shapes=[pltpu.VMEM((D, D), BF), pltpu.SemaphoreType.DMA((len(pieces),))],
        compiler_params=params(),
        cost_estimate=cost(2 * tokens * D * D, 10 * tokens * D, tokens),
        name="middle",
    )(o, x, *pieces, bias, gain, shift)


def mlp_body(count, *refs):
    h_ref, x1_ref, valid_ref, gout_ref = refs[:4]
    ups = refs[4 : 4 + count]
    downs = refs[4 + count : 4 + 2 * count]
    (
        ubias_ref,
        dbias_ref,
        gain_ref,
        out_ref,
        gx1_ref,
        ga_ref,
        dup_ref,
        ddown_ref,
        dubias_ref,
        dvec_ref,
        up,
        down,
        acc,
        gh,
        gm,
        ht,
        act,
        gu,
        sems,
    ) = refs[4 + 2 * count :]
    tokens = h_ref.shape[0]
    fblock = act.shape[1]
    blocks = tokens // ROWS
    step = pl.program_id(0)

    @pl.when(step == 0)
    def _():
        copies = fetch(ups, up, sems.at[0]) + fetch(downs, down, sems.at[1])
        ht[...] = h_ref[...].T
        gm[...] = jnp.where(valid_ref[...] >= 0, gout_ref[...].astype(F32), 0.0).astype(BF)
        acc[...] = jnp.zeros_like(acc)
        gh[...] = jnp.zeros_like(gh)
        for item in copies:
            item.wait()

    start = pl.multiple_of(step * fblock, fblock)
    cols = pl.ds(start, fblock)
    ubias = ubias_ref[...]

    def rows_step(block, total):
        rows = pl.ds(pl.multiple_of(block * ROWS, ROWS), ROWS)
        u = dot(h_ref[rows, :], up[:, cols], NN) + ubias
        phi = 0.5 * (1.0 + lax.erf(u * math.sqrt(0.5)))
        a = (u * phi).astype(BF)
        act[rows, :] = a
        acc[rows, :] += dot(a, down[cols, :], NN)
        slope = phi + u * (jnp.exp2(u * u * (-0.5 * LOG2E)) * (1.0 / math.sqrt(2.0 * math.pi)))
        g = (slope * dot(gm[rows, :], down[cols, :], NT)).astype(BF)
        gu[rows, :] = g
        gh[rows, :] += dot(g, up[:, cols], NT)
        return total + jnp.sum(g.astype(F32), axis=0, keepdims=True)

    dubias_ref[...] = lax.fori_loop(0, blocks, rows_step, jnp.zeros((1, fblock), F32))
    for at in range(0, D, 256):
        block = slice(at, at + 256)
        ddown = dot(act[...], gm[:, block], TN).astype(BF)
        ddown_ref[..., block] = ddown.reshape(ddown_ref.shape[:-1] + (256,))
        dup = dot(ht[...], gu[:, block], NN).astype(BF)
        dup_ref[..., block] = dup.reshape(dup_ref.shape[:-1] + (256,))

    @pl.when(step == pl.num_programs(0) - 1)
    def _():
        gain = gain_ref[...]
        dbias = dbias_ref[...]

        def finish(block, totals):
            dgain, dshift, dob, ddb = totals
            rows = pl.ds(pl.multiple_of(block * ROWS, ROWS), ROWS)
            x1 = x1_ref[rows, :]
            valid = valid_ref[rows, :] >= 0
            out_ref[rows, :] = jnp.where(valid, x1 + acc[rows, :] + dbias, 0.0).astype(BF)
            center, rstd = stats(x1)
            hat = center * rstd
            g = gh[rows, :]
            t = g * gain
            gy = gm[rows, :].astype(F32)
            gx1 = gy + rstd * (
                t
                - jnp.mean(t, axis=-1, keepdims=True)
                - hat * jnp.mean(t * hat, axis=-1, keepdims=True)
            )
            gx1_ref[rows, :] = gx1
            low = gx1.astype(BF)
            ga_ref[rows, :] = low
            return (
                dgain + jnp.sum(g * hat, axis=0, keepdims=True),
                dshift + jnp.sum(g, axis=0, keepdims=True),
                dob + jnp.sum(low.astype(F32), axis=0, keepdims=True),
                ddb + jnp.sum(gy, axis=0, keepdims=True),
            )

        zero = jnp.zeros((1, D), F32)
        totals = lax.fori_loop(0, blocks, finish, (zero,) * 4)
        for place, total in enumerate(totals):
            dvec_ref[place : place + 1, :] = total


def mlp(h, x1, segments, gout, ups, downs, ubias, dbias, gain):
    tokens = h.shape[0]
    count = len(ups)
    hidden = ubias.shape[1]
    fblock = hidden // count
    grads = jax.ShapeDtypeStruct((hidden // fblock, count, D // count, D), BF)
    act = single((tokens, D))
    return pl.pallas_call(
        functools.partial(mlp_body, count),
        grid=(hidden // fblock,),
        in_specs=[act, act, single((tokens, 1)), act]
        + [ANY] * (2 * count)
        + [pl.BlockSpec((1, fblock), lambda i: (0, i)), whole((1, D)), whole((1, D))],
        out_specs=[
            act,
            act,
            act,
            pl.BlockSpec((1, count, D // count, D), lambda i: (i, 0, 0, 0)),
            pl.BlockSpec((hidden // fblock, 1, D // count, D), lambda i: (0, i, 0, 0)),
            pl.BlockSpec((1, fblock), lambda i: (0, i)),
            whole((4, D)),
        ],
        out_shape=[
            jax.ShapeDtypeStruct((tokens, D), BF),
            jax.ShapeDtypeStruct((tokens, D), F32),
            jax.ShapeDtypeStruct((tokens, D), BF),
            grads,
            grads,
            jax.ShapeDtypeStruct((1, hidden), F32),
            jax.ShapeDtypeStruct((4, D), F32),
        ],
        scratch_shapes=[
            pltpu.VMEM((D, hidden), BF),
            pltpu.VMEM((hidden, D), BF),
            pltpu.VMEM((tokens, D), F32),
            pltpu.VMEM((tokens, D), F32),
            pltpu.VMEM((tokens, D), BF),
            pltpu.VMEM((D, tokens), BF),
            pltpu.VMEM((tokens, fblock), BF),
            pltpu.VMEM((tokens, fblock), BF),
            pltpu.SemaphoreType.DMA((2, count)),
        ],
        compiler_params=params(),
        cost_estimate=cost(12 * tokens * D * hidden, 30 * tokens * D, 2 * tokens * hidden),
        name="mlp",
    )(h, x1, segments, gout, *ups, *downs, ubias, dbias, gain)


def outback_body(count, *refs):
    o_ref, ga_ref = refs[:2]
    pieces = refs[2 : 2 + count]
    go_ref, dout_ref, full, sems = refs[2 + count :]
    step = pl.program_id(0)

    @pl.when(step == 0)
    def _():
        for item in fetch(pieces, full, sems):
            item.wait()

    start = pl.multiple_of(step * 256, 256)
    go_ref[...] = dot(ga_ref[...], full[pl.ds(start, 256), :], NT).astype(BF)
    dout_ref[...] = dot(o_ref[...], ga_ref[...], TN).astype(BF)


def outback(o, ga, pieces):
    tokens = o.shape[0]
    col = pl.BlockSpec((tokens, 256), lambda i: (0, i))
    return pl.pallas_call(
        functools.partial(outback_body, len(pieces)),
        grid=(D // 256,),
        in_specs=[col, whole((tokens, D))] + [ANY] * len(pieces),
        out_specs=[col, pl.BlockSpec((256, D), lambda i: (i, 0))],
        out_shape=[jax.ShapeDtypeStruct((tokens, D), BF), jax.ShapeDtypeStruct((D, D), BF)],
        scratch_shapes=[pltpu.VMEM((D, D), BF), pltpu.SemaphoreType.DMA((len(pieces),))],
        compiler_params=params(),
        cost_estimate=cost(4 * tokens * D * D, 6 * tokens * D),
        name="outback",
    )(o, ga, *pieces)


def split3(values):
    first = values.astype(BF)
    rest = values - first.astype(F32)
    second = rest.astype(BF)
    third = (rest - second.astype(F32)).astype(BF)
    return first, second, third


def attback_body(
    q_ref,
    k_ref,
    v_ref,
    segq_ref,
    segk_ref,
    o_ref,
    lse_ref,
    go_ref,
    rq_ref,
    rk_ref,
    qgain_ref,
    kgain_ref,
    g_ref,
    dgain_ref,
    gqt,
    gk,
    gv,
):
    tokens = o_ref.shape[0]
    low = low_half(tokens)
    lane = lax.broadcasted_iota(jnp.int32, (tokens, PAIR), 1)
    q, k, v, go = q_ref[0], k_ref[0], v_ref[0], go_ref[...]
    zero = jnp.zeros_like(q)
    product = o_ref[...].astype(F32) * go.astype(F32)
    minus = jnp.where(lane < 3, BF(-1.0), zero)
    for head in range(2):
        mine = low if head == 0 else jnp.logical_not(low)
        at = head * HD
        hi, mid, lo = split3(lse_ref[:, at : at + 1])
        segq = segq_ref[...]
        for place, piece in ((65, hi), (66, mid), (67, lo)):
            segq = jnp.where(lane == place, piece, segq)
        q_mine = jnp.where(mine, q, zero)
        go_mine = jnp.where(mine, go, zero)
        k_mine = jnp.where(mine, k, zero)
        q_wide = jnp.concatenate([q_mine, segq], axis=1)
        inner = jnp.sum(jnp.where(mine, product, 0.0), axis=-1, keepdims=True)
        extra = zero
        for place, piece in enumerate(split3(inner)):
            extra = jnp.where(lane == place, piece, extra)
        go_wide = jnp.concatenate([go_mine, extra], axis=1)
        for block in range(tokens // ROWS):
            rows = slice(block * ROWS, block * ROWS + ROWS)
            k_wide = jnp.concatenate([k[rows], segk_ref[rows, :]], axis=1)
            v_wide = jnp.concatenate([v[rows], minus[rows]], axis=1)
            p = jnp.exp2(dot(k_wide, q_wide, NT) * LOG2E)
            gs = (p * dot(v_wide, go_wide, NT)).astype(BF)
            value_part = dot(p.astype(BF), go_mine, NN)
            key_part = dot(gs, q_mine, NN)
            query_part = dot(k_mine[rows], gs, TN)
            if head == 0:
                gv[rows, :] = value_part
                gk[rows, :] = key_part
            else:
                gv[rows, :] += value_part
                gk[rows, :] += key_part
            if head == 0 and block == 0:
                gqt[...] = query_part
            else:
                gqt[...] += query_part
    g_ref[2] = gv[...].astype(BF)
    gq = gqt[...].T * 0.125
    pieces = (
        (0, gq, q.astype(F32) * 8.0, qgain_ref[...], rq_ref[0]),
        (1, gk[...], k.astype(F32), kgain_ref[...], rk_ref[0]),
    )
    for part, grad, normed, gain, rstd in pieces:
        hat = normed / gain
        t = grad * gain
        dgain_ref[part] = jnp.broadcast_to(jnp.sum(grad * hat, axis=0, keepdims=True), (8, PAIR))
        g_ref[part] = (rstd * (t - pair_mean(t, low) - hat * pair_mean(t * hat, low))).astype(BF)


def attback(qkv, segq, segk, o, lse, go, rstd, qgain, kgain):
    tokens = o.shape[0]

    def part(which):
        return pl.BlockSpec((1, tokens, PAIR), lambda i: (which, 0, i))

    col = pl.BlockSpec((tokens, PAIR), lambda i: (0, i))
    seg = whole((tokens, PAIR))
    return pl.pallas_call(
        attback_body,
        grid=(PAIRS,),
        in_specs=[part(0), part(1), part(2), seg, seg, col, col, col, part(0), part(1)]
        + [whole((1, PAIR))] * 2,
        out_specs=[
            pl.BlockSpec((3, tokens, PAIR), lambda i: (0, 0, i)),
            pl.BlockSpec((2, 8, PAIR), lambda i: (0, 0, i)),
        ],
        out_shape=[
            jax.ShapeDtypeStruct((3, tokens, D), BF),
            jax.ShapeDtypeStruct((2, 8, D), F32),
        ],
        scratch_shapes=[
            pltpu.VMEM((PAIR, tokens), F32),
            pltpu.VMEM((tokens, PAIR), F32),
            pltpu.VMEM((tokens, PAIR), F32),
        ],
        compiler_params=params(),
        cost_estimate=cost(
            HEADS * tokens * tokens * 256 * 10, 30 * tokens * D, HEADS * tokens * tokens
        ),
        name="attback",
    )(qkv, qkv, qkv, segq, segk, o, lse, go, rstd, rstd, qgain, kgain)


def qkvgrad_body(h_ref, g_ref, dw_ref, db_ref, ht):
    @pl.when(pl.program_id(0) == 0)
    def _():
        ht[...] = h_ref[...].T

    g = g_ref[0]
    dw_ref[...] = dot(ht[...], g, NN).astype(BF)
    db_ref[...] = jnp.sum(g.astype(F32), axis=0, keepdims=True)


def qkvgrad(h, g):
    tokens = h.shape[0]
    return pl.pallas_call(
        qkvgrad_body,
        grid=(3, 3),
        in_specs=[
            whole((tokens, D)),
            pl.BlockSpec((1, tokens, 256), lambda i, j: (i, 0, j)),
        ],
        out_specs=[
            pl.BlockSpec((D, 256), lambda i, j: (0, 3 * i + j)),
            pl.BlockSpec((1, 256), lambda i, j: (0, 3 * i + j)),
        ],
        out_shape=[
            jax.ShapeDtypeStruct((D, 3 * D), BF),
            jax.ShapeDtypeStruct((1, 3 * D), F32),
        ],
        scratch_shapes=[pltpu.VMEM((D, tokens), BF)],
        compiler_params=params("arbitrary", "arbitrary"),
        cost_estimate=cost(6 * tokens * D * D, 14 * tokens * D),
        name="qkvgrad",
    )(h, g)


def back_body(count, *refs):
    g_ref, x_ref, gx1_ref = refs[:3]
    pieces = refs[3 : 3 + count]
    gain_ref, gx_ref, dvec_ref, full, sems = refs[3 + count :]
    step = pl.program_id(0)

    @pl.when(step == 0)
    def _():
        for item in fetch(pieces, full, sems):
            item.wait()
        dvec_ref[...] = jnp.zeros_like(dvec_ref)

    g = dot(g_ref[0], full[:, :D], NT)
    g += dot(g_ref[1], full[:, D : 2 * D], NT)
    g += dot(g_ref[2], full[:, 2 * D :], NT)
    center, rstd = stats(x_ref[...].astype(F32))
    hat = center * rstd
    t = g * gain_ref[...]
    gx = gx1_ref[...] + rstd * (
        t - jnp.mean(t, axis=-1, keepdims=True) - hat * jnp.mean(t * hat, axis=-1, keepdims=True)
    )
    gx_ref[...] = gx.astype(BF)
    dvec_ref[0:1, :] += jnp.sum(g * hat, axis=0, keepdims=True)
    dvec_ref[1:2, :] += jnp.sum(g, axis=0, keepdims=True)


def back(g, x, gx1, pieces, gain):
    tokens = x.shape[0]
    row = pl.BlockSpec((ROWS, D), lambda i: (i, 0))
    return pl.pallas_call(
        functools.partial(back_body, len(pieces)),
        grid=(tokens // ROWS,),
        in_specs=[pl.BlockSpec((3, ROWS, D), lambda i: (0, i, 0)), row, row]
        + [ANY] * len(pieces)
        + [whole((1, D))],
        out_specs=[row, whole((2, D))],
        out_shape=[jax.ShapeDtypeStruct((tokens, D), BF), jax.ShapeDtypeStruct((2, D), F32)],
        scratch_shapes=[pltpu.VMEM((D, 3 * D), BF), pltpu.SemaphoreType.DMA((len(pieces),))],
        compiler_params=params(),
        cost_estimate=cost(6 * tokens * D * D, 16 * tokens * D, tokens),
        name="back",
    )(g, x, gx1, *pieces, gain)


CHUNKS = 12
RANK_ROWS = 192
STAGES_AT = (0, 1, 3, 5, 6, 8, 10, 11, 13)
OUT_TICK, ATT_TICK, GRAD_TICK, BACK_TICK, SMALL_TICK = 0, 3, 15, 18, 22
TICKS = 2 * (CHUNKS - 1) + STAGES_AT[-1] + 2


def finish_body(count, *refs):
    (
        o_ref,
        ga_ref,
        q_ref,
        k_ref,
        v_ref,
        segq_ref,
        segk_ref,
        opair_ref,
        lse_ref,
        rq_ref,
        rk_ref,
        qgain_ref,
        kgain_ref,
        h_ref,
        x_ref,
        gx1_ref,
        gain_ref,
        dubias_ref,
        dvec_ref,
        up_ref,
        down_ref,
    ) = refs[:21]
    out_pieces = refs[21 : 21 + count]
    qkv_pieces = refs[21 + count : 21 + 2 * count]
    (
        gx_ref,
        total_ref,
        small_ref,
        out_full,
        qkv_full,
        go,
        g3,
        ht,
        gqt,
        gk,
        gv,
        own,
        held,
        r0,
        r1,
        r2,
        r3,
        r4,
        done,
        small,
        rsmall,
        weight_sems,
        local_sems,
        send_sems,
        recv_sems,
        done_sems,
        ssend_sems,
        srecv_sems,
    ) = refs[21 + 2 * count :]
    tick = pl.program_id(0)
    tokens = o_ref.shape[0]

    rank, group = lax.axis_index("fsdp"), lax.axis_index("dp")
    c, x = rank % 2, rank // 2
    y, z1, z2 = group % 2, (group // 2) % 2, group // 4
    partners = (
        {"fsdp": flip(rank, 1)},
        {"fsdp": flip(rank, 2)},
        {"dp": flip(group, 1)},
        {"dp": flip(group, 2)},
        {"dp": flip(group, 4)},
    )
    row_y = pl.multiple_of(y * 96, 48)
    other_y = pl.multiple_of((1 - y) * 96, 48)
    row_z = pl.multiple_of(y * 96 + z1 * 48, 48)
    other_z = pl.multiple_of(y * 96 + (1 - z1) * 48, 48)
    col_z = pl.multiple_of(z2 * 384, 384)
    other_col = pl.multiple_of((1 - z2) * 384, 384)

    def remote(stage, chunk, src, dst, partner):
        return pltpu.make_async_remote_copy(
            src_ref=src,
            dst_ref=dst,
            send_sem=send_sems.at[stage, chunk],
            recv_sem=recv_sems.at[stage, chunk],
            device_id=partners[partner],
            device_id_type=pl.DeviceIdType.MESH,
        )

    def first_send(source, place, chunk):
        return remote(0, chunk, source.at[place, :, 1 - c], r0.at[chunk], 0)

    def sends(stage, chunk):
        if stage == 1:
            return remote(1, chunk, held.at[chunk, 1 - x], r1.at[chunk], 1)
        if stage == 2:
            return remote(2, chunk, held.at[chunk, x, pl.ds(other_y, 96)], r2.at[chunk], 2)
        if stage == 3:
            return remote(3, chunk, held.at[chunk, x, pl.ds(other_z, 48)], r3.at[chunk], 3)
        if stage == 4:
            src = held.at[chunk, x, pl.ds(row_z, 48), pl.ds(other_col, 384)]
            return remote(4, chunk, src, r4.at[chunk], 4)
        if stage == 5:
            place = done.at[chunk, pl.ds(row_z, 48), pl.ds(col_z, 384)]
            return remote(5, chunk, place, place, 4)
        if stage == 6:
            place = done.at[chunk, pl.ds(row_z, 48)]
            return remote(6, chunk, place, place, 3)
        place = done.at[chunk, pl.ds(row_y, 96)]
        return remote(7, chunk, place, place, 2)

    def stored(chunk):
        return pltpu.make_async_copy(done.at[chunk], total_ref.at[chunk], done_sems.at[chunk])

    def add(left, right):
        return (left.astype(F32) + right.astype(F32)).astype(BF)

    sources = ((up_ref, 0, 4), (down_ref, 4, 8), (own, 8, CHUNKS))

    def start_chunk(chunk):
        for source, begin, end in sources:

            @pl.when((chunk >= begin) & (chunk < end))
            def _(source=source, begin=begin):
                place = chunk - begin
                first_send(source, place, chunk).start()
                pltpu.make_async_copy(
                    source.at[place, :, c], held.at[chunk], local_sems.at[chunk]
                ).start()

    def pass_on(stage, chunk):
        if stage == 1:
            for source, begin, end in sources:

                @pl.when((chunk >= begin) & (chunk < end))
                def _(source=source, begin=begin):
                    place = chunk - begin
                    first_send(source, place, chunk).wait()
                    pltpu.make_async_copy(
                        source.at[place, :, c], held.at[chunk], local_sems.at[chunk]
                    ).wait()

            def add_rows(i, _):
                rows = pl.ds(pl.multiple_of((i % 4) * 48, 48), 48)
                held[chunk, i // 4, rows, :] = add(
                    held[chunk, i // 4, rows, :], r0[chunk, i // 4, rows, :]
                )
                return 0

            lax.fori_loop(0, 8, add_rows, 0)
        elif stage == 2:
            sends(1, chunk).wait()

            def add_rows(i, _):
                rows = pl.ds(pl.multiple_of(i * 48, 48), 48)
                held[chunk, x, rows, :] = add(held[chunk, x, rows, :], r1[chunk, rows, :])
                return 0

            lax.fori_loop(0, 4, add_rows, 0)
        elif stage == 3:
            sends(2, chunk).wait()

            def add_rows(i, _):
                rows = pl.ds(pl.multiple_of(row_y + i * 48, 48), 48)
                came = pl.ds(pl.multiple_of(i * 48, 48), 48)
                held[chunk, x, rows, :] = add(held[chunk, x, rows, :], r2[chunk, came, :])
                return 0

            lax.fori_loop(0, 2, add_rows, 0)
        elif stage == 4:
            sends(3, chunk).wait()
            rows = pl.ds(row_z, 48)
            held[chunk, x, rows, :] = add(held[chunk, x, rows, :], r3[chunk])
        elif stage == 5:
            sends(4, chunk).wait()
            rows, cols = pl.ds(row_z, 48), pl.ds(col_z, 384)
            done[chunk, rows, cols] = add(held[chunk, x, rows, cols], r4[chunk])
        else:
            sends(stage - 1, chunk).wait()
        if stage < 8:
            sends(stage, chunk).start()
        else:
            stored(chunk).start()

    def small_send(step):
        return pltpu.make_async_remote_copy(
            src_ref=small.at[step],
            dst_ref=rsmall.at[step],
            send_sem=ssend_sems.at[step],
            recv_sem=srecv_sems.at[step],
            device_id=partners[step],
            device_id_type=pl.DeviceIdType.MESH,
        )

    def weights(which):
        full, pieces = ((out_full, out_pieces), (qkv_full, qkv_pieces))[which]
        rows = full.shape[0] // count
        return [
            pltpu.make_async_copy(
                piece,
                full.at[pl.ds(pl.multiple_of(flip(rank, distance) * rows, rows), rows)],
                weight_sems.at[which, distance],
            )
            for distance, piece in enumerate(pieces)
        ]

    @pl.when(tick == 0)
    def _():
        barrier = pltpu.get_barrier_semaphore()
        for partner in partners:
            pl.semaphore_signal(
                barrier, inc=1, device_id=partner, device_id_type=pl.DeviceIdType.MESH
            )
        for item in weights(0) + weights(1):
            item.start()
        small[0] = jnp.zeros_like(small[0])
        pl.semaphore_wait(barrier, len(partners))

    for stage in reversed(range(9)):
        moment = tick - STAGES_AT[stage]

        @pl.when((moment >= 0) & (moment < 2 * CHUNKS) & (moment % 2 == 0))
        def _(stage=stage, moment=moment):
            chunk = moment // 2
            if stage == 0:
                start_chunk(chunk)
            else:
                pass_on(stage, chunk)

    @pl.when(tick < ATT_TICK)
    def _():
        @pl.when(tick == 0)
        def _():
            for item in weights(0):
                item.wait()

        start = pl.multiple_of(tick * 256, 256)
        block = pl.ds(start, 256)
        go[:, block] = dot(ga_ref[...], out_full[block, :], NT).astype(BF)
        dout = dot(o_ref[:, block], ga_ref[...], TN).astype(BF)
        for part in range(4):
            piece = dout[part * 64 : part * 64 + 64]
            row = tick * 256 + part * 64
            shard = row // RANK_ROWS
            own[
                0,
                shard // 2,
                shard % 2,
                pl.ds(pl.multiple_of(row % RANK_ROWS, 64), 64),
                :,
            ] = piece

    @pl.when((tick >= ATT_TICK) & (tick < GRAD_TICK))
    def _():
        pair = (tick - ATT_TICK) // 2
        head = (tick - ATT_TICK) % 2
        pair_cols = pl.ds(pl.multiple_of(pair * PAIR, PAIR), PAIR)
        lane = lax.broadcasted_iota(jnp.int32, (tokens, PAIR), 1)
        mine = lane // HD == head
        q, k, v, go_pair = q_ref[0], k_ref[0], v_ref[0], go[:, pair_cols]
        zero = jnp.zeros_like(q)
        minus = jnp.where(lane < 3, BF(-1.0), zero)

        @pl.when(head == 0)
        def _():
            gqt[...] = jnp.zeros_like(gqt)
            gk[...] = jnp.zeros_like(gk)
            gv[...] = jnp.zeros_like(gv)

        product = opair_ref[...].astype(F32) * go_pair.astype(F32)
        inner = jnp.sum(jnp.where(mine, product, 0.0), axis=-1, keepdims=True)
        logs = jnp.sum(jnp.where(lane == head * HD, lse_ref[...], 0.0), axis=-1, keepdims=True)
        segq = segq_ref[...]
        for place, piece in enumerate(split3(logs)):
            segq = jnp.where(lane == 65 + place, piece, segq)
        extra = zero
        for place, piece in enumerate(split3(inner)):
            extra = jnp.where(lane == place, piece, extra)
        q_mine = jnp.where(mine, q, zero)
        go_mine = jnp.where(mine, go_pair, zero)
        k_mine = jnp.where(mine, k, zero)
        q_wide = jnp.concatenate([q_mine, segq], axis=1)
        go_wide = jnp.concatenate([go_mine, extra], axis=1)
        for block in range(tokens // ROWS):
            rows = slice(block * ROWS, block * ROWS + ROWS)
            k_wide = jnp.concatenate([k[rows], segk_ref[rows, :]], axis=1)
            v_wide = jnp.concatenate([v[rows], minus[rows]], axis=1)
            p = jnp.exp2(dot(k_wide, q_wide, NT) * LOG2E)
            gs = (p * dot(v_wide, go_wide, NT)).astype(BF)
            gv[rows, :] += dot(p.astype(BF), go_mine, NN)
            gk[rows, :] += dot(gs, q_mine, NN)
            gqt[...] += dot(k_mine[rows], gs, TN)

        @pl.when(head == 1)
        def _():
            low = low_half(tokens)
            g3[2, :, pair_cols] = gv[...].astype(BF)
            gq = gqt[...].T * 0.125
            pieces = (
                (0, gq, q.astype(F32) * 8.0, qgain_ref[...], rq_ref[0]),
                (1, gk[...], k.astype(F32), kgain_ref[...], rk_ref[0]),
            )
            for part, grad, normed, gain, rstd in pieces:
                hat = normed / gain
                t = grad * gain
                lanes = slice(part * PAIR, part * PAIR + PAIR)
                small[0, 5:6, lanes] += jnp.sum(grad * hat, axis=0, keepdims=True)
                g3[part, :, pair_cols] = (
                    rstd * (t - pair_mean(t, low) - hat * pair_mean(t * hat, low))
                ).astype(BF)

    @pl.when((tick >= GRAD_TICK) & (tick < BACK_TICK))
    def _():
        part = tick - GRAD_TICK

        @pl.when(tick == GRAD_TICK)
        def _():
            ht[...] = h_ref[...].T

        for at in range(0, D, 256):
            g = g3[part, :, at : at + 256]
            own[1 + part, :, :, :, at : at + 256] = (
                dot(ht[...], g, NN).astype(BF).reshape(2, 2, RANK_ROWS, 256)
            )
            small[0, pl.ds(2 + part, 1), at : at + 256] = jnp.sum(
                g.astype(F32), axis=0, keepdims=True
            )

    @pl.when((tick >= BACK_TICK) & (tick < SMALL_TICK))
    def _():
        @pl.when(tick == BACK_TICK)
        def _():
            for item in weights(1):
                item.wait()

        rows = pl.ds(pl.multiple_of((tick - BACK_TICK) * ROWS, ROWS), ROWS)
        g = dot(g3[0, rows, :], qkv_full[:, :D], NT)
        g += dot(g3[1, rows, :], qkv_full[:, D : 2 * D], NT)
        g += dot(g3[2, rows, :], qkv_full[:, 2 * D :], NT)
        center, rstd = stats(x_ref[...].astype(F32))
        hat = center * rstd
        t = g * gain_ref[...]
        gx = gx1_ref[...] + rstd * (
            t
            - jnp.mean(t, axis=-1, keepdims=True)
            - hat * jnp.mean(t * hat, axis=-1, keepdims=True)
        )
        gx_ref[...] = gx.astype(BF)
        small[0, 0:1, :] += jnp.sum(g * hat, axis=0, keepdims=True)
        small[0, 1:2, :] += jnp.sum(g, axis=0, keepdims=True)

    @pl.when(tick == SMALL_TICK)
    def _():
        small[0, 6:10, :] = dvec_ref[...]
        for part in range(4):
            small[0, 10 + part : 11 + part, :] = dubias_ref[:, part * D : part * D + D]
        small_send(0).start()

    for step in range(5):

        @pl.when(tick == SMALL_TICK + 1 + step)
        def _(step=step):
            small_send(step).wait()
            small[step + 1] = small[step] + rsmall[step]
            if step < 4:
                small_send(step + 1).start()
            else:
                small_ref[...] = small[5]

    @pl.when(tick == TICKS - 1)
    def _():
        for chunk in range(CHUNKS):
            stored(chunk).wait()


def finish(o, ga, qkv, segq, segk, lse, rstd, qgain, kgain, h, x, gx1, gain, dubias, dvec, dup, ddown, outs, qkvs):
    tokens = o.shape[0]
    count = len(outs)
    split = (dup.shape[0], 2, 2, RANK_ROWS, D)

    def pair_of(i):
        return jnp.clip((i - ATT_TICK) // 2, 0, PAIRS - 1)

    def part(which):
        return pl.BlockSpec((1, tokens, PAIR), lambda i: (which, 0, pair_of(i)))

    col = pl.BlockSpec((tokens, PAIR), lambda i: (0, pair_of(i)))
    row = pl.BlockSpec(
        (ROWS, D), lambda i: (jnp.clip(i - BACK_TICK, 0, tokens // ROWS - 1), 0)
    )
    act = single((tokens, D))
    seg = single((tokens, PAIR))
    grid = pl.GridSpec(
        grid=(TICKS,),
        in_specs=[act, act, part(0), part(1), part(2), seg, seg, col, col, part(0), part(1)]
        + [single((1, PAIR))] * 2
        + [act, row, row, single((1, D)), single((1, 4 * D)), single((4, D)), ANY, ANY]
        + [ANY] * (2 * count),
        out_specs=[row, ANY, single((16, D))],
        scratch_shapes=[
            pltpu.VMEM((D, D), BF),
            pltpu.VMEM((D, 3 * D), BF),
            pltpu.VMEM((tokens, D), BF),
            pltpu.VMEM((3, tokens, D), BF),
            pltpu.VMEM((D, tokens), BF),
            pltpu.VMEM((PAIR, tokens), F32),
            pltpu.VMEM((tokens, PAIR), F32),
            pltpu.VMEM((tokens, PAIR), F32),
            pltpu.VMEM((4, 2, 2, RANK_ROWS, D), BF),
            pltpu.VMEM((CHUNKS, 2, RANK_ROWS, D), BF),
            pltpu.VMEM((CHUNKS, 2, RANK_ROWS, D), BF),
            pltpu.VMEM((CHUNKS, RANK_ROWS, D), BF),
            pltpu.VMEM((CHUNKS, 96, D), BF),
            pltpu.VMEM((CHUNKS, 48, D), BF),
            pltpu.VMEM((CHUNKS, 48, D // 2), BF),
            pltpu.VMEM((CHUNKS, RANK_ROWS, D), BF),
            pltpu.VMEM((6, 16, D), F32),
            pltpu.VMEM((5, 16, D), F32),
            pltpu.SemaphoreType.DMA((2, count)),
            pltpu.SemaphoreType.DMA((CHUNKS,)),
            pltpu.SemaphoreType.DMA((8, CHUNKS)),
            pltpu.SemaphoreType.DMA((8, CHUNKS)),
            pltpu.SemaphoreType.DMA((CHUNKS,)),
            pltpu.SemaphoreType.DMA((5,)),
            pltpu.SemaphoreType.DMA((5,)),
        ],
    )
    return pl.pallas_call(
        functools.partial(finish_body, count),
        grid_spec=grid,
        out_shape=[
            jax.ShapeDtypeStruct((tokens, D), BF),
            jax.ShapeDtypeStruct((CHUNKS, RANK_ROWS, D), BF),
            jax.ShapeDtypeStruct((16, D), F32),
        ],
        compiler_params=pltpu.CompilerParams(
            dimension_semantics=("arbitrary",),
            vmem_limit_bytes=63 * 1024 * 1024,
            collective_id=1,
            has_side_effects=True,
        ),
        name="finish",
    )(
        o, ga, qkv, qkv, qkv, segq, segk, o, lse, rstd, rstd, qgain, kgain, h, x, gx1, gain,
        dubias, dvec, dup.reshape(split), ddown.reshape(split), *outs, *qkvs,
    )


def swap(values, axis, mask, size):
    return lax.ppermute(values, axis, [(i, i ^ mask) for i in range(size)])


def bits_of(size):
    return [1 << b for b in range(size.bit_length() - 1)]


def gather_shards(shard, size):
    held = [shard]
    for mask in reversed(bits_of(size)):
        held = held + [swap(item, "fsdp", mask, size) for item in held]
    order = [0]
    for mask in reversed(bits_of(size)):
        order = order + [place ^ mask for place in order]
    placed = [None] * size
    for place, item in zip(order, held):
        placed[place] = item
    return placed


def reduce_grad(grad, order, sizes):
    fsdp, dp = sizes["fsdp"], sizes["dp"]
    rows, columns = grad.shape
    names = [("fsdp", m) for m in reversed(bits_of(fsdp))] + [
        ("dp", m) for m in reversed(bits_of(dp))
    ]
    held = grad.reshape((2,) * len(names) + (rows // fsdp // dp, columns))
    undo = []
    for step in order:
        axis, mask = step
        place = names.index(step)
        mine = (lax.axis_index(axis) // mask) % 2
        send = lax.dynamic_index_in_dim(held, 1 - mine, place, keepdims=False)
        keep = lax.dynamic_index_in_dim(held, mine, place, keepdims=False)
        held = (
            keep.astype(F32) + swap(send, axis, mask, sizes[axis]).astype(F32)
        ).astype(BF)
        names.pop(place)
        if axis == "dp":
            place -= sum(name == "fsdp" for name, _ in names[:place])
            undo.append((axis, mask, place, mine))
    for axis, mask, place, mine in reversed(undo):
        other = swap(held, axis, mask, sizes[axis])
        first = jnp.where(mine == 0, held, other)
        second = jnp.where(mine == 0, other, held)
        held = jnp.stack([first, second], axis=place)
    return held.reshape(rows // fsdp, columns).astype(F32)


def reduce_small(grad, sizes):
    held = grad.reshape((2,) * len(bits_of(sizes["fsdp"])) + (grad.shape[1],))
    for mask in reversed(bits_of(sizes["fsdp"])):
        mine = (lax.axis_index("fsdp") // mask) % 2
        send = lax.dynamic_index_in_dim(held, 1 - mine, 0, keepdims=False)
        keep = lax.dynamic_index_in_dim(held, mine, 0, keepdims=False)
        held = keep + swap(send, "fsdp", mask, sizes["fsdp"])
    for mask in bits_of(sizes["dp"]):
        held = held + swap(held, "dp", mask, sizes["dp"])
    return held


def local(sizes, *arguments):
    (
        block_input,
        segment_ids,
        norm1_gain,
        norm1_bias,
        qkv_weight,
        qkv_bias,
        query_gain,
        key_gain,
        out_weight,
        out_bias,
        norm2_gain,
        norm2_bias,
        up_weight,
        up_bias,
        down_weight,
        down_bias,
        output_grad,
    ) = arguments
    fsdp = sizes["fsdp"]
    rank = lax.axis_index("fsdp")
    small_args = (
        norm1_gain,
        norm1_bias,
        qkv_bias,
        query_gain,
        key_gain,
        out_bias,
        norm2_gain,
        norm2_bias,
        up_bias,
        down_bias,
    )
    widths = [item.shape[0] for item in small_args]
    packed = jnp.stack(gather_shards(jnp.concatenate(small_args), fsdp))
    packed = packed[jnp.arange(fsdp) ^ rank].astype(F32)
    smalls = []
    at = 0
    for width in widths:
        smalls.append(packed[:, at : at + width].reshape(1, fsdp * width))
        at += width
    gain1, shift1, qkvb, qgain, kgain, outb, gain2, shift2, upb, downb = smalls
    qgain = jnp.concatenate([qgain, qgain], axis=1)
    kgain = jnp.concatenate([kgain, kgain], axis=1)
    qkv_pieces = gather_shards(qkv_weight, fsdp)
    out_pieces = gather_shards(out_weight, fsdp)
    up_pieces = gather_shards(up_weight, fsdp)
    down_pieces = gather_shards(down_weight, fsdp)

    lane = jnp.arange(PAIR)[None, :]
    seg_col = segment_ids[:, None]
    match = (seg_col == lane) & (lane < HD)
    segq = jnp.where(match, QMARK, jnp.where(lane == HD, 1.0, 0.0)).astype(BF)
    segk = jnp.where(
        match,
        KMARK,
        jnp.where(lane == HD, -QMARK * KMARK, jnp.where((lane > HD) & (lane <= HD + 3), -1.0, 0.0)),
    ).astype(BF)

    h1, qkv, rstd = front(block_input, gain1, shift1, qkv_pieces, qkvb, qgain, kgain)
    mixed, lse = attend(qkv, segq, segk)
    x1, h2 = middle(mixed, block_input, out_pieces, outb, gain2, shift2)
    output, gx1, ga, dup, ddown, dubias, dvec2 = mlp(
        h2, x1, seg_col, output_grad, up_pieces, down_pieces, upb, downb, gain2
    )
    if fsdp == 4 and sizes["dp"] == 8:
        input_grad, totals, small = finish(
            mixed, ga, qkv, segq, segk, lse, rstd, qgain, kgain, h1, block_input, gx1, gain1,
            dubias, dvec2, dup, ddown, out_pieces, qkv_pieces,
        )
        totals = totals.astype(F32)
        up_total = totals[0:4].transpose(1, 0, 2).reshape(D // fsdp, 4 * D)
        down_total = totals[4:8].reshape(D, D)
        out_total = totals[8]
        qkv_total = totals[9:12].transpose(1, 0, 2).reshape(D // fsdp, 3 * D)
        dvec1 = small[0:2]
        dqkvb = small[2:5]
        dgains = small[5, : 2 * PAIR].reshape(2, 2, HD).sum(axis=1)
        dvec2 = small[6:10]
        dubias = small[10:14]
    else:
        go, dout = outback(mixed, ga, out_pieces)
        gqkv, dheads = attback(qkv, segq, segk, mixed, lse, go, rstd, qgain, kgain)
        dqkv, dqkvb = qkvgrad(h1, gqkv)
        input_grad, dvec1 = back(gqkv, block_input, gx1, qkv_pieces, gain1)
        order = [("fsdp", m) for m in bits_of(fsdp)] + [("dp", m) for m in bits_of(sizes["dp"])]
        dup = dup.transpose(1, 2, 0, 3).reshape(D, -1)
        ddown = ddown.transpose(1, 0, 2, 3).reshape(-1, D)
        up_total, down_total, out_total, qkv_total = [
            reduce_grad(grad, order, sizes) for grad in (dup, ddown, dout, dqkv)
        ]
        dgains = dheads[:, 0, :].reshape(2, HEADS, HD).sum(axis=1)

    parts = (
        dvec1[0],
        dvec1[1],
        dqkvb,
        dgains[0],
        dgains[1],
        dvec2[2],
        dvec2[0],
        dvec2[1],
        dubias,
        dvec2[3],
    )
    small = jnp.concatenate([part.reshape(fsdp, -1) for part in parts], axis=1)
    if fsdp == 4 and sizes["dp"] == 8:
        small = lax.dynamic_index_in_dim(small, rank, 0, keepdims=False)
    else:
        small = reduce_small(small, sizes)
    shares = []
    at = 0
    for width in widths:
        shares.append(small[at : at + width])
        at += width
    n1g, n1b, qkvb_total, qg, kg, outb_total, n2g, n2b, upb_total, downb_total = shares
    return (
        output,
        input_grad,
        n1g,
        n1b,
        qkv_total,
        qkvb_total,
        qg,
        kg,
        out_total,
        outb_total,
        n2g,
        n2b,
        up_total,
        upb_total,
        down_total,
        downb_total,
    )


def solution(mesh):
    rows, shard = P(("dp", "fsdp"), None), P("fsdp")
    matrix = P("fsdp", None)
    placed = (
        (rows, P(("dp", "fsdp")), shard, shard, matrix, shard, shard, shard)
        + (matrix, shard, shard, shard, matrix, shard, matrix, shard, rows)
    )
    results = (
        (rows, rows, shard, shard, matrix, shard, shard, shard)
        + (matrix, shard, shard, shard, matrix, shard, matrix, shard)
    )
    return jax.shard_map(
        functools.partial(local, dict(mesh.shape)),
        mesh=mesh,
        in_specs=placed,
        out_specs=results,
        check_vma=False,
    )
```

```python
import functools
import math

import jax
import jax.numpy as jnp
from jax import lax
from jax.experimental import pallas as pl
from jax.experimental.pallas import tpu as pltpu
from jax.sharding import PartitionSpec as P

D = 768
HEADS = 12
HD = 64
PAIR = 128
PAIRS = HEADS // 2
EPS = 1e-06
BF = jnp.bfloat16
F32 = jnp.float32
LOG2E = 1.4426950408889634
ROWS = 256
QMARK = 16.0
KMARK = 12.0

NN = (((1,), (0,)), ((), ()))
NT = (((1,), (1,)), ((), ()))
TN = (((0,), (0,)), ((), ()))


def dot(left, right, dims):
    return lax.dot_general(left, right, dims, preferred_element_type=F32)


def params(*semantics):
    return pltpu.CompilerParams(
        dimension_semantics=semantics or ("arbitrary",), vmem_limit_bytes=60 * 1024 * 1024
    )


def cost(flops, nbytes, trans=0):
    return pl.CostEstimate(flops=int(flops), bytes_accessed=int(nbytes), transcendentals=int(trans))


def whole(shape):
    return pl.BlockSpec(shape, lambda *_: (0,) * len(shape))


def single(shape):
    return pl.BlockSpec(shape, lambda *_: (0,) * len(shape), pipeline_mode=pl.Buffered(1))


ANY = pl.BlockSpec(memory_space=pl.ANY)


def flip(rank, distance):
    bit = 1
    while bit <= distance:
        if distance & bit:
            rank = rank + bit * (1 - 2 * ((rank // bit) % 2))
        bit *= 2
    return rank


def fetch(pieces, full, sems):
    if len(pieces) == 1:
        copies = [pltpu.make_async_copy(pieces[0], full, sems.at[0])]
        copies[0].start()
        return copies
    rank = lax.axis_index("fsdp")
    rows = full.shape[0] // len(pieces)
    copies = []
    for distance, piece in enumerate(pieces):
        start = pl.multiple_of(flip(rank, distance) * rows, rows)
        copies.append(
            pltpu.make_async_copy(piece, full.at[pl.ds(start, rows)], sems.at[distance])
        )
    for item in copies:
        item.start()
    return copies


def stats(values):
    center = values - jnp.mean(values, axis=-1, keepdims=True)
    rstd = lax.rsqrt(jnp.mean(center * center, axis=-1, keepdims=True) + EPS)
    return center, rstd


def low_half(rows):
    return lax.broadcasted_iota(jnp.int32, (rows, PAIR), 1) < HD


def pair_mean(values, low):
    first = jnp.sum(jnp.where(low, values, 0.0), axis=-1, keepdims=True)
    second = jnp.sum(jnp.where(low, 0.0, values), axis=-1, keepdims=True)
    return jnp.where(low, first, second) * (1.0 / HD)


def front_body(count, *refs):
    x_ref, gain_ref, shift_ref = refs[:3]
    pieces = refs[3 : 3 + count]
    bias_ref, qgain_ref, kgain_ref, h_ref, qkv_ref, rstd_ref, full, sems = refs[3 + count :]

    @pl.when(pl.program_id(0) == 0)
    def _():
        for item in fetch(pieces, full, sems):
            item.wait()

    center, rstd = stats(x_ref[...].astype(F32))
    h = (center * rstd * gain_ref[...] + shift_ref[...]).astype(BF)
    h_ref[...] = h
    low = low_half(h.shape[0])
    for part in range(3):
        for block in range(D // 256):
            at = part * D + block * 256
            y = dot(h, full[:, at : at + 256], NN) + bias_ref[:, at : at + 256]
            if part == 2:
                qkv_ref[2, :, block * 256 : block * 256 + 256] = y.astype(BF)
                continue
            gain = (qgain_ref, kgain_ref)[part][...]
            for half in range(2):
                tile = y[:, half * PAIR : half * PAIR + PAIR]
                cols = slice(block * 256 + half * PAIR, block * 256 + half * PAIR + PAIR)
                c = tile - pair_mean(tile, low)
                r = lax.rsqrt(pair_mean(c * c, low) + EPS)
                normed = (c * r * gain).astype(BF)
                qkv_ref[part, :, cols] = normed * BF(0.125) if part == 0 else normed
                rstd_ref[part, :, cols] = r


def front(x, gain, shift, pieces, bias, qgain, kgain):
    tokens = x.shape[0]
    row = pl.BlockSpec((ROWS, D), lambda i: (i, 0))
    return pl.pallas_call(
        functools.partial(front_body, len(pieces)),
        grid=(tokens // ROWS,),
        in_specs=[row, whole((1, D)), whole((1, D))]
        + [ANY] * len(pieces)
        + [whole((1, 3 * D)), whole((1, PAIR)), whole((1, PAIR))],
        out_specs=[
            row,
            pl.BlockSpec((3, ROWS, D), lambda i: (0, i, 0)),
            pl.BlockSpec((2, ROWS, D), lambda i: (0, i, 0)),
        ],
        out_shape=[
            jax.ShapeDtypeStruct((tokens, D), BF),
            jax.ShapeDtypeStruct((3, tokens, D), BF),
            jax.ShapeDtypeStruct((2, tokens, D), F32),
        ],
        scratch_shapes=[pltpu.VMEM((D, 3 * D), BF), pltpu.SemaphoreType.DMA((len(pieces),))],
        compiler_params=params(),
        cost_estimate=cost(2 * tokens * D * 3 * D, 18 * tokens * D, tokens),
        name="front",
    )(x, gain, shift, *pieces, bias, qgain, kgain)


def attend_body(q_ref, k_ref, v_ref, segq_ref, segk_ref, o_ref, lse_ref):
    tokens = o_ref.shape[0]
    low = low_half(tokens)
    keys = jnp.concatenate([k_ref[0], segk_ref[...]], axis=1)
    values = v_ref[0]
    one = jnp.ones_like(values)
    values_a = jnp.where(low, values, one)
    values_b = jnp.where(low, one, values)
    low_rows = low_half(ROWS)
    for block in range(tokens // ROWS):
        rows = slice(block * ROWS, block * ROWS + ROWS)
        q = q_ref[0, rows, :]
        seg = segq_ref[rows, :]
        zero = jnp.zeros_like(q)
        sa = dot(jnp.concatenate([jnp.where(low_rows, q, zero), seg], axis=1), keys, NT)
        acc_a = dot(jnp.exp2(sa * LOG2E).astype(BF), values_a, NN)
        sb = dot(jnp.concatenate([jnp.where(low_rows, zero, q), seg], axis=1), keys, NT)
        acc_b = dot(jnp.exp2(sb * LOG2E).astype(BF), values_b, NN)
        top = jnp.where(low_rows, acc_a, acc_b)
        total = pltpu.roll(jnp.where(low_rows, acc_b, acc_a), HD, 1)
        total = jnp.where(total > 0, total, 1.0)
        o_ref[rows, :] = (top / total).astype(BF)
        lse_ref[rows, :] = jnp.log(total)


def attend(qkv, segq, segk):
    tokens = qkv.shape[1]

    def part(which):
        return pl.BlockSpec((1, tokens, PAIR), lambda i: (which, 0, i))

    col = pl.BlockSpec((tokens, PAIR), lambda i: (0, i))
    return pl.pallas_call(
        attend_body,
        grid=(PAIRS,),
        in_specs=[part(0), part(1), part(2), whole((tokens, PAIR)), whole((tokens, PAIR))],
        out_specs=[col, col],
        out_shape=[
            jax.ShapeDtypeStruct((tokens, D), BF),
            jax.ShapeDtypeStruct((tokens, D), F32),
        ],
        compiler_params=params(),
        cost_estimate=cost(
            HEADS * tokens * tokens * 256 * 6, 10 * tokens * D, HEADS * tokens * tokens
        ),
        name="attend",
    )(qkv, qkv, qkv, segq, segk)


def middle_body(count, *refs):
    o_ref, x_ref = refs[:2]
    pieces = refs[2 : 2 + count]
    bias_ref, gain_ref, shift_ref, x1_ref, h_ref, full, sems = refs[2 + count :]

    @pl.when(pl.program_id(0) == 0)
    def _():
        for item in fetch(pieces, full, sems):
            item.wait()

    x1 = x_ref[...].astype(F32) + dot(o_ref[...], full[...], NN) + bias_ref[...]
    x1_ref[...] = x1
    center, rstd = stats(x1)
    h_ref[...] = (center * rstd * gain_ref[...] + shift_ref[...]).astype(BF)


def middle(o, x, pieces, bias, gain, shift):
    tokens = x.shape[0]
    row = pl.BlockSpec((ROWS, D), lambda i: (i, 0))
    return pl.pallas_call(
        functools.partial(middle_body, len(pieces)),
        grid=(tokens // ROWS,),
        in_specs=[row, row] + [ANY] * len(pieces) + [whole((1, D))] * 3,
        out_specs=[row, row],
        out_shape=[
            jax.ShapeDtypeStruct((tokens, D), F32),
            jax.ShapeDtypeStruct((tokens, D), BF),
        ],
        scratch_shapes=[pltpu.VMEM((D, D), BF), pltpu.SemaphoreType.DMA((len(pieces),))],
        compiler_params=params(),
        cost_estimate=cost(2 * tokens * D * D, 10 * tokens * D, tokens),
        name="middle",
    )(o, x, *pieces, bias, gain, shift)


def mlp_body(count, *refs):
    h_ref, x1_ref, valid_ref, gout_ref = refs[:4]
    ups = refs[4 : 4 + count]
    downs = refs[4 + count : 4 + 2 * count]
    (
        ubias_ref,
        dbias_ref,
        gain_ref,
        out_ref,
        gx1_ref,
        ga_ref,
        dup_ref,
        ddown_ref,
        dubias_ref,
        dvec_ref,
        up,
        down,
        acc,
        gh,
        gm,
        ht,
        act,
        gu,
        sems,
    ) = refs[4 + 2 * count :]
    tokens = h_ref.shape[0]
    fblock = act.shape[1]
    blocks = tokens // ROWS
    step = pl.program_id(0)

    @pl.when(step == 0)
    def _():
        copies = fetch(ups, up, sems.at[0]) + fetch(downs, down, sems.at[1])
        ht[...] = h_ref[...].T
        gm[...] = jnp.where(valid_ref[...] >= 0, gout_ref[...].astype(F32), 0.0).astype(BF)
        acc[...] = jnp.zeros_like(acc)
        gh[...] = jnp.zeros_like(gh)
        for item in copies:
            item.wait()

    start = pl.multiple_of(step * fblock, fblock)
    cols = pl.ds(start, fblock)
    ubias = ubias_ref[...]

    def rows_step(block, total):
        rows = pl.ds(pl.multiple_of(block * ROWS, ROWS), ROWS)
        u = dot(h_ref[rows, :], up[:, cols], NN) + ubias
        phi = 0.5 * (1.0 + lax.erf(u * math.sqrt(0.5)))
        a = (u * phi).astype(BF)
        act[rows, :] = a
        acc[rows, :] += dot(a, down[cols, :], NN)
        slope = phi + u * (jnp.exp2(u * u * (-0.5 * LOG2E)) * (1.0 / math.sqrt(2.0 * math.pi)))
        g = (slope * dot(gm[rows, :], down[cols, :], NT)).astype(BF)
        gu[rows, :] = g
        gh[rows, :] += dot(g, up[:, cols], NT)
        return total + jnp.sum(g.astype(F32), axis=0, keepdims=True)

    dubias_ref[...] = lax.fori_loop(0, blocks, rows_step, jnp.zeros((1, fblock), F32))
    for at in range(0, D, 256):
        block = slice(at, at + 256)
        ddown = dot(act[...], gm[:, block], TN).astype(BF)
        ddown_ref[..., block] = ddown.reshape(ddown_ref.shape[:-1] + (256,))
        dup = dot(ht[...], gu[:, block], NN).astype(BF)
        dup_ref[..., block] = dup.reshape(dup_ref.shape[:-1] + (256,))

    @pl.when(step == pl.num_programs(0) - 1)
    def _():
        gain = gain_ref[...]
        dbias = dbias_ref[...]

        def finish(block, totals):
            dgain, dshift, dob, ddb = totals
            rows = pl.ds(pl.multiple_of(block * ROWS, ROWS), ROWS)
            x1 = x1_ref[rows, :]
            valid = valid_ref[rows, :] >= 0
            out_ref[rows, :] = jnp.where(valid, x1 + acc[rows, :] + dbias, 0.0).astype(BF)
            center, rstd = stats(x1)
            hat = center * rstd
            g = gh[rows, :]
            t = g * gain
            gy = gm[rows, :].astype(F32)
            gx1 = gy + rstd * (
                t
                - jnp.mean(t, axis=-1, keepdims=True)
                - hat * jnp.mean(t * hat, axis=-1, keepdims=True)
            )
            gx1_ref[rows, :] = gx1
            low = gx1.astype(BF)
            ga_ref[rows, :] = low
            return (
                dgain + jnp.sum(g * hat, axis=0, keepdims=True),
                dshift + jnp.sum(g, axis=0, keepdims=True),
                dob + jnp.sum(low.astype(F32), axis=0, keepdims=True),
                ddb + jnp.sum(gy, axis=0, keepdims=True),
            )

        zero = jnp.zeros((1, D), F32)
        totals = lax.fori_loop(0, blocks, finish, (zero,) * 4)
        for place, total in enumerate(totals):
            dvec_ref[place : place + 1, :] = total


def mlp(h, x1, segments, gout, ups, downs, ubias, dbias, gain, shards):
    tokens = h.shape[0]
    count = len(ups)
    hidden = ubias.shape[1]
    fblock = hidden // shards
    grads = jax.ShapeDtypeStruct((hidden // fblock, shards, D // shards, D), BF)
    act = single((tokens, D))
    return pl.pallas_call(
        functools.partial(mlp_body, count),
        grid=(hidden // fblock,),
        in_specs=[act, act, single((tokens, 1)), act]
        + [ANY] * (2 * count)
        + [pl.BlockSpec((1, fblock), lambda i: (0, i)), whole((1, D)), whole((1, D))],
        out_specs=[
            act,
            act,
            act,
            pl.BlockSpec((1, shards, D // shards, D), lambda i: (i, 0, 0, 0)),
            pl.BlockSpec((hidden // fblock, 1, D // shards, D), lambda i: (0, i, 0, 0)),
            pl.BlockSpec((1, fblock), lambda i: (0, i)),
            whole((4, D)),
        ],
        out_shape=[
            jax.ShapeDtypeStruct((tokens, D), BF),
            jax.ShapeDtypeStruct((tokens, D), F32),
            jax.ShapeDtypeStruct((tokens, D), BF),
            grads,
            grads,
            jax.ShapeDtypeStruct((1, hidden), F32),
            jax.ShapeDtypeStruct((4, D), F32),
        ],
        scratch_shapes=[
            pltpu.VMEM((D, hidden), BF),
            pltpu.VMEM((hidden, D), BF),
            pltpu.VMEM((tokens, D), F32),
            pltpu.VMEM((tokens, D), F32),
            pltpu.VMEM((tokens, D), BF),
            pltpu.VMEM((D, tokens), BF),
            pltpu.VMEM((tokens, fblock), BF),
            pltpu.VMEM((tokens, fblock), BF),
            pltpu.SemaphoreType.DMA((2, count)),
        ],
        compiler_params=params(),
        cost_estimate=cost(12 * tokens * D * hidden, 30 * tokens * D, 2 * tokens * hidden),
        name="mlp",
    )(h, x1, segments, gout, *ups, *downs, ubias, dbias, gain)


def outback_body(count, *refs):
    o_ref, ga_ref = refs[:2]
    pieces = refs[2 : 2 + count]
    go_ref, dout_ref, full, sems = refs[2 + count :]
    step = pl.program_id(0)

    @pl.when(step == 0)
    def _():
        for item in fetch(pieces, full, sems):
            item.wait()

    start = pl.multiple_of(step * 256, 256)
    go_ref[...] = dot(ga_ref[...], full[pl.ds(start, 256), :], NT).astype(BF)
    dout_ref[...] = dot(o_ref[...], ga_ref[...], TN).astype(BF)


def outback(o, ga, pieces):
    tokens = o.shape[0]
    col = pl.BlockSpec((tokens, 256), lambda i: (0, i))
    return pl.pallas_call(
        functools.partial(outback_body, len(pieces)),
        grid=(D // 256,),
        in_specs=[col, whole((tokens, D))] + [ANY] * len(pieces),
        out_specs=[col, pl.BlockSpec((256, D), lambda i: (i, 0))],
        out_shape=[jax.ShapeDtypeStruct((tokens, D), BF), jax.ShapeDtypeStruct((D, D), BF)],
        scratch_shapes=[pltpu.VMEM((D, D), BF), pltpu.SemaphoreType.DMA((len(pieces),))],
        compiler_params=params(),
        cost_estimate=cost(4 * tokens * D * D, 6 * tokens * D),
        name="outback",
    )(o, ga, *pieces)


def split3(values):
    first = values.astype(BF)
    rest = values - first.astype(F32)
    second = rest.astype(BF)
    third = (rest - second.astype(F32)).astype(BF)
    return first, second, third


def attback_body(
    q_ref,
    k_ref,
    v_ref,
    segq_ref,
    segk_ref,
    o_ref,
    lse_ref,
    go_ref,
    rq_ref,
    rk_ref,
    qgain_ref,
    kgain_ref,
    g_ref,
    dgain_ref,
    gqt,
    gk,
    gv,
):
    tokens = o_ref.shape[0]
    low = low_half(tokens)
    lane = lax.broadcasted_iota(jnp.int32, (tokens, PAIR), 1)
    q, k, v, go = q_ref[0], k_ref[0], v_ref[0], go_ref[...]
    zero = jnp.zeros_like(q)
    product = o_ref[...].astype(F32) * go.astype(F32)
    minus = jnp.where(lane < 3, BF(-1.0), zero)
    for head in range(2):
        mine = low if head == 0 else jnp.logical_not(low)
        at = head * HD
        hi, mid, lo = split3(lse_ref[:, at : at + 1])
        segq = segq_ref[...]
        for place, piece in ((65, hi), (66, mid), (67, lo)):
            segq = jnp.where(lane == place, piece, segq)
        q_mine = jnp.where(mine, q, zero)
        go_mine = jnp.where(mine, go, zero)
        k_mine = jnp.where(mine, k, zero)
        q_wide = jnp.concatenate([q_mine, segq], axis=1)
        inner = jnp.sum(jnp.where(mine, product, 0.0), axis=-1, keepdims=True)
        extra = zero
        for place, piece in enumerate(split3(inner)):
            extra = jnp.where(lane == place, piece, extra)
        go_wide = jnp.concatenate([go_mine, extra], axis=1)
        for block in range(tokens // ROWS):
            rows = slice(block * ROWS, block * ROWS + ROWS)
            k_wide = jnp.concatenate([k[rows], segk_ref[rows, :]], axis=1)
            v_wide = jnp.concatenate([v[rows], minus[rows]], axis=1)
            p = jnp.exp2(dot(k_wide, q_wide, NT) * LOG2E)
            gs = (p * dot(v_wide, go_wide, NT)).astype(BF)
            value_part = dot(p.astype(BF), go_mine, NN)
            key_part = dot(gs, q_mine, NN)
            query_part = dot(k_mine[rows], gs, TN)
            if head == 0:
                gv[rows, :] = value_part
                gk[rows, :] = key_part
            else:
                gv[rows, :] += value_part
                gk[rows, :] += key_part
            if head == 0 and block == 0:
                gqt[...] = query_part
            else:
                gqt[...] += query_part
    g_ref[2] = gv[...].astype(BF)
    gq = gqt[...].T * 0.125
    pieces = (
        (0, gq, q.astype(F32) * 8.0, qgain_ref[...], rq_ref[0]),
        (1, gk[...], k.astype(F32), kgain_ref[...], rk_ref[0]),
    )
    for part, grad, normed, gain, rstd in pieces:
        hat = normed / gain
        t = grad * gain
        dgain_ref[part] = jnp.broadcast_to(jnp.sum(grad * hat, axis=0, keepdims=True), (8, PAIR))
        g_ref[part] = (rstd * (t - pair_mean(t, low) - hat * pair_mean(t * hat, low))).astype(BF)


def attback(qkv, segq, segk, o, lse, go, rstd, qgain, kgain):
    tokens = o.shape[0]

    def part(which):
        return pl.BlockSpec((1, tokens, PAIR), lambda i: (which, 0, i))

    col = pl.BlockSpec((tokens, PAIR), lambda i: (0, i))
    seg = whole((tokens, PAIR))
    return pl.pallas_call(
        attback_body,
        grid=(PAIRS,),
        in_specs=[part(0), part(1), part(2), seg, seg, col, col, col, part(0), part(1)]
        + [whole((1, PAIR))] * 2,
        out_specs=[
            pl.BlockSpec((3, tokens, PAIR), lambda i: (0, 0, i)),
            pl.BlockSpec((2, 8, PAIR), lambda i: (0, 0, i)),
        ],
        out_shape=[
            jax.ShapeDtypeStruct((3, tokens, D), BF),
            jax.ShapeDtypeStruct((2, 8, D), F32),
        ],
        scratch_shapes=[
            pltpu.VMEM((PAIR, tokens), F32),
            pltpu.VMEM((tokens, PAIR), F32),
            pltpu.VMEM((tokens, PAIR), F32),
        ],
        compiler_params=params(),
        cost_estimate=cost(
            HEADS * tokens * tokens * 256 * 10, 30 * tokens * D, HEADS * tokens * tokens
        ),
        name="attback",
    )(qkv, qkv, qkv, segq, segk, o, lse, go, rstd, rstd, qgain, kgain)


def qkvgrad_body(h_ref, g_ref, dw_ref, db_ref, ht):
    @pl.when(pl.program_id(0) == 0)
    def _():
        ht[...] = h_ref[...].T

    g = g_ref[0]
    dw_ref[...] = dot(ht[...], g, NN).astype(BF)
    db_ref[...] = jnp.sum(g.astype(F32), axis=0, keepdims=True)


def qkvgrad(h, g):
    tokens = h.shape[0]
    return pl.pallas_call(
        qkvgrad_body,
        grid=(3, 3),
        in_specs=[
            whole((tokens, D)),
            pl.BlockSpec((1, tokens, 256), lambda i, j: (i, 0, j)),
        ],
        out_specs=[
            pl.BlockSpec((D, 256), lambda i, j: (0, 3 * i + j)),
            pl.BlockSpec((1, 256), lambda i, j: (0, 3 * i + j)),
        ],
        out_shape=[
            jax.ShapeDtypeStruct((D, 3 * D), BF),
            jax.ShapeDtypeStruct((1, 3 * D), F32),
        ],
        scratch_shapes=[pltpu.VMEM((D, tokens), BF)],
        compiler_params=params("arbitrary", "arbitrary"),
        cost_estimate=cost(6 * tokens * D * D, 14 * tokens * D),
        name="qkvgrad",
    )(h, g)


def back_body(count, *refs):
    g_ref, x_ref, gx1_ref = refs[:3]
    pieces = refs[3 : 3 + count]
    gain_ref, gx_ref, dvec_ref, full, sems = refs[3 + count :]
    step = pl.program_id(0)

    @pl.when(step == 0)
    def _():
        for item in fetch(pieces, full, sems):
            item.wait()
        dvec_ref[...] = jnp.zeros_like(dvec_ref)

    g = dot(g_ref[0], full[:, :D], NT)
    g += dot(g_ref[1], full[:, D : 2 * D], NT)
    g += dot(g_ref[2], full[:, 2 * D :], NT)
    center, rstd = stats(x_ref[...].astype(F32))
    hat = center * rstd
    t = g * gain_ref[...]
    gx = gx1_ref[...] + rstd * (
        t - jnp.mean(t, axis=-1, keepdims=True) - hat * jnp.mean(t * hat, axis=-1, keepdims=True)
    )
    gx_ref[...] = gx.astype(BF)
    dvec_ref[0:1, :] += jnp.sum(g * hat, axis=0, keepdims=True)
    dvec_ref[1:2, :] += jnp.sum(g, axis=0, keepdims=True)


def back(g, x, gx1, pieces, gain):
    tokens = x.shape[0]
    row = pl.BlockSpec((ROWS, D), lambda i: (i, 0))
    return pl.pallas_call(
        functools.partial(back_body, len(pieces)),
        grid=(tokens // ROWS,),
        in_specs=[pl.BlockSpec((3, ROWS, D), lambda i: (0, i, 0)), row, row]
        + [ANY] * len(pieces)
        + [whole((1, D))],
        out_specs=[row, whole((2, D))],
        out_shape=[jax.ShapeDtypeStruct((tokens, D), BF), jax.ShapeDtypeStruct((2, D), F32)],
        scratch_shapes=[pltpu.VMEM((D, 3 * D), BF), pltpu.SemaphoreType.DMA((len(pieces),))],
        compiler_params=params(),
        cost_estimate=cost(6 * tokens * D * D, 16 * tokens * D, tokens),
        name="back",
    )(g, x, gx1, *pieces, gain)


CHUNKS = 12
RANK_ROWS = 192
STAGES_AT = (0, 1, 4, 6, 7, 9, 11, 12, 14)
ATT_TICK, BACK_TICK, SMALL_TICK = 3, 18, 22
TICKS = BACK_TICK + STAGES_AT[-1] + 2


def finish_body(count, *refs):
    (
        o_ref,
        ga_ref,
        q_ref,
        k_ref,
        v_ref,
        segq_ref,
        segk_ref,
        opair_ref,
        lse_ref,
        rq_ref,
        rk_ref,
        qgain_ref,
        kgain_ref,
        h_ref,
        x_ref,
        gx1_ref,
        gain_ref,
        dubias_ref,
        dvec_ref,
        up_ref,
        down_ref,
    ) = refs[:21]
    out_pieces = refs[21 : 21 + count]
    qkv_pieces = refs[21 + count : 21 + 2 * count]
    (
        gx_ref,
        total_ref,
        small_ref,
        out_full,
        qkv_full,
        go,
        g3,
        ht,
        gqt,
        gk,
        gv,
        own,
        held,
        r0,
        r1,
        r2,
        r3,
        r4,
        done,
        small,
        rsmall,
        weight_sems,
        local_sems,
        send_sems,
        recv_sems,
        done_sems,
        ssend_sems,
        srecv_sems,
    ) = refs[21 + 2 * count :]
    tick = pl.program_id(0)
    tokens = o_ref.shape[0]

    rank, group = lax.axis_index("fsdp"), lax.axis_index("dp")
    c, x = rank % 2, rank // 2
    y, z1, z2 = group % 2, (group // 2) % 2, group // 4
    partners = (
        {"fsdp": flip(rank, 1)},
        {"fsdp": flip(rank, 2)},
        {"dp": flip(group, 1)},
        {"dp": flip(group, 2)},
        {"dp": flip(group, 4)},
    )
    row_y = pl.multiple_of(y * 96, 48)
    other_y = pl.multiple_of((1 - y) * 96, 48)
    row_z = pl.multiple_of(y * 96 + z1 * 48, 48)
    other_z = pl.multiple_of(y * 96 + (1 - z1) * 48, 48)
    col_z = pl.multiple_of(z2 * 384, 384)
    other_col = pl.multiple_of((1 - z2) * 384, 384)

    def remote(stage, chunk, src, dst, partner):
        return pltpu.make_async_remote_copy(
            src_ref=src,
            dst_ref=dst,
            send_sem=send_sems.at[stage, chunk],
            recv_sem=recv_sems.at[stage, chunk],
            device_id=partners[partner],
            device_id_type=pl.DeviceIdType.MESH,
        )

    def first_send(source, place, chunk):
        return remote(0, chunk, source.at[place, :, 1 - c], r0.at[chunk], 0)

    def sends(stage, chunk):
        if stage == 1:
            return remote(1, chunk, held.at[chunk, 1 - x], r1.at[chunk], 1)
        if stage == 2:
            return remote(2, chunk, held.at[chunk, x, pl.ds(other_y, 96)], r2.at[chunk], 2)
        if stage == 3:
            return remote(3, chunk, held.at[chunk, x, pl.ds(other_z, 48)], r3.at[chunk], 3)
        if stage == 4:
            src = held.at[chunk, x, pl.ds(row_z, 48), pl.ds(other_col, 384)]
            return remote(4, chunk, src, r4.at[chunk], 4)
        if stage == 5:
            place = done.at[chunk, pl.ds(row_z, 48), pl.ds(col_z, 384)]
            return remote(5, chunk, place, place, 4)
        if stage == 6:
            place = done.at[chunk, pl.ds(row_z, 48)]
            return remote(6, chunk, place, place, 3)
        place = done.at[chunk, pl.ds(row_y, 96)]
        return remote(7, chunk, place, place, 2)

    def stored(chunk):
        return pltpu.make_async_copy(done.at[chunk], total_ref.at[chunk], done_sems.at[chunk])

    def add(left, right):
        return (left.astype(F32) + right.astype(F32)).astype(BF)

    sources = (
        (up_ref, 0, 4, 0),
        (down_ref, 4, 6, 4),
        (own, 6, 7, 6),
        (down_ref, 7, 9, 5),
        (own, 9, CHUNKS, 8),
    )

    def start_chunk(chunk):
        for source, begin, end, base in sources:

            @pl.when((chunk >= begin) & (chunk < end))
            def _(source=source, base=base):
                place = chunk - base
                first_send(source, place, chunk).start()
                pltpu.make_async_copy(
                    source.at[place, :, c], held.at[chunk], local_sems.at[chunk]
                ).start()

    def pass_on(stage, chunk):
        if stage == 1:
            for source, begin, end, base in sources:

                @pl.when((chunk >= begin) & (chunk < end))
                def _(source=source, base=base):
                    place = chunk - base
                    first_send(source, place, chunk).wait()
                    pltpu.make_async_copy(
                        source.at[place, :, c], held.at[chunk], local_sems.at[chunk]
                    ).wait()

            def add_rows(i, _):
                rows = pl.ds(pl.multiple_of((i % 4) * 48, 48), 48)
                held[chunk, i // 4, rows, :] = add(
                    held[chunk, i // 4, rows, :], r0[chunk, i // 4, rows, :]
                )
                return 0

            lax.fori_loop(0, 8, add_rows, 0)
        elif stage == 2:
            sends(1, chunk).wait()

            def add_rows(i, _):
                rows = pl.ds(pl.multiple_of(i * 48, 48), 48)
                held[chunk, x, rows, :] = add(held[chunk, x, rows, :], r1[chunk, rows, :])
                return 0

            lax.fori_loop(0, 4, add_rows, 0)
        elif stage == 3:
            sends(2, chunk).wait()

            def add_rows(i, _):
                rows = pl.ds(pl.multiple_of(row_y + i * 48, 48), 48)
                came = pl.ds(pl.multiple_of(i * 48, 48), 48)
                held[chunk, x, rows, :] = add(held[chunk, x, rows, :], r2[chunk, came, :])
                return 0

            lax.fori_loop(0, 2, add_rows, 0)
        elif stage == 4:
            sends(3, chunk).wait()
            rows = pl.ds(row_z, 48)
            held[chunk, x, rows, :] = add(held[chunk, x, rows, :], r3[chunk])
        elif stage == 5:
            sends(4, chunk).wait()
            rows, cols = pl.ds(row_z, 48), pl.ds(col_z, 384)
            done[chunk, rows, cols] = add(held[chunk, x, rows, cols], r4[chunk])
        else:
            sends(stage - 1, chunk).wait()
        if stage < 8:
            sends(stage, chunk).start()
        else:
            stored(chunk).start()

    def small_send(step):
        return pltpu.make_async_remote_copy(
            src_ref=small.at[step],
            dst_ref=rsmall.at[step],
            send_sem=ssend_sems.at[step],
            recv_sem=srecv_sems.at[step],
            device_id=partners[step],
            device_id_type=pl.DeviceIdType.MESH,
        )

    def weights(which):
        full, pieces = ((out_full, out_pieces), (qkv_full, qkv_pieces))[which]
        if count == 1:
            return [pltpu.make_async_copy(pieces[0], full, weight_sems.at[which, 0])]
        rows = full.shape[0] // count
        return [
            pltpu.make_async_copy(
                piece,
                full.at[pl.ds(pl.multiple_of(flip(rank, distance) * rows, rows), rows)],
                weight_sems.at[which, distance],
            )
            for distance, piece in enumerate(pieces)
        ]

    @pl.when(tick == 0)
    def _():
        barrier = pltpu.get_barrier_semaphore()
        for partner in partners:
            pl.semaphore_signal(
                barrier, inc=1, device_id=partner, device_id_type=pl.DeviceIdType.MESH
            )
        for item in weights(0) + weights(1):
            item.start()
        small[0] = jnp.zeros_like(small[0])
        pl.semaphore_wait(barrier, len(partners))

    for stage in reversed(range(9)):
        moment = tick - STAGES_AT[stage]

        chunk = (moment * 11 + 17) // 18

        @pl.when((moment >= 0) & (chunk < CHUNKS) & (chunk * 18 // 11 == moment))
        def _(stage=stage, chunk=chunk):
            if stage == 0:
                start_chunk(chunk)
            else:
                pass_on(stage, chunk)

    @pl.when(tick < ATT_TICK)
    def _():
        @pl.when(tick == 0)
        def _():
            for item in weights(0):
                item.wait()

        start = pl.multiple_of(tick * 256, 256)
        block = pl.ds(start, 256)
        go[:, block] = dot(ga_ref[...], out_full[block, :], NT).astype(BF)
        dout = dot(o_ref[:, block], ga_ref[...], TN).astype(BF)
        for part in range(4):
            piece = dout[part * 64 : part * 64 + 64]
            row = tick * 256 + part * 64
            shard = row // RANK_ROWS
            own[
                2,
                shard // 2,
                shard % 2,
                pl.ds(pl.multiple_of(row % RANK_ROWS, 64), 64),
                :,
            ] = piece

    turn = (tick - ATT_TICK) // 5
    place_in_turn = (tick - ATT_TICK) % 5

    @pl.when((tick >= ATT_TICK) & (tick < BACK_TICK) & (place_in_turn < 4))
    def _():
        pair = 2 * turn + place_in_turn // 2
        head = place_in_turn % 2
        pair_cols = pl.ds(pl.multiple_of(pair * PAIR, PAIR), PAIR)
        lane = lax.broadcasted_iota(jnp.int32, (tokens, PAIR), 1)
        mine = lane // HD == head
        q, k, v, go_pair = q_ref[0], k_ref[0], v_ref[0], go[:, pair_cols]
        zero = jnp.zeros_like(q)
        minus = jnp.where(lane < 3, BF(-1.0), zero)

        @pl.when(head == 0)
        def _():
            gqt[...] = jnp.zeros_like(gqt)
            gk[...] = jnp.zeros_like(gk)
            gv[...] = jnp.zeros_like(gv)

        product = opair_ref[...].astype(F32) * go_pair.astype(F32)
        inner = jnp.sum(jnp.where(mine, product, 0.0), axis=-1, keepdims=True)
        logs = jnp.sum(jnp.where(lane == head * HD, lse_ref[...], 0.0), axis=-1, keepdims=True)
        segq = segq_ref[...]
        for place, piece in enumerate(split3(logs)):
            segq = jnp.where(lane == 65 + place, piece, segq)
        extra = zero
        for place, piece in enumerate(split3(inner)):
            extra = jnp.where(lane == place, piece, extra)
        q_mine = jnp.where(mine, q, zero)
        go_mine = jnp.where(mine, go_pair, zero)
        k_mine = jnp.where(mine, k, zero)
        q_wide = jnp.concatenate([q_mine, segq], axis=1)
        go_wide = jnp.concatenate([go_mine, extra], axis=1)
        for block in range(tokens // ROWS):
            rows = slice(block * ROWS, block * ROWS + ROWS)
            k_wide = jnp.concatenate([k[rows], segk_ref[rows, :]], axis=1)
            v_wide = jnp.concatenate([v[rows], minus[rows]], axis=1)
            p = jnp.exp2(dot(k_wide, q_wide, NT) * LOG2E)
            gs = (p * dot(v_wide, go_wide, NT)).astype(BF)
            gv[rows, :] += dot(p.astype(BF), go_mine, NN)
            gk[rows, :] += dot(gs, q_mine, NN)
            gqt[...] += dot(k_mine[rows], gs, TN)

        @pl.when(head == 1)
        def _():
            low = low_half(tokens)
            g3[2, :, pair_cols] = gv[...].astype(BF)
            gq = gqt[...].T * 0.125
            pieces = (
                (0, gq, q.astype(F32) * 8.0, qgain_ref[...], rq_ref[0]),
                (1, gk[...], k.astype(F32), kgain_ref[...], rk_ref[0]),
            )
            for part, grad, normed, gain, rstd in pieces:
                hat = normed / gain
                t = grad * gain
                lanes = slice(part * PAIR, part * PAIR + PAIR)
                small[0, 5:6, lanes] += jnp.sum(grad * hat, axis=0, keepdims=True)
                g3[part, :, pair_cols] = (
                    rstd * (t - pair_mean(t, low) - hat * pair_mean(t * hat, low))
                ).astype(BF)

    @pl.when((tick >= ATT_TICK) & (tick < BACK_TICK) & (place_in_turn == 4))
    def _():
        @pl.when(turn == 0)
        def _():
            ht[...] = h_ref[...].T

        cols = pl.ds(pl.multiple_of(turn * 256, 256), 256)
        for part in range(3):
            g = g3[part, :, cols]
            own[turn + turn // 2, :, :, :, part * 256 : part * 256 + 256] = (
                dot(ht[...], g, NN).astype(BF).reshape(2, 2, RANK_ROWS, 256)
            )
            small[0, 2 + part : 3 + part, cols] = jnp.sum(g.astype(F32), axis=0, keepdims=True)

    @pl.when((tick >= BACK_TICK) & (tick < SMALL_TICK))
    def _():
        @pl.when(tick == BACK_TICK)
        def _():
            for item in weights(1):
                item.wait()

        rows = pl.ds(pl.multiple_of((tick - BACK_TICK) * ROWS, ROWS), ROWS)
        g = dot(g3[0, rows, :], qkv_full[:, :D], NT)
        g += dot(g3[1, rows, :], qkv_full[:, D : 2 * D], NT)
        g += dot(g3[2, rows, :], qkv_full[:, 2 * D :], NT)
        center, rstd = stats(x_ref[...].astype(F32))
        hat = center * rstd
        t = g * gain_ref[...]
        gx = gx1_ref[...] + rstd * (
            t
            - jnp.mean(t, axis=-1, keepdims=True)
            - hat * jnp.mean(t * hat, axis=-1, keepdims=True)
        )
        gx_ref[...] = gx.astype(BF)
        small[0, 0:1, :] += jnp.sum(g * hat, axis=0, keepdims=True)
        small[0, 1:2, :] += jnp.sum(g, axis=0, keepdims=True)

    @pl.when(tick == SMALL_TICK)
    def _():
        small[0, 6:10, :] = dvec_ref[...]
        for part in range(4):
            small[0, 10 + part : 11 + part, :] = dubias_ref[:, part * D : part * D + D]
        small_send(0).start()

    for step in range(5):

        @pl.when(tick == SMALL_TICK + 1 + step)
        def _(step=step):
            small_send(step).wait()
            small[step + 1] = small[step] + rsmall[step]
            if step < 4:
                small_send(step + 1).start()
            else:
                small_ref[...] = small[5]

    @pl.when(tick == TICKS - 1)
    def _():
        for chunk in range(CHUNKS):
            stored(chunk).wait()


def finish(o, ga, qkv, segq, segk, lse, rstd, qgain, kgain, h, x, gx1, gain, dubias, dvec, dup, ddown, outs, qkvs):
    tokens = o.shape[0]
    count = len(outs)
    split = (dup.shape[0], 2, 2, RANK_ROWS, D)

    def pair_of(i):
        after = jnp.clip(i - ATT_TICK, 0, BACK_TICK - ATT_TICK - 1)
        return 2 * (after // 5) + jnp.minimum(after % 5, 3) // 2

    def part(which):
        return pl.BlockSpec((1, tokens, PAIR), lambda i: (which, 0, pair_of(i)))

    col = pl.BlockSpec((tokens, PAIR), lambda i: (0, pair_of(i)))
    row = pl.BlockSpec(
        (ROWS, D), lambda i: (jnp.clip(i - BACK_TICK, 0, tokens // ROWS - 1), 0)
    )
    act = single((tokens, D))
    seg = single((tokens, PAIR))
    grid = pl.GridSpec(
        grid=(TICKS,),
        in_specs=[act, act, part(0), part(1), part(2), seg, seg, col, col, part(0), part(1)]
        + [single((1, PAIR))] * 2
        + [act, row, row, single((1, D)), single((1, 4 * D)), single((4, D)), ANY, ANY]
        + [ANY] * (2 * count),
        out_specs=[row, ANY, single((16, D))],
        scratch_shapes=[
            pltpu.VMEM((D, D), BF),
            pltpu.VMEM((D, 3 * D), BF),
            pltpu.VMEM((tokens, D), BF),
            pltpu.VMEM((3, tokens, D), BF),
            pltpu.VMEM((D, tokens), BF),
            pltpu.VMEM((PAIR, tokens), F32),
            pltpu.VMEM((tokens, PAIR), F32),
            pltpu.VMEM((tokens, PAIR), F32),
            pltpu.VMEM((4, 2, 2, RANK_ROWS, D), BF),
            pltpu.VMEM((CHUNKS, 2, RANK_ROWS, D), BF),
            pltpu.VMEM((CHUNKS, 2, RANK_ROWS, D), BF),
            pltpu.VMEM((CHUNKS, RANK_ROWS, D), BF),
            pltpu.VMEM((CHUNKS, 96, D), BF),
            pltpu.VMEM((CHUNKS, 48, D), BF),
            pltpu.VMEM((CHUNKS, 48, D // 2), BF),
            pltpu.VMEM((CHUNKS, RANK_ROWS, D), BF),
            pltpu.VMEM((6, 16, D), F32),
            pltpu.VMEM((5, 16, D), F32),
            pltpu.SemaphoreType.DMA((2, count)),
            pltpu.SemaphoreType.DMA((CHUNKS,)),
            pltpu.SemaphoreType.DMA((8, CHUNKS)),
            pltpu.SemaphoreType.DMA((8, CHUNKS)),
            pltpu.SemaphoreType.DMA((CHUNKS,)),
            pltpu.SemaphoreType.DMA((5,)),
            pltpu.SemaphoreType.DMA((5,)),
        ],
    )
    return pl.pallas_call(
        functools.partial(finish_body, count),
        grid_spec=grid,
        out_shape=[
            jax.ShapeDtypeStruct((tokens, D), BF),
            jax.ShapeDtypeStruct((CHUNKS, RANK_ROWS, D), BF),
            jax.ShapeDtypeStruct((16, D), F32),
        ],
        compiler_params=pltpu.CompilerParams(
            dimension_semantics=("arbitrary",),
            vmem_limit_bytes=63 * 1024 * 1024,
            collective_id=1,
            has_side_effects=True,
        ),
        name="finish",
    )(
        o, ga, qkv, qkv, qkv, segq, segk, o, lse, rstd, rstd, qgain, kgain, h, x, gx1, gain,
        dubias, dvec, dup.reshape(split), ddown.reshape(split), *outs, *qkvs,
    )


def unpack_body(total_ref, up_ref, down_ref, out_ref, qkv_ref):
    for chunk in range(CHUNKS):
        block = total_ref[chunk].astype(F32)
        if chunk < 4:
            up_ref[:, chunk * D : chunk * D + D] = block
        elif chunk in (4, 5, 7, 8):
            down_ref[chunk - 4 - chunk // 7] = block
        elif chunk == 10:
            out_ref[...] = block
        else:
            turn = (6, 9, 11).index(chunk)
            for part in range(3):
                at = part * D + turn * 256
                qkv_ref[:, at : at + 256] = block[:, part * 256 : part * 256 + 256]


def unpack(totals):
    step = 48

    def rows(columns):
        return pl.BlockSpec((step, columns), lambda i: (i, 0))

    return pl.pallas_call(
        unpack_body,
        grid=(RANK_ROWS // step,),
        in_specs=[pl.BlockSpec((CHUNKS, step, D), lambda i: (0, i, 0))],
        out_specs=[
            rows(4 * D),
            pl.BlockSpec((4, step, D), lambda i: (0, i, 0)),
            rows(D),
            rows(3 * D),
        ],
        out_shape=[
            jax.ShapeDtypeStruct((RANK_ROWS, 4 * D), F32),
            jax.ShapeDtypeStruct((4, RANK_ROWS, D), F32),
            jax.ShapeDtypeStruct((RANK_ROWS, D), F32),
            jax.ShapeDtypeStruct((RANK_ROWS, 3 * D), F32),
        ],
        compiler_params=params(),
        name="unpack",
    )(totals)


FRONT_TICK, PAIR_TICK, MID_TICK, BEGIN_TICKS = 1, 5, 11, 15
OWN_CORE, OVER_X, OVER_Y, X_CORE, Y_CORE = range(5)


def begin_body(
    x_ref,
    segq_ref,
    segk_ref,
    pack_ref,
    wq_ref,
    wo_ref,
    wu_ref,
    wd_ref,
    h_ref,
    qkv_ref,
    rstd_ref,
    o_ref,
    lse_ref,
    x1_ref,
    h2_ref,
    gain1_ref,
    gain2_ref,
    dbias_ref,
    qgain_ref,
    kgain_ref,
    ubias_ref,
    wq_out,
    wo_out,
    wu_out,
    wd_out,
    wq,
    wo,
    wu,
    wd,
    pack,
    vecs,
    qkv,
    mixed,
    send_sems,
    recv_sems,
    local_sems,
    out_sems,
):
    tick = pl.program_id(0)
    tokens = x_ref.shape[0]
    rank, group = lax.axis_index("fsdp"), lax.axis_index("dp")
    y = group % 2
    across = flip(rank, 2)
    partners = ({"fsdp": flip(rank, 1)}, {"fsdp": across}, {"dp": flip(group, 1)})
    shards = (wq_ref, wo_ref, wu_ref, wd_ref, pack_ref)
    fulls = (wq, wo, wu, wd, pack)
    outs = (wq_out, wo_out, wu_out, wd_out)
    QKV, OUT, UP, DOWN, PACK = range(5)

    def remote(which, event, src, dst, partner):
        return pltpu.make_async_remote_copy(
            src_ref=src,
            dst_ref=dst,
            send_sem=send_sems.at[which, event],
            recv_sem=recv_sems.at[which, event],
            device_id=partners[partner],
            device_id_type=pl.DeviceIdType.MESH,
        )

    def event(which, kind):
        shard, full = shards[which], fulls[which]
        if which == PACK:
            if kind == X_CORE:
                return remote(which, kind, full.at[across], full.at[across], 0)
            return remote(which, kind, shard, full.at[rank], kind)
        half = full.shape[1] // 2
        near = pl.ds(pl.multiple_of(y * half, half), half)
        far = pl.ds(pl.multiple_of((1 - y) * half, half), half)
        if kind == OWN_CORE:
            return remote(which, kind, shard, full.at[rank], 0)
        if kind == OVER_X:
            return remote(which, kind, shard.at[near], full.at[rank, near], 1)
        place = full.at[across, far if kind == Y_CORE else near]
        return remote(which, kind, place, place, 2 if kind == OVER_Y else 0)

    def own(which):
        return pltpu.make_async_copy(shards[which], fulls[which].at[rank], local_sems.at[which])

    def stored(which):
        return pltpu.make_async_copy(fulls[which], outs[which], out_sems.at[which])

    def complete(which):
        for kind in (OWN_CORE, X_CORE, Y_CORE):
            event(which, kind).wait()
        own(which).wait()
        stored(which).start()

    @pl.when(tick == 0)
    def _():
        barrier = pltpu.get_barrier_semaphore()
        for partner in partners:
            pl.semaphore_signal(
                barrier, inc=1, device_id=partner, device_id_type=pl.DeviceIdType.MESH
            )
        for which in (PACK, QKV, OUT, UP, DOWN):
            own(which).start()
        pl.semaphore_wait(barrier, len(partners))
        for kind in (OWN_CORE, OVER_X):
            event(PACK, kind).start()
            event(QKV, kind).start()
        event(PACK, OVER_X).wait()
        event(PACK, X_CORE).start()
        own(PACK).wait()
        event(PACK, OWN_CORE).wait()
        event(PACK, X_CORE).wait()

        held = [pack[shard].astype(F32) for shard in range(4)]
        lane = lax.broadcasted_iota(jnp.int32, (256, D), 1)
        line = lax.broadcasted_iota(jnp.int32, (256, D), 0)
        total = jnp.zeros((16, D), F32)
        for slot in range(4):
            rows = [held[slot][0:6]]
            for part in range(3):
                shard, piece = (4 * part + slot) // 3, (4 * part + slot) % 3
                rows.append(held[shard][6 + piece : 7 + piece])
            for part in range(4):
                rows.append(held[part][9 + slot : 10 + slot])
            rows.append(jnp.zeros((3, 256), F32))
            chosen = jnp.where((lane == line + slot * 192) & (line < 192), BF(1.0), BF(0.0))
            total += dot(jnp.concatenate(rows, axis=0).astype(BF), chosen, NN)
        vecs[...] = total
        lane, line = lane[:, :PAIR], line[:, :PAIR]
        heads = jnp.zeros((16, PAIR), F32)
        for shard in range(4):
            chosen = jnp.where((lane % HD == line + shard * 16) & (line < 16), BF(1.0), BF(0.0))
            heads += dot(pack[shard], chosen, NN)
        gain1_ref[...] = total[0:1]
        gain2_ref[...] = total[3:4]
        dbias_ref[...] = total[5:6]
        for part in range(4):
            ubias_ref[:, part * D : part * D + D] = total[9 + part : 10 + part]
        qgain_ref[...] = heads[13:14]
        kgain_ref[...] = heads[14:15]

        event(QKV, OVER_X).wait()
        event(QKV, OVER_Y).start()
        event(QKV, X_CORE).start()
        for which in (OUT, UP):
            event(which, OVER_X).start()
        for which in (OUT, UP, DOWN):
            event(which, OWN_CORE).start()
        event(QKV, OVER_Y).wait()
        event(QKV, Y_CORE).start()
        complete(QKV)

    @pl.when(tick == 2)
    def _():
        for which in (OUT, UP):
            event(which, OVER_X).wait()
            event(which, OVER_Y).start()
            event(which, X_CORE).start()
        event(DOWN, OVER_X).start()

    @pl.when(tick == 7)
    def _():
        for which in (OUT, UP):
            event(which, OVER_Y).wait()
            event(which, Y_CORE).start()
        event(DOWN, OVER_X).wait()
        event(DOWN, OVER_Y).start()
        event(DOWN, X_CORE).start()

    @pl.when(tick == MID_TICK)
    def _():
        complete(OUT)

    @pl.when(tick == MID_TICK + 1)
    def _():
        complete(UP)

    @pl.when(tick == MID_TICK + 2)
    def _():
        event(DOWN, OVER_Y).wait()
        event(DOWN, Y_CORE).start()

    @pl.when((tick >= FRONT_TICK) & (tick < PAIR_TICK))
    def _():
        rows = pl.ds(pl.multiple_of((tick - FRONT_TICK) * ROWS, ROWS), ROWS)
        center, rstd = stats(x_ref[rows, :].astype(F32))
        h = (center * rstd * vecs[0:1, :] + vecs[1:2, :]).astype(BF)
        h_ref[...] = h
        low = low_half(ROWS)
        for part in range(3):
            for block in range(D // 256):
                at = part * D + block * 256
                weight = wq[:, :, at : at + 256].reshape(D, 256)
                y_block = dot(h, weight, NN) + vecs[
                    6 + part : 7 + part, block * 256 : block * 256 + 256
                ]
                if part == 2:
                    value = y_block.astype(BF)
                    qkv_ref[2, :, block * 256 : block * 256 + 256] = value
                    qkv[2, rows, block * 256 : block * 256 + 256] = value
                    continue
                gain = (qgain_ref, kgain_ref)[part][...]
                for half in range(2):
                    tile = y_block[:, half * PAIR : half * PAIR + PAIR]
                    cols = slice(block * 256 + half * PAIR, block * 256 + half * PAIR + PAIR)
                    c = tile - pair_mean(tile, low)
                    r = lax.rsqrt(pair_mean(c * c, low) + EPS)
                    normed = (c * r * gain).astype(BF)
                    if part == 0:
                        normed = normed * BF(0.125)
                    qkv_ref[part, :, cols] = normed
                    qkv[part, rows, cols] = normed
                    rstd_ref[part, :, cols] = r

    @pl.when((tick >= PAIR_TICK) & (tick < MID_TICK))
    def _():
        pair_cols = pl.ds(pl.multiple_of((tick - PAIR_TICK) * PAIR, PAIR), PAIR)
        low = low_half(tokens)
        keys = jnp.concatenate([qkv[1, :, pair_cols], segk_ref[...]], axis=1)
        values = qkv[2, :, pair_cols]
        one = jnp.ones_like(values)
        values_a = jnp.where(low, values, one)
        values_b = jnp.where(low, one, values)
        low_rows = low_half(ROWS)
        for block in range(tokens // ROWS):
            rows = slice(block * ROWS, block * ROWS + ROWS)
            q = qkv[0, rows, pair_cols]
            seg = segq_ref[rows, :]
            zero = jnp.zeros_like(q)
            sa = dot(jnp.concatenate([jnp.where(low_rows, q, zero), seg], axis=1), keys, NT)
            acc_a = dot(jnp.exp2(sa * LOG2E).astype(BF), values_a, NN)
            sb = dot(jnp.concatenate([jnp.where(low_rows, zero, q), seg], axis=1), keys, NT)
            acc_b = dot(jnp.exp2(sb * LOG2E).astype(BF), values_b, NN)
            top = jnp.where(low_rows, acc_a, acc_b)
            sums = pltpu.roll(jnp.where(low_rows, acc_b, acc_a), HD, 1)
            sums = jnp.where(sums > 0, sums, 1.0)
            value = (top / sums).astype(BF)
            o_ref[rows, :] = value
            mixed[rows, pair_cols] = value
            lse_ref[rows, :] = jnp.log(sums)

    @pl.when(tick >= MID_TICK)
    def _():
        rows = pl.ds(pl.multiple_of((tick - MID_TICK) * ROWS, ROWS), ROWS)
        x1 = (
            x_ref[rows, :].astype(F32)
            + dot(mixed[rows, :], wo[...].reshape(D, D), NN)
            + vecs[2:3, :]
        )
        x1_ref[...] = x1
        center, rstd = stats(x1)
        h2_ref[...] = (center * rstd * vecs[3:4, :] + vecs[4:5, :]).astype(BF)

    @pl.when(tick == BEGIN_TICKS - 1)
    def _():
        complete(DOWN)
        for which in (QKV, OUT, UP, DOWN):
            stored(which).wait()


def begin(x, segq, segk, pack, matrices):
    tokens = x.shape[0]

    def rows(tick):
        return lambda i: jnp.clip(i - tick, 0, tokens // ROWS - 1)

    at_front, at_middle = rows(FRONT_TICK), rows(MID_TICK)
    col = pl.BlockSpec((tokens, PAIR), lambda i: (0, jnp.clip(i - PAIR_TICK, 0, PAIRS - 1)))
    early = pl.BlockSpec((ROWS, D), lambda i: (at_front(i), 0))
    late = pl.BlockSpec((ROWS, D), lambda i: (at_middle(i), 0))
    fulls = [(4,) + matrix.shape for matrix in matrices]
    grid = pl.GridSpec(
        grid=(BEGIN_TICKS,),
        in_specs=[single((tokens, D)), single((tokens, PAIR)), single((tokens, PAIR))] + [ANY] * 5,
        out_specs=[
            early,
            pl.BlockSpec((3, ROWS, D), lambda i: (0, at_front(i), 0)),
            pl.BlockSpec((2, ROWS, D), lambda i: (0, at_front(i), 0)),
            col,
            col,
            late,
            late,
        ]
        + [single((1, D))] * 3
        + [single((1, PAIR))] * 2
        + [single((1, 4 * D))]
        + [ANY] * 4,
        scratch_shapes=[pltpu.VMEM(shape, BF) for shape in fulls]
        + [
            pltpu.VMEM((4, 16, 256), BF),
            pltpu.VMEM((16, D), F32),
            pltpu.VMEM((3, tokens, D), BF),
            pltpu.VMEM((tokens, D), BF),
            pltpu.SemaphoreType.DMA((5, 5)),
            pltpu.SemaphoreType.DMA((5, 5)),
            pltpu.SemaphoreType.DMA((5,)),
            pltpu.SemaphoreType.DMA((4,)),
        ],
    )
    return pl.pallas_call(
        begin_body,
        grid_spec=grid,
        out_shape=[
            jax.ShapeDtypeStruct((tokens, D), BF),
            jax.ShapeDtypeStruct((3, tokens, D), BF),
            jax.ShapeDtypeStruct((2, tokens, D), F32),
            jax.ShapeDtypeStruct((tokens, D), BF),
            jax.ShapeDtypeStruct((tokens, D), F32),
            jax.ShapeDtypeStruct((tokens, D), F32),
            jax.ShapeDtypeStruct((tokens, D), BF),
        ]
        + [jax.ShapeDtypeStruct((1, D), F32)] * 3
        + [jax.ShapeDtypeStruct((1, PAIR), F32)] * 2
        + [jax.ShapeDtypeStruct((1, 4 * D), F32)]
        + [jax.ShapeDtypeStruct(shape, BF) for shape in fulls],
        compiler_params=pltpu.CompilerParams(
            dimension_semantics=("arbitrary",),
            vmem_limit_bytes=60 * 1024 * 1024,
            collective_id=0,
            has_side_effects=True,
        ),
        name="begin",
    )(x, segq, segk, pack, *matrices)


def swap(values, axis, mask, size):
    return lax.ppermute(values, axis, [(i, i ^ mask) for i in range(size)])


def bits_of(size):
    return [1 << b for b in range(size.bit_length() - 1)]


def gather_shards(shard, size):
    held = [shard]
    for mask in reversed(bits_of(size)):
        held = held + [swap(item, "fsdp", mask, size) for item in held]
    order = [0]
    for mask in reversed(bits_of(size)):
        order = order + [place ^ mask for place in order]
    placed = [None] * size
    for place, item in zip(order, held):
        placed[place] = item
    return placed


def reduce_grad(grad, order, sizes):
    fsdp, dp = sizes["fsdp"], sizes["dp"]
    rows, columns = grad.shape
    names = [("fsdp", m) for m in reversed(bits_of(fsdp))] + [
        ("dp", m) for m in reversed(bits_of(dp))
    ]
    held = grad.reshape((2,) * len(names) + (rows // fsdp // dp, columns))
    undo = []
    for step in order:
        axis, mask = step
        place = names.index(step)
        mine = (lax.axis_index(axis) // mask) % 2
        send = lax.dynamic_index_in_dim(held, 1 - mine, place, keepdims=False)
        keep = lax.dynamic_index_in_dim(held, mine, place, keepdims=False)
        held = (
            keep.astype(F32) + swap(send, axis, mask, sizes[axis]).astype(F32)
        ).astype(BF)
        names.pop(place)
        if axis == "dp":
            place -= sum(name == "fsdp" for name, _ in names[:place])
            undo.append((axis, mask, place, mine))
    for axis, mask, place, mine in reversed(undo):
        other = swap(held, axis, mask, sizes[axis])
        first = jnp.where(mine == 0, held, other)
        second = jnp.where(mine == 0, other, held)
        held = jnp.stack([first, second], axis=place)
    return held.reshape(rows // fsdp, columns).astype(F32)


def reduce_small(grad, sizes):
    held = grad.reshape((2,) * len(bits_of(sizes["fsdp"])) + (grad.shape[1],))
    for mask in reversed(bits_of(sizes["fsdp"])):
        mine = (lax.axis_index("fsdp") // mask) % 2
        send = lax.dynamic_index_in_dim(held, 1 - mine, 0, keepdims=False)
        keep = lax.dynamic_index_in_dim(held, mine, 0, keepdims=False)
        held = keep + swap(send, "fsdp", mask, sizes["fsdp"])
    for mask in bits_of(sizes["dp"]):
        held = held + swap(held, "dp", mask, sizes["dp"])
    return held


def local(sizes, *arguments):
    (
        block_input,
        segment_ids,
        norm1_gain,
        norm1_bias,
        qkv_weight,
        qkv_bias,
        query_gain,
        key_gain,
        out_weight,
        out_bias,
        norm2_gain,
        norm2_bias,
        up_weight,
        up_bias,
        down_weight,
        down_bias,
        output_grad,
    ) = arguments
    fsdp = sizes["fsdp"]
    rank = lax.axis_index("fsdp")
    small_args = (
        norm1_gain,
        norm1_bias,
        qkv_bias,
        query_gain,
        key_gain,
        out_bias,
        norm2_gain,
        norm2_bias,
        up_bias,
        down_bias,
    )
    widths = [item.shape[0] for item in small_args]
    lane = jnp.arange(PAIR)[None, :]
    seg_col = segment_ids[:, None]
    match = (seg_col == lane) & (lane < HD)
    segq = jnp.where(match, QMARK, jnp.where(lane == HD, 1.0, 0.0)).astype(BF)
    segk = jnp.where(
        match,
        KMARK,
        jnp.where(lane == HD, -QMARK * KMARK, jnp.where((lane > HD) & (lane <= HD + 3), -1.0, 0.0)),
    ).astype(BF)

    joined = fsdp == 4 and sizes["dp"] == 8
    if joined:
        narrow = [item.reshape(-1, 192) for item in small_args if item.shape[0] >= 192]
        order = (0, 1, 3, 4, 5, 7, 2, 6)
        lines = jnp.pad(jnp.concatenate([narrow[n] for n in order]), ((0, 0), (0, 64)))
        heads = [jnp.pad(item.reshape(1, -1), ((0, 0), (0, 240))) for item in small_args[3:5]]
        pack = jnp.concatenate([lines] + heads + [jnp.zeros((1, 256), BF)])
        (
            h1, qkv, rstd, mixed, lse, x1, h2, gain1, gain2, downb, qgain, kgain, upb, *fulls
        ) = begin(
            block_input, segq, segk, pack, (qkv_weight, out_weight, up_weight, down_weight)
        )
        qkv_pieces, out_pieces, up_pieces, down_pieces = [
            [full.reshape(-1, full.shape[-1])] for full in fulls
        ]
    else:
        packed = jnp.stack(gather_shards(jnp.concatenate(small_args), fsdp))
        packed = packed[jnp.arange(fsdp) ^ rank].astype(F32)
        smalls = []
        at = 0
        for width in widths:
            smalls.append(packed[:, at : at + width].reshape(1, fsdp * width))
            at += width
        gain1, shift1, qkvb, qgain, kgain, outb, gain2, shift2, upb, downb = smalls
        qgain = jnp.concatenate([qgain, qgain], axis=1)
        kgain = jnp.concatenate([kgain, kgain], axis=1)
        qkv_pieces = gather_shards(qkv_weight, fsdp)
        out_pieces = gather_shards(out_weight, fsdp)
        up_pieces = gather_shards(up_weight, fsdp)
        down_pieces = gather_shards(down_weight, fsdp)

        h1, qkv, rstd = front(block_input, gain1, shift1, qkv_pieces, qkvb, qgain, kgain)
        mixed, lse = attend(qkv, segq, segk)
        x1, h2 = middle(mixed, block_input, out_pieces, outb, gain2, shift2)
    output, gx1, ga, dup, ddown, dubias, dvec2 = mlp(
        h2, x1, seg_col, output_grad, up_pieces, down_pieces, upb, downb, gain2, fsdp
    )
    if joined:
        input_grad, totals, small = finish(
            mixed, ga, qkv, segq, segk, lse, rstd, qgain, kgain, h1, block_input, gx1, gain1,
            dubias, dvec2, dup, ddown, out_pieces, qkv_pieces,
        )
        up_total, down_total, out_total, qkv_total = unpack(totals)
        down_total = down_total.reshape(D, D)
        dvec1 = small[0:2]
        dqkvb = small[2:5]
        dgains = small[5, : 2 * PAIR].reshape(2, 2, HD).sum(axis=1)
        dvec2 = small[6:10]
        dubias = small[10:14]
    else:
        go, dout = outback(mixed, ga, out_pieces)
        gqkv, dheads = attback(qkv, segq, segk, mixed, lse, go, rstd, qgain, kgain)
        dqkv, dqkvb = qkvgrad(h1, gqkv)
        input_grad, dvec1 = back(gqkv, block_input, gx1, qkv_pieces, gain1)
        order = [("fsdp", m) for m in bits_of(fsdp)] + [("dp", m) for m in bits_of(sizes["dp"])]
        dup = dup.transpose(1, 2, 0, 3).reshape(D, -1)
        ddown = ddown.transpose(1, 0, 2, 3).reshape(-1, D)
        up_total, down_total, out_total, qkv_total = [
            reduce_grad(grad, order, sizes) for grad in (dup, ddown, dout, dqkv)
        ]
        dgains = dheads[:, 0, :].reshape(2, HEADS, HD).sum(axis=1)

    parts = (
        dvec1[0],
        dvec1[1],
        dqkvb,
        dgains[0],
        dgains[1],
        dvec2[2],
        dvec2[0],
        dvec2[1],
        dubias,
        dvec2[3],
    )
    small = jnp.concatenate([part.reshape(fsdp, -1) for part in parts], axis=1)
    if joined:
        small = lax.dynamic_index_in_dim(small, rank, 0, keepdims=False)
    else:
        small = reduce_small(small, sizes)
    shares = []
    at = 0
    for width in widths:
        shares.append(small[at : at + width])
        at += width
    n1g, n1b, qkvb_total, qg, kg, outb_total, n2g, n2b, upb_total, downb_total = shares
    return (
        output,
        input_grad,
        n1g,
        n1b,
        qkv_total,
        qkvb_total,
        qg,
        kg,
        out_total,
        outb_total,
        n2g,
        n2b,
        up_total,
        upb_total,
        down_total,
        downb_total,
    )


def solution(mesh):
    rows, shard = P(("dp", "fsdp"), None), P("fsdp")
    matrix = P("fsdp", None)
    placed = (
        (rows, P(("dp", "fsdp")), shard, shard, matrix, shard, shard, shard)
        + (matrix, shard, shard, shard, matrix, shard, matrix, shard, rows)
    )
    results = (
        (rows, rows, shard, shard, matrix, shard, shard, shard)
        + (matrix, shard, shard, shard, matrix, shard, matrix, shard)
    )
    return jax.shard_map(
        functools.partial(local, dict(mesh.shape)),
        mesh=mesh,
        in_specs=placed,
        out_specs=results,
        check_vma=False,
    )
```

```python
import functools
import math

import jax
import jax.numpy as jnp
from jax import lax
from jax.experimental import pallas as pl
from jax.experimental.pallas import tpu as pltpu
from jax.sharding import PartitionSpec as P

D = 768
HEADS = 12
HD = 64
PAIR = 128
PAIRS = HEADS // 2
EPS = 1e-06
BF = jnp.bfloat16
F32 = jnp.float32
LOG2E = 1.4426950408889634
ROWS = 256
QMARK = 16.0
KMARK = 12.0

NN = (((1,), (0,)), ((), ()))
NT = (((1,), (1,)), ((), ()))
TN = (((0,), (0,)), ((), ()))


def dot(left, right, dims):
    return lax.dot_general(left, right, dims, preferred_element_type=F32)


def params(*semantics):
    return pltpu.CompilerParams(
        dimension_semantics=semantics or ("arbitrary",), vmem_limit_bytes=60 * 1024 * 1024
    )


def cost(flops, nbytes, trans=0):
    return pl.CostEstimate(flops=int(flops), bytes_accessed=int(nbytes), transcendentals=int(trans))


def whole(shape):
    return pl.BlockSpec(shape, lambda *_: (0,) * len(shape))


def single(shape):
    return pl.BlockSpec(shape, lambda *_: (0,) * len(shape), pipeline_mode=pl.Buffered(1))


ANY = pl.BlockSpec(memory_space=pl.ANY)


def flip(rank, distance):
    bit = 1
    while bit <= distance:
        if distance & bit:
            rank = rank + bit * (1 - 2 * ((rank // bit) % 2))
        bit *= 2
    return rank


def fetch(pieces, full, sems):
    if len(pieces) == 1:
        copies = [pltpu.make_async_copy(pieces[0], full, sems.at[0])]
        copies[0].start()
        return copies
    rank = lax.axis_index("fsdp")
    rows = full.shape[0] // len(pieces)
    copies = []
    for distance, piece in enumerate(pieces):
        start = pl.multiple_of(flip(rank, distance) * rows, rows)
        copies.append(
            pltpu.make_async_copy(piece, full.at[pl.ds(start, rows)], sems.at[distance])
        )
    for item in copies:
        item.start()
    return copies


def stats(values):
    center = values - jnp.mean(values, axis=-1, keepdims=True)
    rstd = lax.rsqrt(jnp.mean(center * center, axis=-1, keepdims=True) + EPS)
    return center, rstd


def low_half(rows):
    return lax.broadcasted_iota(jnp.int32, (rows, PAIR), 1) < HD


def pair_mean(values, low):
    first = jnp.sum(jnp.where(low, values, 0.0), axis=-1, keepdims=True)
    second = jnp.sum(jnp.where(low, 0.0, values), axis=-1, keepdims=True)
    return jnp.where(low, first, second) * (1.0 / HD)


def front_body(count, *refs):
    x_ref, gain_ref, shift_ref = refs[:3]
    pieces = refs[3 : 3 + count]
    bias_ref, qgain_ref, kgain_ref, h_ref, qkv_ref, rstd_ref, full, sems = refs[3 + count :]

    @pl.when(pl.program_id(0) == 0)
    def _():
        for item in fetch(pieces, full, sems):
            item.wait()

    center, rstd = stats(x_ref[...].astype(F32))
    h = (center * rstd * gain_ref[...] + shift_ref[...]).astype(BF)
    h_ref[...] = h
    low = low_half(h.shape[0])
    for part in range(3):
        for block in range(D // 256):
            at = part * D + block * 256
            y = dot(h, full[:, at : at + 256], NN) + bias_ref[:, at : at + 256]
            if part == 2:
                qkv_ref[2, :, block * 256 : block * 256 + 256] = y.astype(BF)
                continue
            gain = (qgain_ref, kgain_ref)[part][...]
            for half in range(2):
                tile = y[:, half * PAIR : half * PAIR + PAIR]
                cols = slice(block * 256 + half * PAIR, block * 256 + half * PAIR + PAIR)
                c = tile - pair_mean(tile, low)
                r = lax.rsqrt(pair_mean(c * c, low) + EPS)
                normed = (c * r * gain).astype(BF)
                qkv_ref[part, :, cols] = normed * BF(0.125) if part == 0 else normed
                rstd_ref[part, :, cols] = r


def front(x, gain, shift, pieces, bias, qgain, kgain):
    tokens = x.shape[0]
    row = pl.BlockSpec((ROWS, D), lambda i: (i, 0))
    return pl.pallas_call(
        functools.partial(front_body, len(pieces)),
        grid=(tokens // ROWS,),
        in_specs=[row, whole((1, D)), whole((1, D))]
        + [ANY] * len(pieces)
        + [whole((1, 3 * D)), whole((1, PAIR)), whole((1, PAIR))],
        out_specs=[
            row,
            pl.BlockSpec((3, ROWS, D), lambda i: (0, i, 0)),
            pl.BlockSpec((2, ROWS, D), lambda i: (0, i, 0)),
        ],
        out_shape=[
            jax.ShapeDtypeStruct((tokens, D), BF),
            jax.ShapeDtypeStruct((3, tokens, D), BF),
            jax.ShapeDtypeStruct((2, tokens, D), F32),
        ],
        scratch_shapes=[pltpu.VMEM((D, 3 * D), BF), pltpu.SemaphoreType.DMA((len(pieces),))],
        compiler_params=params(),
        cost_estimate=cost(2 * tokens * D * 3 * D, 18 * tokens * D, tokens),
        name="front",
    )(x, gain, shift, *pieces, bias, qgain, kgain)


def attend_body(q_ref, k_ref, v_ref, segq_ref, segk_ref, o_ref, lse_ref):
    tokens = o_ref.shape[0]
    low = low_half(tokens)
    keys = jnp.concatenate([k_ref[0], segk_ref[...]], axis=1)
    values = v_ref[0]
    one = jnp.ones_like(values)
    values_a = jnp.where(low, values, one)
    values_b = jnp.where(low, one, values)
    low_rows = low_half(ROWS)
    for block in range(tokens // ROWS):
        rows = slice(block * ROWS, block * ROWS + ROWS)
        q = q_ref[0, rows, :]
        seg = segq_ref[rows, :]
        zero = jnp.zeros_like(q)
        sa = dot(jnp.concatenate([jnp.where(low_rows, q, zero), seg], axis=1), keys, NT)
        acc_a = dot(jnp.exp2(sa * LOG2E).astype(BF), values_a, NN)
        sb = dot(jnp.concatenate([jnp.where(low_rows, zero, q), seg], axis=1), keys, NT)
        acc_b = dot(jnp.exp2(sb * LOG2E).astype(BF), values_b, NN)
        top = jnp.where(low_rows, acc_a, acc_b)
        total = pltpu.roll(jnp.where(low_rows, acc_b, acc_a), HD, 1)
        total = jnp.where(total > 0, total, 1.0)
        o_ref[rows, :] = (top / total).astype(BF)
        lse_ref[rows, :] = jnp.log(total)


def attend(qkv, segq, segk):
    tokens = qkv.shape[1]

    def part(which):
        return pl.BlockSpec((1, tokens, PAIR), lambda i: (which, 0, i))

    col = pl.BlockSpec((tokens, PAIR), lambda i: (0, i))
    return pl.pallas_call(
        attend_body,
        grid=(PAIRS,),
        in_specs=[part(0), part(1), part(2), whole((tokens, PAIR)), whole((tokens, PAIR))],
        out_specs=[col, col],
        out_shape=[
            jax.ShapeDtypeStruct((tokens, D), BF),
            jax.ShapeDtypeStruct((tokens, D), F32),
        ],
        compiler_params=params(),
        cost_estimate=cost(
            HEADS * tokens * tokens * 256 * 6, 10 * tokens * D, HEADS * tokens * tokens
        ),
        name="attend",
    )(qkv, qkv, qkv, segq, segk)


def middle_body(count, *refs):
    o_ref, x_ref = refs[:2]
    pieces = refs[2 : 2 + count]
    bias_ref, gain_ref, shift_ref, x1_ref, h_ref, full, sems = refs[2 + count :]

    @pl.when(pl.program_id(0) == 0)
    def _():
        for item in fetch(pieces, full, sems):
            item.wait()

    x1 = x_ref[...].astype(F32) + dot(o_ref[...], full[...], NN) + bias_ref[...]
    x1_ref[...] = x1
    center, rstd = stats(x1)
    h_ref[...] = (center * rstd * gain_ref[...] + shift_ref[...]).astype(BF)


def middle(o, x, pieces, bias, gain, shift):
    tokens = x.shape[0]
    row = pl.BlockSpec((ROWS, D), lambda i: (i, 0))
    return pl.pallas_call(
        functools.partial(middle_body, len(pieces)),
        grid=(tokens // ROWS,),
        in_specs=[row, row] + [ANY] * len(pieces) + [whole((1, D))] * 3,
        out_specs=[row, row],
        out_shape=[
            jax.ShapeDtypeStruct((tokens, D), F32),
            jax.ShapeDtypeStruct((tokens, D), BF),
        ],
        scratch_shapes=[pltpu.VMEM((D, D), BF), pltpu.SemaphoreType.DMA((len(pieces),))],
        compiler_params=params(),
        cost_estimate=cost(2 * tokens * D * D, 10 * tokens * D, tokens),
        name="middle",
    )(o, x, *pieces, bias, gain, shift)


def mlp_body(count, *refs):
    h_ref, x1_ref, valid_ref, gout_ref = refs[:4]
    ups = refs[4 : 4 + count]
    downs = refs[4 + count : 4 + 2 * count]
    (
        ubias_ref,
        dbias_ref,
        gain_ref,
        out_ref,
        gx1_ref,
        ga_ref,
        dup_ref,
        ddown_ref,
        dubias_ref,
        dvec_ref,
        up,
        down,
        acc,
        gh,
        gm,
        ht,
        act,
        gu,
        sems,
    ) = refs[4 + 2 * count :]
    tokens = h_ref.shape[0]
    fblock = act.shape[1]
    blocks = tokens // ROWS
    step = pl.program_id(0)

    def block_copies(block):
        at = pl.ds(block * fblock, fblock)
        return (
            pltpu.make_async_copy(ups[0].at[:, at], up.at[:, at], sems.at[0, block]),
            pltpu.make_async_copy(downs[0].at[at], down.at[at], sems.at[1, block]),
        )

    total_blocks = up.shape[1] // fblock
    if count == 1:
        for block in range(total_blocks):

            @pl.when(step == 0)
            def _(block=block):
                for item in block_copies(block):
                    item.start()

    @pl.when(step == 0)
    def _():
        copies = []
        if count > 1:
            copies = fetch(ups, up, sems.at[0]) + fetch(downs, down, sems.at[1])
        ht[...] = h_ref[...].T
        gm[...] = jnp.where(valid_ref[...] >= 0, gout_ref[...].astype(F32), 0.0).astype(BF)
        acc[...] = jnp.zeros_like(acc)
        gh[...] = jnp.zeros_like(gh)
        for item in copies:
            item.wait()

    if count == 1:
        for block in range(total_blocks):

            @pl.when(step == block)
            def _(block=block):
                for item in block_copies(block):
                    item.wait()

    start = pl.multiple_of(step * fblock, fblock)
    cols = pl.ds(start, fblock)
    ubias = ubias_ref[...]

    def rows_step(block, total):
        rows = pl.ds(pl.multiple_of(block * ROWS, ROWS), ROWS)
        u = dot(h_ref[rows, :], up[:, cols], NN) + ubias
        phi = 0.5 * (1.0 + lax.erf(u * math.sqrt(0.5)))
        a = (u * phi).astype(BF)
        act[rows, :] = a
        acc[rows, :] += dot(a, down[cols, :], NN)
        slope = phi + u * (jnp.exp2(u * u * (-0.5 * LOG2E)) * (1.0 / math.sqrt(2.0 * math.pi)))
        g = (slope * dot(gm[rows, :], down[cols, :], NT)).astype(BF)
        gu[rows, :] = g
        gh[rows, :] += dot(g, up[:, cols], NT)
        return total + jnp.sum(g.astype(F32), axis=0, keepdims=True)

    dubias_ref[...] = lax.fori_loop(0, blocks, rows_step, jnp.zeros((1, fblock), F32))
    for at in range(0, D, 256):
        block = slice(at, at + 256)
        ddown = dot(act[...], gm[:, block], TN).astype(BF)
        ddown_ref[..., block] = ddown.reshape(ddown_ref.shape[:-1] + (256,))
        dup = dot(ht[...], gu[:, block], NN).astype(BF)
        dup_ref[..., block] = dup.reshape(dup_ref.shape[:-1] + (256,))

    @pl.when(step == pl.num_programs(0) - 1)
    def _():
        gain = gain_ref[...]
        dbias = dbias_ref[...]

        def finish(block, totals):
            dgain, dshift, dob, ddb = totals
            rows = pl.ds(pl.multiple_of(block * ROWS, ROWS), ROWS)
            x1 = x1_ref[rows, :]
            valid = valid_ref[rows, :] >= 0
            out_ref[rows, :] = jnp.where(valid, x1 + acc[rows, :] + dbias, 0.0).astype(BF)
            center, rstd = stats(x1)
            hat = center * rstd
            g = gh[rows, :]
            t = g * gain
            gy = gm[rows, :].astype(F32)
            gx1 = gy + rstd * (
                t
                - jnp.mean(t, axis=-1, keepdims=True)
                - hat * jnp.mean(t * hat, axis=-1, keepdims=True)
            )
            gx1_ref[rows, :] = gx1
            low = gx1.astype(BF)
            ga_ref[rows, :] = low
            return (
                dgain + jnp.sum(g * hat, axis=0, keepdims=True),
                dshift + jnp.sum(g, axis=0, keepdims=True),
                dob + jnp.sum(low.astype(F32), axis=0, keepdims=True),
                ddb + jnp.sum(gy, axis=0, keepdims=True),
            )

        zero = jnp.zeros((1, D), F32)
        totals = lax.fori_loop(0, blocks, finish, (zero,) * 4)
        for place, total in enumerate(totals):
            dvec_ref[place : place + 1, :] = total


def mlp(h, x1, segments, gout, ups, downs, ubias, dbias, gain, shards):
    tokens = h.shape[0]
    count = len(ups)
    hidden = ubias.shape[1]
    fblock = hidden // shards
    grads = jax.ShapeDtypeStruct((hidden // fblock, shards, D // shards, D), BF)
    act = single((tokens, D))
    return pl.pallas_call(
        functools.partial(mlp_body, count),
        grid=(hidden // fblock,),
        in_specs=[act, act, single((tokens, 1)), act]
        + [ANY] * (2 * count)
        + [pl.BlockSpec((1, fblock), lambda i: (0, i)), whole((1, D)), whole((1, D))],
        out_specs=[
            act,
            act,
            act,
            pl.BlockSpec((1, shards, D // shards, D), lambda i: (i, 0, 0, 0)),
            pl.BlockSpec((hidden // fblock, 1, D // shards, D), lambda i: (0, i, 0, 0)),
            pl.BlockSpec((1, fblock), lambda i: (0, i)),
            whole((4, D)),
        ],
        out_shape=[
            jax.ShapeDtypeStruct((tokens, D), BF),
            jax.ShapeDtypeStruct((tokens, D), F32),
            jax.ShapeDtypeStruct((tokens, D), BF),
            grads,
            grads,
            jax.ShapeDtypeStruct((1, hidden), F32),
            jax.ShapeDtypeStruct((4, D), F32),
        ],
        scratch_shapes=[
            pltpu.VMEM((D, hidden), BF),
            pltpu.VMEM((hidden, D), BF),
            pltpu.VMEM((tokens, D), F32),
            pltpu.VMEM((tokens, D), F32),
            pltpu.VMEM((tokens, D), BF),
            pltpu.VMEM((D, tokens), BF),
            pltpu.VMEM((tokens, fblock), BF),
            pltpu.VMEM((tokens, fblock), BF),
            pltpu.SemaphoreType.DMA((2, shards)),
        ],
        compiler_params=params(),
        cost_estimate=cost(12 * tokens * D * hidden, 30 * tokens * D, 2 * tokens * hidden),
        name="mlp",
    )(h, x1, segments, gout, *ups, *downs, ubias, dbias, gain)


def outback_body(count, *refs):
    o_ref, ga_ref = refs[:2]
    pieces = refs[2 : 2 + count]
    go_ref, dout_ref, full, sems = refs[2 + count :]
    step = pl.program_id(0)

    @pl.when(step == 0)
    def _():
        for item in fetch(pieces, full, sems):
            item.wait()

    start = pl.multiple_of(step * 256, 256)
    go_ref[...] = dot(ga_ref[...], full[pl.ds(start, 256), :], NT).astype(BF)
    dout_ref[...] = dot(o_ref[...], ga_ref[...], TN).astype(BF)


def outback(o, ga, pieces):
    tokens = o.shape[0]
    col = pl.BlockSpec((tokens, 256), lambda i: (0, i))
    return pl.pallas_call(
        functools.partial(outback_body, len(pieces)),
        grid=(D // 256,),
        in_specs=[col, whole((tokens, D))] + [ANY] * len(pieces),
        out_specs=[col, pl.BlockSpec((256, D), lambda i: (i, 0))],
        out_shape=[jax.ShapeDtypeStruct((tokens, D), BF), jax.ShapeDtypeStruct((D, D), BF)],
        scratch_shapes=[pltpu.VMEM((D, D), BF), pltpu.SemaphoreType.DMA((len(pieces),))],
        compiler_params=params(),
        cost_estimate=cost(4 * tokens * D * D, 6 * tokens * D),
        name="outback",
    )(o, ga, *pieces)


def split3(values):
    first = values.astype(BF)
    rest = values - first.astype(F32)
    second = rest.astype(BF)
    third = (rest - second.astype(F32)).astype(BF)
    return first, second, third


def attback_body(
    q_ref,
    k_ref,
    v_ref,
    segq_ref,
    segk_ref,
    o_ref,
    lse_ref,
    go_ref,
    rq_ref,
    rk_ref,
    qgain_ref,
    kgain_ref,
    g_ref,
    dgain_ref,
    gqt,
    gk,
    gv,
):
    tokens = o_ref.shape[0]
    low = low_half(tokens)
    lane = lax.broadcasted_iota(jnp.int32, (tokens, PAIR), 1)
    q, k, v, go = q_ref[0], k_ref[0], v_ref[0], go_ref[...]
    zero = jnp.zeros_like(q)
    product = o_ref[...].astype(F32) * go.astype(F32)
    minus = jnp.where(lane < 3, BF(-1.0), zero)
    for head in range(2):
        mine = low if head == 0 else jnp.logical_not(low)
        at = head * HD
        hi, mid, lo = split3(lse_ref[:, at : at + 1])
        segq = segq_ref[...]
        for place, piece in ((65, hi), (66, mid), (67, lo)):
            segq = jnp.where(lane == place, piece, segq)
        q_mine = jnp.where(mine, q, zero)
        go_mine = jnp.where(mine, go, zero)
        k_mine = jnp.where(mine, k, zero)
        q_wide = jnp.concatenate([q_mine, segq], axis=1)
        inner = jnp.sum(jnp.where(mine, product, 0.0), axis=-1, keepdims=True)
        extra = zero
        for place, piece in enumerate(split3(inner)):
            extra = jnp.where(lane == place, piece, extra)
        go_wide = jnp.concatenate([go_mine, extra], axis=1)
        for block in range(tokens // ROWS):
            rows = slice(block * ROWS, block * ROWS + ROWS)
            k_wide = jnp.concatenate([k[rows], segk_ref[rows, :]], axis=1)
            v_wide = jnp.concatenate([v[rows], minus[rows]], axis=1)
            p = jnp.exp2(dot(k_wide, q_wide, NT) * LOG2E)
            gs = (p * dot(v_wide, go_wide, NT)).astype(BF)
            value_part = dot(p.astype(BF), go_mine, NN)
            key_part = dot(gs, q_mine, NN)
            query_part = dot(k_mine[rows], gs, TN)
            if head == 0:
                gv[rows, :] = value_part
                gk[rows, :] = key_part
            else:
                gv[rows, :] += value_part
                gk[rows, :] += key_part
            if head == 0 and block == 0:
                gqt[...] = query_part
            else:
                gqt[...] += query_part
    g_ref[2] = gv[...].astype(BF)
    gq = gqt[...].T * 0.125
    pieces = (
        (0, gq, q.astype(F32) * 8.0, qgain_ref[...], rq_ref[0]),
        (1, gk[...], k.astype(F32), kgain_ref[...], rk_ref[0]),
    )
    for part, grad, normed, gain, rstd in pieces:
        hat = normed / gain
        t = grad * gain
        dgain_ref[part] = jnp.broadcast_to(jnp.sum(grad * hat, axis=0, keepdims=True), (8, PAIR))
        g_ref[part] = (rstd * (t - pair_mean(t, low) - hat * pair_mean(t * hat, low))).astype(BF)


def attback(qkv, segq, segk, o, lse, go, rstd, qgain, kgain):
    tokens = o.shape[0]

    def part(which):
        return pl.BlockSpec((1, tokens, PAIR), lambda i: (which, 0, i))

    col = pl.BlockSpec((tokens, PAIR), lambda i: (0, i))
    seg = whole((tokens, PAIR))
    return pl.pallas_call(
        attback_body,
        grid=(PAIRS,),
        in_specs=[part(0), part(1), part(2), seg, seg, col, col, col, part(0), part(1)]
        + [whole((1, PAIR))] * 2,
        out_specs=[
            pl.BlockSpec((3, tokens, PAIR), lambda i: (0, 0, i)),
            pl.BlockSpec((2, 8, PAIR), lambda i: (0, 0, i)),
        ],
        out_shape=[
            jax.ShapeDtypeStruct((3, tokens, D), BF),
            jax.ShapeDtypeStruct((2, 8, D), F32),
        ],
        scratch_shapes=[
            pltpu.VMEM((PAIR, tokens), F32),
            pltpu.VMEM((tokens, PAIR), F32),
            pltpu.VMEM((tokens, PAIR), F32),
        ],
        compiler_params=params(),
        cost_estimate=cost(
            HEADS * tokens * tokens * 256 * 10, 30 * tokens * D, HEADS * tokens * tokens
        ),
        name="attback",
    )(qkv, qkv, qkv, segq, segk, o, lse, go, rstd, rstd, qgain, kgain)


def qkvgrad_body(h_ref, g_ref, dw_ref, db_ref, ht):
    @pl.when(pl.program_id(0) == 0)
    def _():
        ht[...] = h_ref[...].T

    g = g_ref[0]
    dw_ref[...] = dot(ht[...], g, NN).astype(BF)
    db_ref[...] = jnp.sum(g.astype(F32), axis=0, keepdims=True)


def qkvgrad(h, g):
    tokens = h.shape[0]
    return pl.pallas_call(
        qkvgrad_body,
        grid=(3, 3),
        in_specs=[
            whole((tokens, D)),
            pl.BlockSpec((1, tokens, 256), lambda i, j: (i, 0, j)),
        ],
        out_specs=[
            pl.BlockSpec((D, 256), lambda i, j: (0, 3 * i + j)),
            pl.BlockSpec((1, 256), lambda i, j: (0, 3 * i + j)),
        ],
        out_shape=[
            jax.ShapeDtypeStruct((D, 3 * D), BF),
            jax.ShapeDtypeStruct((1, 3 * D), F32),
        ],
        scratch_shapes=[pltpu.VMEM((D, tokens), BF)],
        compiler_params=params("arbitrary", "arbitrary"),
        cost_estimate=cost(6 * tokens * D * D, 14 * tokens * D),
        name="qkvgrad",
    )(h, g)


def back_body(count, *refs):
    g_ref, x_ref, gx1_ref = refs[:3]
    pieces = refs[3 : 3 + count]
    gain_ref, gx_ref, dvec_ref, full, sems = refs[3 + count :]
    step = pl.program_id(0)

    @pl.when(step == 0)
    def _():
        for item in fetch(pieces, full, sems):
            item.wait()
        dvec_ref[...] = jnp.zeros_like(dvec_ref)

    g = dot(g_ref[0], full[:, :D], NT)
    g += dot(g_ref[1], full[:, D : 2 * D], NT)
    g += dot(g_ref[2], full[:, 2 * D :], NT)
    center, rstd = stats(x_ref[...].astype(F32))
    hat = center * rstd
    t = g * gain_ref[...]
    gx = gx1_ref[...] + rstd * (
        t - jnp.mean(t, axis=-1, keepdims=True) - hat * jnp.mean(t * hat, axis=-1, keepdims=True)
    )
    gx_ref[...] = gx.astype(BF)
    dvec_ref[0:1, :] += jnp.sum(g * hat, axis=0, keepdims=True)
    dvec_ref[1:2, :] += jnp.sum(g, axis=0, keepdims=True)


def back(g, x, gx1, pieces, gain):
    tokens = x.shape[0]
    row = pl.BlockSpec((ROWS, D), lambda i: (i, 0))
    return pl.pallas_call(
        functools.partial(back_body, len(pieces)),
        grid=(tokens // ROWS,),
        in_specs=[pl.BlockSpec((3, ROWS, D), lambda i: (0, i, 0)), row, row]
        + [ANY] * len(pieces)
        + [whole((1, D))],
        out_specs=[row, whole((2, D))],
        out_shape=[jax.ShapeDtypeStruct((tokens, D), BF), jax.ShapeDtypeStruct((2, D), F32)],
        scratch_shapes=[pltpu.VMEM((D, 3 * D), BF), pltpu.SemaphoreType.DMA((len(pieces),))],
        compiler_params=params(),
        cost_estimate=cost(6 * tokens * D * D, 16 * tokens * D, tokens),
        name="back",
    )(g, x, gx1, *pieces, gain)


CHUNKS = 12
RANK_ROWS = 192
STAGES_AT = (0, 1, 4, 6, 8, 10, 12)
LAST_STAGE = len(STAGES_AT) - 1
ATT_TICK, BACK_TICK, SMALL_TICK = 3, 18, 22
TICKS = BACK_TICK + STAGES_AT[-1] + 2


def finish_body(count, *refs):
    (
        o_ref,
        ga_ref,
        q_ref,
        k_ref,
        v_ref,
        segq_ref,
        segk_ref,
        opair_ref,
        lse_ref,
        rq_ref,
        rk_ref,
        qgain_ref,
        kgain_ref,
        h_ref,
        x_ref,
        gx1_ref,
        gain_ref,
        dubias_ref,
        dvec_ref,
        up_ref,
        down_ref,
    ) = refs[:21]
    out_pieces = refs[21 : 21 + count]
    qkv_pieces = refs[21 + count : 21 + 2 * count]
    (
        gx_ref,
        total_ref,
        small_ref,
        out_full,
        qkv_full,
        go,
        g3,
        ht,
        gqt,
        gk,
        gv,
        own,
        held,
        r0,
        r1,
        r2,
        r3,
        done,
        small,
        rsmall,
        weight_sems,
        local_sems,
        send_sems,
        recv_sems,
        done_sems,
        ssend_sems,
        srecv_sems,
    ) = refs[21 + 2 * count :]
    tick = pl.program_id(0)
    tokens = o_ref.shape[0]

    rank, group = lax.axis_index("fsdp"), lax.axis_index("dp")
    c, x = rank % 2, rank // 2
    y, z1, z2 = group % 2, (group // 2) % 2, group // 4
    partners = (
        {"fsdp": flip(rank, 1)},
        {"fsdp": flip(rank, 2)},
        {"dp": flip(group, 1)},
        {"dp": flip(group, 2)},
        {"dp": flip(group, 4)},
        {"dp": flip(group, 6)},
    )
    row_y = pl.multiple_of(y * 96, 48)
    other_y = pl.multiple_of((1 - y) * 96, 48)

    def corner(distance):
        row = flip(z1, 1) if distance % 2 else z1
        col = flip(z2, 1) if distance // 2 else z2
        return (
            pl.ds(pl.multiple_of(y * 96 + row * 48, 48), 48),
            pl.ds(pl.multiple_of(col * 384, 384), 384),
        )

    def remote(stage, chunk, src, dst, partner):
        return pltpu.make_async_remote_copy(
            src_ref=src,
            dst_ref=dst,
            send_sem=send_sems.at[stage, chunk],
            recv_sem=recv_sems.at[stage, chunk],
            device_id=partners[partner],
            device_id_type=pl.DeviceIdType.MESH,
        )

    def first_send(source, place, chunk):
        return remote(0, chunk, source.at[place, :, 1 - c], r0.at[chunk], 0)

    def sends(stage, chunk):
        if stage == 1:
            return [remote(1, chunk, held.at[chunk, 1 - x], r1.at[chunk], 1)]
        if stage == 2:
            return [remote(2, chunk, held.at[chunk, x, pl.ds(other_y, 96)], r2.at[chunk], 2)]
        if stage == 3:
            return [
                remote(
                    2 + d, chunk, held.at[(chunk, x) + corner(d)], r3.at[chunk, d - 1], 2 + d
                )
                for d in (1, 2, 3)
            ]
        if stage == 4:
            place = done.at[(chunk,) + corner(0)]
            return [remote(5 + d, chunk, place, place, 2 + d) for d in (1, 2, 3)]
        place = done.at[chunk, pl.ds(row_y, 96)]
        return [remote(9, chunk, place, place, 2)]

    def finished(stage, chunk):
        for item in sends(stage, chunk):
            item.wait()

    def stored(chunk):
        return pltpu.make_async_copy(done.at[chunk], total_ref.at[chunk], done_sems.at[chunk])

    def add(left, right):
        return (left.astype(F32) + right.astype(F32)).astype(BF)

    sources = (
        (up_ref, 0, 4, 0),
        (down_ref, 4, 6, 4),
        (own, 6, 7, 6),
        (down_ref, 7, 9, 5),
        (own, 9, CHUNKS, 8),
    )

    def start_chunk(chunk):
        for source, begin, end, base in sources:

            @pl.when((chunk >= begin) & (chunk < end))
            def _(source=source, base=base):
                place = chunk - base
                first_send(source, place, chunk).start()
                pltpu.make_async_copy(
                    source.at[place, :, c], held.at[chunk], local_sems.at[chunk]
                ).start()

    def pass_on(stage, chunk):
        if stage == 1:
            for source, begin, end, base in sources:

                @pl.when((chunk >= begin) & (chunk < end))
                def _(source=source, base=base):
                    place = chunk - base
                    first_send(source, place, chunk).wait()
                    pltpu.make_async_copy(
                        source.at[place, :, c], held.at[chunk], local_sems.at[chunk]
                    ).wait()

            def add_rows(i, _):
                rows = pl.ds(pl.multiple_of((i % 4) * 48, 48), 48)
                held[chunk, i // 4, rows, :] = add(
                    held[chunk, i // 4, rows, :], r0[chunk, i // 4, rows, :]
                )
                return 0

            lax.fori_loop(0, 8, add_rows, 0)
        elif stage == 2:
            finished(1, chunk)

            def add_rows(i, _):
                rows = pl.ds(pl.multiple_of(i * 48, 48), 48)
                held[chunk, x, rows, :] = add(held[chunk, x, rows, :], r1[chunk, rows, :])
                return 0

            lax.fori_loop(0, 4, add_rows, 0)
        elif stage == 3:
            finished(2, chunk)

            def add_rows(i, _):
                rows = pl.ds(pl.multiple_of(row_y + i * 48, 48), 48)
                came = pl.ds(pl.multiple_of(i * 48, 48), 48)
                held[chunk, x, rows, :] = add(held[chunk, x, rows, :], r2[chunk, came, :])
                return 0

            lax.fori_loop(0, 2, add_rows, 0)
        elif stage == 4:
            finished(3, chunk)
            rows, cols = corner(0)
            total = held[chunk, x, rows, cols].astype(F32)
            for d in range(3):
                total += r3[chunk, d].astype(F32)
            done[chunk, rows, cols] = total.astype(BF)
        else:
            finished(stage - 1, chunk)
        if stage < LAST_STAGE:
            for item in sends(stage, chunk):
                item.start()
        else:
            stored(chunk).start()

    def small_send(step):
        return pltpu.make_async_remote_copy(
            src_ref=small.at[step],
            dst_ref=rsmall.at[step],
            send_sem=ssend_sems.at[step],
            recv_sem=srecv_sems.at[step],
            device_id=partners[step],
            device_id_type=pl.DeviceIdType.MESH,
        )

    def weights(which):
        full, pieces = ((out_full, out_pieces), (qkv_full, qkv_pieces))[which]
        if count == 1:
            return [pltpu.make_async_copy(pieces[0], full, weight_sems.at[which, 0])]
        rows = full.shape[0] // count
        return [
            pltpu.make_async_copy(
                piece,
                full.at[pl.ds(pl.multiple_of(flip(rank, distance) * rows, rows), rows)],
                weight_sems.at[which, distance],
            )
            for distance, piece in enumerate(pieces)
        ]

    @pl.when(tick == 0)
    def _():
        barrier = pltpu.get_barrier_semaphore()
        for partner in partners:
            pl.semaphore_signal(
                barrier, inc=1, device_id=partner, device_id_type=pl.DeviceIdType.MESH
            )
        for item in weights(0) + weights(1):
            item.start()
        small[0] = jnp.zeros_like(small[0])
        pl.semaphore_wait(barrier, len(partners))

    for stage in reversed(range(LAST_STAGE + 1)):
        moment = tick - STAGES_AT[stage]

        chunk = (moment * 11 + 17) // 18

        @pl.when((moment >= 0) & (chunk < CHUNKS) & (chunk * 18 // 11 == moment))
        def _(stage=stage, chunk=chunk):
            if stage == 0:
                start_chunk(chunk)
            else:
                pass_on(stage, chunk)

    @pl.when(tick < ATT_TICK)
    def _():
        @pl.when(tick == 0)
        def _():
            for item in weights(0):
                item.wait()

        start = pl.multiple_of(tick * 256, 256)
        block = pl.ds(start, 256)
        go[:, block] = dot(ga_ref[...], out_full[block, :], NT).astype(BF)
        dout = dot(o_ref[:, block], ga_ref[...], TN).astype(BF)
        for part in range(4):
            piece = dout[part * 64 : part * 64 + 64]
            row = tick * 256 + part * 64
            shard = row // RANK_ROWS
            own[
                2,
                shard // 2,
                shard % 2,
                pl.ds(pl.multiple_of(row % RANK_ROWS, 64), 64),
                :,
            ] = piece

    turn = (tick - ATT_TICK) // 5
    place_in_turn = (tick - ATT_TICK) % 5

    @pl.when((tick >= ATT_TICK) & (tick < BACK_TICK) & (place_in_turn < 4))
    def _():
        pair = 2 * turn + place_in_turn // 2
        head = place_in_turn % 2
        pair_cols = pl.ds(pl.multiple_of(pair * PAIR, PAIR), PAIR)
        lane = lax.broadcasted_iota(jnp.int32, (tokens, PAIR), 1)
        mine = lane // HD == head
        q, k, v, go_pair = q_ref[0], k_ref[0], v_ref[0], go[:, pair_cols]
        zero = jnp.zeros_like(q)
        minus = jnp.where(lane < 3, BF(-1.0), zero)

        @pl.when(head == 0)
        def _():
            gqt[...] = jnp.zeros_like(gqt)
            gk[...] = jnp.zeros_like(gk)
            gv[...] = jnp.zeros_like(gv)

        product = opair_ref[...].astype(F32) * go_pair.astype(F32)
        inner = jnp.sum(jnp.where(mine, product, 0.0), axis=-1, keepdims=True)
        logs = jnp.sum(jnp.where(lane == head * HD, lse_ref[...], 0.0), axis=-1, keepdims=True)
        segq = segq_ref[...]
        for place, piece in enumerate(split3(logs)):
            segq = jnp.where(lane == 65 + place, piece, segq)
        extra = zero
        for place, piece in enumerate(split3(inner)):
            extra = jnp.where(lane == place, piece, extra)
        q_mine = jnp.where(mine, q, zero)
        go_mine = jnp.where(mine, go_pair, zero)
        k_mine = jnp.where(mine, k, zero)
        q_wide = jnp.concatenate([q_mine, segq], axis=1)
        go_wide = jnp.concatenate([go_mine, extra], axis=1)
        for block in range(tokens // ROWS):
            rows = slice(block * ROWS, block * ROWS + ROWS)
            k_wide = jnp.concatenate([k[rows], segk_ref[rows, :]], axis=1)
            v_wide = jnp.concatenate([v[rows], minus[rows]], axis=1)
            p = jnp.exp2(dot(k_wide, q_wide, NT) * LOG2E)
            gs = (p * dot(v_wide, go_wide, NT)).astype(BF)
            gv[rows, :] += dot(p.astype(BF), go_mine, NN)
            gk[rows, :] += dot(gs, q_mine, NN)
            gqt[...] += dot(k_mine[rows], gs, TN)

        @pl.when(head == 1)
        def _():
            low = low_half(tokens)
            g3[2, :, pair_cols] = gv[...].astype(BF)
            gq = gqt[...].T * 0.125
            pieces = (
                (0, gq, q.astype(F32) * 8.0, qgain_ref[...], rq_ref[0]),
                (1, gk[...], k.astype(F32), kgain_ref[...], rk_ref[0]),
            )
            for part, grad, normed, gain, rstd in pieces:
                hat = normed / gain
                t = grad * gain
                lanes = slice(part * PAIR, part * PAIR + PAIR)
                small[0, 5:6, lanes] += jnp.sum(grad * hat, axis=0, keepdims=True)
                g3[part, :, pair_cols] = (
                    rstd * (t - pair_mean(t, low) - hat * pair_mean(t * hat, low))
                ).astype(BF)

    @pl.when((tick >= ATT_TICK) & (tick < BACK_TICK) & (place_in_turn == 4))
    def _():
        @pl.when(turn == 0)
        def _():
            ht[...] = h_ref[...].T

        cols = pl.ds(pl.multiple_of(turn * 256, 256), 256)
        for part in range(3):
            g = g3[part, :, cols]
            own[turn + turn // 2, :, :, :, part * 256 : part * 256 + 256] = (
                dot(ht[...], g, NN).astype(BF).reshape(2, 2, RANK_ROWS, 256)
            )
            small[0, 2 + part : 3 + part, cols] = jnp.sum(g.astype(F32), axis=0, keepdims=True)

    @pl.when((tick >= BACK_TICK) & (tick < SMALL_TICK))
    def _():
        @pl.when(tick == BACK_TICK)
        def _():
            for item in weights(1):
                item.wait()

        rows = pl.ds(pl.multiple_of((tick - BACK_TICK) * ROWS, ROWS), ROWS)
        g = dot(g3[0, rows, :], qkv_full[:, :D], NT)
        g += dot(g3[1, rows, :], qkv_full[:, D : 2 * D], NT)
        g += dot(g3[2, rows, :], qkv_full[:, 2 * D :], NT)
        center, rstd = stats(x_ref[...].astype(F32))
        hat = center * rstd
        t = g * gain_ref[...]
        gx = gx1_ref[...] + rstd * (
            t
            - jnp.mean(t, axis=-1, keepdims=True)
            - hat * jnp.mean(t * hat, axis=-1, keepdims=True)
        )
        gx_ref[...] = gx.astype(BF)
        small[0, 0:1, :] += jnp.sum(g * hat, axis=0, keepdims=True)
        small[0, 1:2, :] += jnp.sum(g, axis=0, keepdims=True)

    @pl.when(tick == SMALL_TICK)
    def _():
        small[0, 6:10, :] = dvec_ref[...]
        for part in range(4):
            small[0, 10 + part : 11 + part, :] = dubias_ref[:, part * D : part * D + D]
        small_send(0).start()

    for step in range(5):

        @pl.when(tick == SMALL_TICK + 1 + step)
        def _(step=step):
            small_send(step).wait()
            small[step + 1] = small[step] + rsmall[step]
            if step < 4:
                small_send(step + 1).start()
            else:
                small_ref[...] = small[5]

    @pl.when(tick == TICKS - 1)
    def _():
        for chunk in range(CHUNKS):
            stored(chunk).wait()


def finish(o, ga, qkv, segq, segk, lse, rstd, qgain, kgain, h, x, gx1, gain, dubias, dvec, dup, ddown, outs, qkvs):
    tokens = o.shape[0]
    count = len(outs)
    split = (dup.shape[0], 2, 2, RANK_ROWS, D)

    def pair_of(i):
        after = jnp.clip(i - ATT_TICK, 0, BACK_TICK - ATT_TICK - 1)
        return 2 * (after // 5) + jnp.minimum(after % 5, 3) // 2

    def part(which):
        return pl.BlockSpec((1, tokens, PAIR), lambda i: (which, 0, pair_of(i)))

    col = pl.BlockSpec((tokens, PAIR), lambda i: (0, pair_of(i)))
    row = pl.BlockSpec(
        (ROWS, D), lambda i: (jnp.clip(i - BACK_TICK, 0, tokens // ROWS - 1), 0)
    )
    act = single((tokens, D))
    seg = single((tokens, PAIR))
    grid = pl.GridSpec(
        grid=(TICKS,),
        in_specs=[act, act, part(0), part(1), part(2), seg, seg, col, col, part(0), part(1)]
        + [single((1, PAIR))] * 2
        + [act, row, row, single((1, D)), single((1, 4 * D)), single((4, D)), ANY, ANY]
        + [ANY] * (2 * count),
        out_specs=[row, ANY, single((16, D))],
        scratch_shapes=[
            pltpu.VMEM((D, D), BF),
            pltpu.VMEM((D, 3 * D), BF),
            pltpu.VMEM((tokens, D), BF),
            pltpu.VMEM((3, tokens, D), BF),
            pltpu.VMEM((D, tokens), BF),
            pltpu.VMEM((PAIR, tokens), F32),
            pltpu.VMEM((tokens, PAIR), F32),
            pltpu.VMEM((tokens, PAIR), F32),
            pltpu.VMEM((4, 2, 2, RANK_ROWS, D), BF),
            pltpu.VMEM((CHUNKS, 2, RANK_ROWS, D), BF),
            pltpu.VMEM((CHUNKS, 2, RANK_ROWS, D), BF),
            pltpu.VMEM((CHUNKS, RANK_ROWS, D), BF),
            pltpu.VMEM((CHUNKS, 96, D), BF),
            pltpu.VMEM((CHUNKS, 3, 48, D // 2), BF),
            pltpu.VMEM((CHUNKS, RANK_ROWS, D), BF),
            pltpu.VMEM((6, 16, D), F32),
            pltpu.VMEM((5, 16, D), F32),
            pltpu.SemaphoreType.DMA((2, count)),
            pltpu.SemaphoreType.DMA((CHUNKS,)),
            pltpu.SemaphoreType.DMA((10, CHUNKS)),
            pltpu.SemaphoreType.DMA((10, CHUNKS)),
            pltpu.SemaphoreType.DMA((CHUNKS,)),
            pltpu.SemaphoreType.DMA((5,)),
            pltpu.SemaphoreType.DMA((5,)),
        ],
    )
    return pl.pallas_call(
        functools.partial(finish_body, count),
        grid_spec=grid,
        out_shape=[
            jax.ShapeDtypeStruct((tokens, D), BF),
            jax.ShapeDtypeStruct((CHUNKS, RANK_ROWS, D), BF),
            jax.ShapeDtypeStruct((16, D), F32),
        ],
        compiler_params=pltpu.CompilerParams(
            dimension_semantics=("arbitrary",),
            vmem_limit_bytes=63 * 1024 * 1024,
            collective_id=1,
            has_side_effects=True,
        ),
        name="finish",
    )(
        o, ga, qkv, qkv, qkv, segq, segk, o, lse, rstd, rstd, qgain, kgain, h, x, gx1, gain,
        dubias, dvec, dup.reshape(split), ddown.reshape(split), *outs, *qkvs,
    )


def unpack_body(total_ref, up_ref, down_ref, out_ref, qkv_ref):
    for chunk in range(CHUNKS):
        block = total_ref[chunk].astype(F32)
        if chunk < 4:
            up_ref[:, chunk * D : chunk * D + D] = block
        elif chunk in (4, 5, 7, 8):
            down_ref[chunk - 4 - chunk // 7] = block
        elif chunk == 10:
            out_ref[...] = block
        else:
            turn = (6, 9, 11).index(chunk)
            for part in range(3):
                at = part * D + turn * 256
                qkv_ref[:, at : at + 256] = block[:, part * 256 : part * 256 + 256]


def unpack(totals):
    step = 48

    def rows(columns):
        return pl.BlockSpec((step, columns), lambda i: (i, 0))

    return pl.pallas_call(
        unpack_body,
        grid=(RANK_ROWS // step,),
        in_specs=[pl.BlockSpec((CHUNKS, step, D), lambda i: (0, i, 0))],
        out_specs=[
            rows(4 * D),
            pl.BlockSpec((4, step, D), lambda i: (0, i, 0)),
            rows(D),
            rows(3 * D),
        ],
        out_shape=[
            jax.ShapeDtypeStruct((RANK_ROWS, 4 * D), F32),
            jax.ShapeDtypeStruct((4, RANK_ROWS, D), F32),
            jax.ShapeDtypeStruct((RANK_ROWS, D), F32),
            jax.ShapeDtypeStruct((RANK_ROWS, 3 * D), F32),
        ],
        compiler_params=params(),
        name="unpack",
    )(totals)


FRONT_TICK, PAIR_TICK, MID_TICK, BEGIN_TICKS = 1, 5, 11, 15
OWN_CORE, OVER_X, OVER_Y, X_CORE, Y_CORE = range(5)
QKV_PIECE = 32
LINE_ROWS = (0, 1, 6, 13, 14, 2, 3, 4, 9, 5)


def begin_body(
    x_ref,
    ids_ref,
    *rest,
):
    lines = rest[:10]
    (
        wq_ref,
        wo_ref,
        wu_ref,
        wd_ref,
        segq_ref,
        segk_ref,
        h_ref,
        qkv_ref,
        rstd_ref,
        o_ref,
        lse_ref,
        x1_ref,
        h2_ref,
        gain1_ref,
        gain2_ref,
        dbias_ref,
        qgain_ref,
        kgain_ref,
        ubias_ref,
        wq_out,
        wo_out,
        wu_out,
        wd_out,
        wq,
        wo,
        wu,
        wd,
        pack_ref,
        pack,
        vecs,
        qkv,
        mixed,
        send_sems,
        recv_sems,
        local_sems,
        out_sems,
    ) = rest[10:]
    tick = pl.program_id(0)
    tokens = x_ref.shape[0]
    rank, group = lax.axis_index("fsdp"), lax.axis_index("dp")
    y = group % 2
    across = flip(rank, 2)
    partners = ({"fsdp": flip(rank, 1)}, {"fsdp": across}, {"dp": flip(group, 1)})
    shards = (wq_ref, wo_ref, wu_ref, wd_ref, pack_ref)
    fulls = (wq, wo, wu, wd, pack)
    outs = (wq_out, wo_out, wu_out, wd_out)
    QKV, OUT, UP, DOWN, PACK = range(5)

    def remote(which, event, src, dst, partner):
        return pltpu.make_async_remote_copy(
            src_ref=src,
            dst_ref=dst,
            send_sem=send_sems.at[which, event],
            recv_sem=recv_sems.at[which, event],
            device_id=partners[partner],
            device_id_type=pl.DeviceIdType.MESH,
        )

    def piece_of_qkv(piece, kind):
        third = QKV_PIECE
        near = pl.ds(pl.multiple_of(y * 3 * third + piece * third, third), third)
        far = pl.ds(pl.multiple_of((1 - y) * 3 * third + piece * third, third), third)
        slot = 5 + piece
        if kind == OVER_X:
            return remote(slot, kind, wq_ref.at[near], wq.at[rank, near], 1)
        place = wq.at[across, far if kind == Y_CORE else near]
        return remote(slot, kind, place, place, 2 if kind == OVER_Y else 0)

    def event(which, kind):
        shard, full = shards[which], fulls[which]
        if which == PACK:
            if kind == X_CORE:
                return remote(which, kind, full.at[across], full.at[across], 0)
            return remote(which, kind, shard, full.at[rank], kind)
        half = full.shape[1] // 2
        near = pl.ds(pl.multiple_of(y * half, half), half)
        far = pl.ds(pl.multiple_of((1 - y) * half, half), half)
        if kind == OWN_CORE:
            return remote(which, kind, shard, full.at[rank], 0)
        if kind == OVER_X:
            return remote(which, kind, shard.at[near], full.at[rank, near], 1)
        place = full.at[across, far if kind == Y_CORE else near]
        return remote(which, kind, place, place, 2 if kind == OVER_Y else 0)

    def own(which):
        return pltpu.make_async_copy(shards[which], fulls[which].at[rank], local_sems.at[which])

    def stored(which):
        return pltpu.make_async_copy(fulls[which], outs[which], out_sems.at[which])

    def complete(which):
        event(which, OWN_CORE).wait()
        for kind in (X_CORE, Y_CORE):
            if which == QKV:
                for piece in range(3):
                    piece_of_qkv(piece, kind).wait()
            else:
                event(which, kind).wait()
        own(which).wait()
        stored(which).start()

    @pl.when(tick == 0)
    def _():
        barrier = pltpu.get_barrier_semaphore()
        for partner in partners:
            pl.semaphore_signal(
                barrier, inc=1, device_id=partner, device_id_type=pl.DeviceIdType.MESH
            )
        for which in (QKV, OUT, UP, DOWN):
            own(which).start()
        pack_ref[...] = jnp.zeros_like(pack_ref)
        for place, line in enumerate(lines):
            width = min(line.shape[0], 192)
            for piece in range(line.shape[0] // width):
                row = LINE_ROWS[place] + piece
                value = line[piece * width : piece * width + width].astype(F32)
                pack_ref[row : row + 1, :width] = value.reshape(1, width)
        pack[rank] = pack_ref[...]
        pl.semaphore_wait(barrier, len(partners))
        for kind in (OWN_CORE, OVER_X):
            event(PACK, kind).start()
        for piece in range(3):
            piece_of_qkv(piece, OVER_X).start()
        event(QKV, OWN_CORE).start()
        lane = lax.broadcasted_iota(jnp.int32, (tokens, PAIR), 1)
        match = (ids_ref[...] == lane) & (lane < HD)
        segq_ref[...] = jnp.where(
            match, QMARK, jnp.where(lane == HD, 1.0, 0.0)
        ).astype(BF)
        segk_ref[...] = jnp.where(
            match,
            KMARK,
            jnp.where(
                lane == HD,
                -QMARK * KMARK,
                jnp.where((lane > HD) & (lane <= HD + 3), -1.0, 0.0),
            ),
        ).astype(BF)
        event(PACK, OVER_X).wait()
        event(PACK, X_CORE).start()

        def forward(piece):
            piece_of_qkv(piece, OVER_X).wait()
            piece_of_qkv(piece, OVER_Y).start()
            piece_of_qkv(piece, X_CORE).start()

        forward(0)
        event(PACK, OWN_CORE).wait()
        event(PACK, X_CORE).wait()

        held = [pack[shard] for shard in range(4)]
        lane = lax.broadcasted_iota(jnp.int32, (256, D), 1)
        line = lax.broadcasted_iota(jnp.int32, (256, D), 0)
        total = jnp.zeros((16, D), F32)
        for slot in range(4):
            rows = [held[slot][0:6]]
            for part in range(3):
                shard, piece = (4 * part + slot) // 3, (4 * part + slot) % 3
                rows.append(held[shard][6 + piece : 7 + piece])
            for part in range(4):
                rows.append(held[part][9 + slot : 10 + slot])
            rows.append(jnp.zeros((3, 256), F32))
            chosen = jnp.where((lane == line + slot * 192) & (line < 192), BF(1.0), BF(0.0))
            total += dot(jnp.concatenate(rows, axis=0).astype(BF), chosen, NN)
        vecs[...] = total
        lane, line = lane[:, :PAIR], line[:, :PAIR]
        heads = jnp.zeros((16, PAIR), F32)
        for shard in range(4):
            chosen = jnp.where((lane % HD == line + shard * 16) & (line < 16), BF(1.0), BF(0.0))
            heads += dot(pack[shard].astype(BF), chosen, NN)
        gain1_ref[...] = total[0:1]
        gain2_ref[...] = total[3:4]
        dbias_ref[...] = total[5:6]
        for part in range(4):
            ubias_ref[:, part * D : part * D + D] = total[9 + part : 10 + part]
        qgain_ref[...] = heads[13:14]
        kgain_ref[...] = heads[14:15]

        forward(1)
        forward(2)
        for which in (OUT, UP):
            event(which, OVER_X).start()
        for which in (OUT, UP, DOWN):
            event(which, OWN_CORE).start()
        for piece in range(3):
            piece_of_qkv(piece, OVER_Y).wait()
            piece_of_qkv(piece, Y_CORE).start()
        complete(QKV)

    @pl.when(tick == 2)
    def _():
        for which in (OUT, UP):
            event(which, OVER_X).wait()
            event(which, OVER_Y).start()
            event(which, X_CORE).start()
        event(DOWN, OVER_X).start()

    @pl.when(tick == 7)
    def _():
        for which in (OUT, UP):
            event(which, OVER_Y).wait()
            event(which, Y_CORE).start()
        event(DOWN, OVER_X).wait()
        event(DOWN, OVER_Y).start()
        event(DOWN, X_CORE).start()

    @pl.when(tick == MID_TICK)
    def _():
        complete(OUT)

    @pl.when(tick == MID_TICK + 1)
    def _():
        complete(UP)

    @pl.when(tick == MID_TICK + 2)
    def _():
        event(DOWN, OVER_Y).wait()
        event(DOWN, Y_CORE).start()

    @pl.when((tick >= FRONT_TICK) & (tick < PAIR_TICK))
    def _():
        rows = pl.ds(pl.multiple_of((tick - FRONT_TICK) * ROWS, ROWS), ROWS)
        center, rstd = stats(x_ref[rows, :].astype(F32))
        h = (center * rstd * vecs[0:1, :] + vecs[1:2, :]).astype(BF)
        h_ref[...] = h
        low = low_half(ROWS)
        for part in range(3):
            for block in range(D // 256):
                at = part * D + block * 256
                weight = wq[:, :, at : at + 256].reshape(D, 256)
                y_block = dot(h, weight, NN) + vecs[
                    6 + part : 7 + part, block * 256 : block * 256 + 256
                ]
                if part == 2:
                    value = y_block.astype(BF)
                    qkv_ref[2, :, block * 256 : block * 256 + 256] = value
                    qkv[2, rows, block * 256 : block * 256 + 256] = value
                    continue
                gain = (qgain_ref, kgain_ref)[part][...]
                for half in range(2):
                    tile = y_block[:, half * PAIR : half * PAIR + PAIR]
                    cols = slice(block * 256 + half * PAIR, block * 256 + half * PAIR + PAIR)
                    c = tile - pair_mean(tile, low)
                    r = lax.rsqrt(pair_mean(c * c, low) + EPS)
                    normed = (c * r * gain).astype(BF)
                    if part == 0:
                        normed = normed * BF(0.125)
                    qkv_ref[part, :, cols] = normed
                    qkv[part, rows, cols] = normed
                    rstd_ref[part, :, cols] = r

    @pl.when((tick >= PAIR_TICK) & (tick < MID_TICK))
    def _():
        pair_cols = pl.ds(pl.multiple_of((tick - PAIR_TICK) * PAIR, PAIR), PAIR)
        low = low_half(tokens)
        keys = jnp.concatenate([qkv[1, :, pair_cols], segk_ref[...]], axis=1)
        values = qkv[2, :, pair_cols]
        one = jnp.ones_like(values)
        values_a = jnp.where(low, values, one)
        values_b = jnp.where(low, one, values)
        low_rows = low_half(ROWS)
        for block in range(tokens // ROWS):
            rows = slice(block * ROWS, block * ROWS + ROWS)
            q = qkv[0, rows, pair_cols]
            seg = segq_ref[rows, :]
            zero = jnp.zeros_like(q)
            sa = dot(jnp.concatenate([jnp.where(low_rows, q, zero), seg], axis=1), keys, NT)
            acc_a = dot(jnp.exp2(sa * LOG2E).astype(BF), values_a, NN)
            sb = dot(jnp.concatenate([jnp.where(low_rows, zero, q), seg], axis=1), keys, NT)
            acc_b = dot(jnp.exp2(sb * LOG2E).astype(BF), values_b, NN)
            top = jnp.where(low_rows, acc_a, acc_b)
            sums = pltpu.roll(jnp.where(low_rows, acc_b, acc_a), HD, 1)
            sums = jnp.where(sums > 0, sums, 1.0)
            value = (top / sums).astype(BF)
            o_ref[rows, :] = value
            mixed[rows, pair_cols] = value
            lse_ref[rows, :] = jnp.log(sums)

    @pl.when(tick >= MID_TICK)
    def _():
        rows = pl.ds(pl.multiple_of((tick - MID_TICK) * ROWS, ROWS), ROWS)
        x1 = (
            x_ref[rows, :].astype(F32)
            + dot(mixed[rows, :], wo[...].reshape(D, D), NN)
            + vecs[2:3, :]
        )
        x1_ref[...] = x1
        center, rstd = stats(x1)
        h2_ref[...] = (center * rstd * vecs[3:4, :] + vecs[4:5, :]).astype(BF)

    @pl.when(tick == BEGIN_TICKS - 1)
    def _():
        complete(DOWN)
        for which in (QKV, OUT, UP, DOWN):
            stored(which).wait()


def begin(x, ids, lines, matrices):
    tokens = x.shape[0]

    def rows(tick):
        return lambda i: jnp.clip(i - tick, 0, tokens // ROWS - 1)

    at_front, at_middle = rows(FRONT_TICK), rows(MID_TICK)
    col = pl.BlockSpec((tokens, PAIR), lambda i: (0, jnp.clip(i - PAIR_TICK, 0, PAIRS - 1)))
    early = pl.BlockSpec((ROWS, D), lambda i: (at_front(i), 0))
    late = pl.BlockSpec((ROWS, D), lambda i: (at_middle(i), 0))
    fulls = [(4,) + matrix.shape for matrix in matrices]
    grid = pl.GridSpec(
        grid=(BEGIN_TICKS,),
        in_specs=[single((tokens, D)), single((tokens, 1))]
        + [single(line.shape) for line in lines]
        + [ANY] * 4,
        out_specs=[
            single((tokens, PAIR)),
            single((tokens, PAIR)),
            early,
            pl.BlockSpec((3, ROWS, D), lambda i: (0, at_front(i), 0)),
            pl.BlockSpec((2, ROWS, D), lambda i: (0, at_front(i), 0)),
            col,
            col,
            late,
            late,
        ]
        + [single((1, D))] * 3
        + [single((1, PAIR))] * 2
        + [single((1, 4 * D))]
        + [ANY] * 4,
        scratch_shapes=[pltpu.VMEM(shape, BF) for shape in fulls]
        + [
            pltpu.VMEM((16, 256), F32),
            pltpu.VMEM((4, 16, 256), F32),
            pltpu.VMEM((16, D), F32),
            pltpu.VMEM((3, tokens, D), BF),
            pltpu.VMEM((tokens, D), BF),
            pltpu.SemaphoreType.DMA((8, 5)),
            pltpu.SemaphoreType.DMA((8, 5)),
            pltpu.SemaphoreType.DMA((5,)),
            pltpu.SemaphoreType.DMA((4,)),
        ],
    )
    return pl.pallas_call(
        begin_body,
        grid_spec=grid,
        out_shape=[
            jax.ShapeDtypeStruct((tokens, PAIR), BF),
            jax.ShapeDtypeStruct((tokens, PAIR), BF),
            jax.ShapeDtypeStruct((tokens, D), BF),
            jax.ShapeDtypeStruct((3, tokens, D), BF),
            jax.ShapeDtypeStruct((2, tokens, D), F32),
            jax.ShapeDtypeStruct((tokens, D), BF),
            jax.ShapeDtypeStruct((tokens, D), F32),
            jax.ShapeDtypeStruct((tokens, D), F32),
            jax.ShapeDtypeStruct((tokens, D), BF),
        ]
        + [jax.ShapeDtypeStruct((1, D), F32)] * 3
        + [jax.ShapeDtypeStruct((1, PAIR), F32)] * 2
        + [jax.ShapeDtypeStruct((1, 4 * D), F32)]
        + [jax.ShapeDtypeStruct(shape, BF) for shape in fulls],
        compiler_params=pltpu.CompilerParams(
            dimension_semantics=("arbitrary",),
            vmem_limit_bytes=60 * 1024 * 1024,
            collective_id=0,
            has_side_effects=True,
        ),
        name="begin",
    )(x, ids, *lines, *matrices)


def swap(values, axis, mask, size):
    return lax.ppermute(values, axis, [(i, i ^ mask) for i in range(size)])


def bits_of(size):
    return [1 << b for b in range(size.bit_length() - 1)]


def gather_shards(shard, size):
    held = [shard]
    for mask in reversed(bits_of(size)):
        held = held + [swap(item, "fsdp", mask, size) for item in held]
    order = [0]
    for mask in reversed(bits_of(size)):
        order = order + [place ^ mask for place in order]
    placed = [None] * size
    for place, item in zip(order, held):
        placed[place] = item
    return placed


def reduce_grad(grad, order, sizes):
    fsdp, dp = sizes["fsdp"], sizes["dp"]
    rows, columns = grad.shape
    names = [("fsdp", m) for m in reversed(bits_of(fsdp))] + [
        ("dp", m) for m in reversed(bits_of(dp))
    ]
    held = grad.reshape((2,) * len(names) + (rows // fsdp // dp, columns))
    undo = []
    for step in order:
        axis, mask = step
        place = names.index(step)
        mine = (lax.axis_index(axis) // mask) % 2
        send = lax.dynamic_index_in_dim(held, 1 - mine, place, keepdims=False)
        keep = lax.dynamic_index_in_dim(held, mine, place, keepdims=False)
        held = (
            keep.astype(F32) + swap(send, axis, mask, sizes[axis]).astype(F32)
        ).astype(BF)
        names.pop(place)
        if axis == "dp":
            place -= sum(name == "fsdp" for name, _ in names[:place])
            undo.append((axis, mask, place, mine))
    for axis, mask, place, mine in reversed(undo):
        other = swap(held, axis, mask, sizes[axis])
        first = jnp.where(mine == 0, held, other)
        second = jnp.where(mine == 0, other, held)
        held = jnp.stack([first, second], axis=place)
    return held.reshape(rows // fsdp, columns).astype(F32)


def reduce_small(grad, sizes):
    held = grad.reshape((2,) * len(bits_of(sizes["fsdp"])) + (grad.shape[1],))
    for mask in reversed(bits_of(sizes["fsdp"])):
        mine = (lax.axis_index("fsdp") // mask) % 2
        send = lax.dynamic_index_in_dim(held, 1 - mine, 0, keepdims=False)
        keep = lax.dynamic_index_in_dim(held, mine, 0, keepdims=False)
        held = keep + swap(send, "fsdp", mask, sizes["fsdp"])
    for mask in bits_of(sizes["dp"]):
        held = held + swap(held, "dp", mask, sizes["dp"])
    return held


def local(sizes, *arguments):
    (
        block_input,
        segment_ids,
        norm1_gain,
        norm1_bias,
        qkv_weight,
        qkv_bias,
        query_gain,
        key_gain,
        out_weight,
        out_bias,
        norm2_gain,
        norm2_bias,
        up_weight,
        up_bias,
        down_weight,
        down_bias,
        output_grad,
    ) = arguments
    fsdp = sizes["fsdp"]
    rank = lax.axis_index("fsdp")
    small_args = (
        norm1_gain,
        norm1_bias,
        qkv_bias,
        query_gain,
        key_gain,
        out_bias,
        norm2_gain,
        norm2_bias,
        up_bias,
        down_bias,
    )
    widths = [item.shape[0] for item in small_args]
    seg_col = segment_ids[:, None]
    joined = fsdp == 4 and sizes["dp"] == 8
    if joined:
        (
            segq, segk, h1, qkv, rstd, mixed, lse, x1, h2, gain1, gain2, downb, qgain, kgain, upb,
            *fulls,
        ) = begin(
            block_input, seg_col, small_args, (qkv_weight, out_weight, up_weight, down_weight)
        )
        qkv_pieces, out_pieces, up_pieces, down_pieces = [
            [full.reshape(-1, full.shape[-1])] for full in fulls
        ]
    else:
        lane = jnp.arange(PAIR)[None, :]
        match = (seg_col == lane) & (lane < HD)
        segq = jnp.where(match, QMARK, jnp.where(lane == HD, 1.0, 0.0)).astype(BF)
        segk = jnp.where(
            match,
            KMARK,
            jnp.where(lane == HD, -QMARK * KMARK, jnp.where((lane > HD) & (lane <= HD + 3), -1.0, 0.0)),
        ).astype(BF)
        packed = jnp.stack(gather_shards(jnp.concatenate(small_args), fsdp))
        packed = packed[jnp.arange(fsdp) ^ rank].astype(F32)
        smalls = []
        at = 0
        for width in widths:
            smalls.append(packed[:, at : at + width].reshape(1, fsdp * width))
            at += width
        gain1, shift1, qkvb, qgain, kgain, outb, gain2, shift2, upb, downb = smalls
        qgain = jnp.concatenate([qgain, qgain], axis=1)
        kgain = jnp.concatenate([kgain, kgain], axis=1)
        qkv_pieces = gather_shards(qkv_weight, fsdp)
        out_pieces = gather_shards(out_weight, fsdp)
        up_pieces = gather_shards(up_weight, fsdp)
        down_pieces = gather_shards(down_weight, fsdp)

        h1, qkv, rstd = front(block_input, gain1, shift1, qkv_pieces, qkvb, qgain, kgain)
        mixed, lse = attend(qkv, segq, segk)
        x1, h2 = middle(mixed, block_input, out_pieces, outb, gain2, shift2)
    output, gx1, ga, dup, ddown, dubias, dvec2 = mlp(
        h2, x1, seg_col, output_grad, up_pieces, down_pieces, upb, downb, gain2, fsdp
    )
    if joined:
        input_grad, totals, small = finish(
            mixed, ga, qkv, segq, segk, lse, rstd, qgain, kgain, h1, block_input, gx1, gain1,
            dubias, dvec2, dup, ddown, out_pieces, qkv_pieces,
        )
        up_total, down_total, out_total, qkv_total = unpack(totals)
        down_total = down_total.reshape(D, D)
        dvec1 = small[0:2]
        dqkvb = small[2:5]
        dgains = small[5, : 2 * PAIR].reshape(2, 2, HD).sum(axis=1)
        dvec2 = small[6:10]
        dubias = small[10:14]
    else:
        go, dout = outback(mixed, ga, out_pieces)
        gqkv, dheads = attback(qkv, segq, segk, mixed, lse, go, rstd, qgain, kgain)
        dqkv, dqkvb = qkvgrad(h1, gqkv)
        input_grad, dvec1 = back(gqkv, block_input, gx1, qkv_pieces, gain1)
        order = [("fsdp", m) for m in bits_of(fsdp)] + [("dp", m) for m in bits_of(sizes["dp"])]
        dup = dup.transpose(1, 2, 0, 3).reshape(D, -1)
        ddown = ddown.transpose(1, 0, 2, 3).reshape(-1, D)
        up_total, down_total, out_total, qkv_total = [
            reduce_grad(grad, order, sizes) for grad in (dup, ddown, dout, dqkv)
        ]
        dgains = dheads[:, 0, :].reshape(2, HEADS, HD).sum(axis=1)

    parts = (
        dvec1[0],
        dvec1[1],
        dqkvb,
        dgains[0],
        dgains[1],
        dvec2[2],
        dvec2[0],
        dvec2[1],
        dubias,
        dvec2[3],
    )
    small = jnp.concatenate([part.reshape(fsdp, -1) for part in parts], axis=1)
    if joined:
        small = lax.dynamic_index_in_dim(small, rank, 0, keepdims=False)
    else:
        small = reduce_small(small, sizes)
    shares = []
    at = 0
    for width in widths:
        shares.append(small[at : at + width])
        at += width
    n1g, n1b, qkvb_total, qg, kg, outb_total, n2g, n2b, upb_total, downb_total = shares
    return (
        output,
        input_grad,
        n1g,
        n1b,
        qkv_total,
        qkvb_total,
        qg,
        kg,
        out_total,
        outb_total,
        n2g,
        n2b,
        up_total,
        upb_total,
        down_total,
        downb_total,
    )


def solution(mesh):
    rows, shard = P(("dp", "fsdp"), None), P("fsdp")
    matrix = P("fsdp", None)
    placed = (
        (rows, P(("dp", "fsdp")), shard, shard, matrix, shard, shard, shard)
        + (matrix, shard, shard, shard, matrix, shard, matrix, shard, rows)
    )
    results = (
        (rows, rows, shard, shard, matrix, shard, shard, shard)
        + (matrix, shard, shard, shard, matrix, shard, matrix, shard)
    )
    return jax.shard_map(
        functools.partial(local, dict(mesh.shape)),
        mesh=mesh,
        in_specs=placed,
        out_specs=results,
        check_vma=False,
    )
```
